32 devices in a mesh: emb: 4 (over z), col: 2 (over y), row: 4 (over x, core).
Axes of the slice: x: 2, y: 2, z: 4, core: 2. Of those that a mesh axis runs over, the one named last changes fastest.
Arguments:
- inter_mask: int32 [1024, 32768], P('row', 'col')
- emb_user: bfloat16 [1024, 64], P(('row', 'col'), 'emb')
- emb_item: bfloat16 [32768, 64], P(('col', 'row'), 'emb')
- triples: int32 [4096, 3], replicated
Outputs:
- output 1: bfloat16 [1024, 64], P(('row', 'col'), 'emb')
- output 2: bfloat16 [32768, 64], P(('col', 'row'), 'emb')
- output 3: float32 [4096], replicated
All inputs are finite; a program needn't handle non-finite values.
Results may differ from the reference program's by a relative error of at most 0.0133188.
Values are sent between devices in bfloat16 or wider.
A program may use at most 1 GiB of HBM per device.

```python
import jax
import jax.numpy as jnp
from jax import lax

NUM_USERS = 1024
NUM_ITEMS = 32768
EMB_DIM = 64
NUM_TRIPLES = 4096
NUM_LAYERS = 3
SPARSITY = 8
NUM_GROUPS = 8


def setup_inputs(seed: int = 0) -> dict:
    key = jax.random.key(seed)
    key_list = jax.random.split(key, 10)
    inter_mask = (jax.random.randint(key_list[0], (NUM_USERS, NUM_ITEMS), 0, SPARSITY) == 0).astype(jnp.int32)
    mean_user = jax.random.normal(key_list[1], (EMB_DIM,), jnp.float32)
    mean_item = jax.random.normal(key_list[2], (EMB_DIM,), jnp.float32)
    noise_user = jax.random.normal(key_list[3], (NUM_USERS, EMB_DIM), jnp.float32)
    noise_item = jax.random.normal(key_list[4], (NUM_ITEMS, EMB_DIM), jnp.float32)
    group_user = jax.random.normal(key_list[8], (NUM_GROUPS, EMB_DIM), jnp.float32)
    group_item = jax.random.normal(key_list[9], (NUM_GROUPS, EMB_DIM), jnp.float32)
    user_group = (jnp.arange(NUM_USERS) * NUM_GROUPS) // NUM_USERS
    item_group = (jnp.arange(NUM_ITEMS) * NUM_GROUPS) // NUM_ITEMS
    emb_user = (0.5 * (mean_user[None, :] + 1.5 * group_user[user_group] + noise_user)).astype(jnp.bfloat16)
    emb_item = (0.5 * (mean_item[None, :] + 1.5 * group_item[item_group] + noise_item)).astype(jnp.bfloat16)
    users = jax.random.randint(key_list[5], (NUM_TRIPLES,), 0, NUM_USERS).at[0].set(NUM_USERS - 1)
    pos_items = jax.random.randint(key_list[6], (NUM_TRIPLES,), 0, NUM_ITEMS).at[0].set(NUM_ITEMS - 1)
    neg_items = jax.random.randint(key_list[7], (NUM_TRIPLES,), 0, NUM_ITEMS).at[1].set(0)
    triples = jnp.stack([users, pos_items, neg_items], axis=1).astype(jnp.int32)
    return {"inter_mask": inter_mask, "emb_user": emb_user, "emb_item": emb_item, "triples": triples}


def reference(inter_mask, emb_user, emb_item, triples):
    deg_user = jnp.maximum(jnp.sum(inter_mask, axis=1), 1).astype(jnp.float32)
    deg_item = jnp.maximum(jnp.sum(inter_mask, axis=0), 1).astype(jnp.float32)
    adj_norm = ((lax.rsqrt(deg_user)[:, None] * inter_mask.astype(jnp.float32)) * lax.rsqrt(deg_item)[None, :]).astype(jnp.bfloat16)

    def layer_step(carry, unused):
        user_cur, item_cur, user_acc, item_acc = carry
        user_next = jnp.dot(adj_norm, item_cur, preferred_element_type=jnp.float32).astype(jnp.bfloat16)
        item_next = jnp.dot(adj_norm.T, user_cur, preferred_element_type=jnp.float32).astype(jnp.bfloat16)
        new_carry = (user_next, item_next, user_acc + user_next.astype(jnp.float32), item_acc + item_next.astype(jnp.float32))
        return new_carry, None

    init_state = (emb_user, emb_item, emb_user.astype(jnp.float32), emb_item.astype(jnp.float32))
    carry_out, scan_ys = lax.scan(layer_step, init_state, None, length=NUM_LAYERS)
    final_user = (carry_out[2] / (NUM_LAYERS + 1)).astype(jnp.bfloat16)
    final_item = (carry_out[3] / (NUM_LAYERS + 1)).astype(jnp.bfloat16)
    e_user = jnp.take(final_user, triples[:, 0], axis=0).astype(jnp.float32)
    e_pos = jnp.take(final_item, triples[:, 1], axis=0).astype(jnp.float32)
    e_neg = jnp.take(final_item, triples[:, 2], axis=0).astype(jnp.float32)
    score = jnp.sum(e_user * (e_pos - e_neg), axis=1)
    bpr_loss = jax.nn.softplus(-score)
    return final_user, final_item, bpr_loss
```

```python
import functools

import jax
import jax.numpy as jnp
from jax import lax
from jax.experimental import pallas as pl
from jax.experimental.pallas import tpu as pltpu
from jax.sharding import PartitionSpec as P

NUM_LAYERS = 3
MESH = pl.DeviceIdType.MESH
F32 = jnp.float32
BF16 = jnp.bfloat16

NQ = 4
NS = 4
LB = 256
GL = 256


class Copies:
    def __init__(self, send_sems, recv_sems):
        self.send_sems, self.recv_sems, self.started = send_sems, recv_sems, []

    def send(self, src, dst, device):
        k = len(self.started)
        copy = pltpu.make_async_remote_copy(
            src_ref=src, dst_ref=dst, send_sem=self.send_sems.at[k],
            recv_sem=self.recv_sems.at[k], device_id=device, device_id_type=MESH)
        copy.start()
        self.started.append(copy)
        return copy

    def drain(self):
        for copy in self.started:
            copy.wait_send()


NUM_SEMS = 120


def kernel(mask_hbm, u0_ref, i0_ref, trip_ref, outu_ref, outi_ref, loss_ref,
           maskv, adj, csum, crd, crx, cch, invi, racc, rsum, rrecv, invu,
           upan, upart, urecv, ipan, ipart, ird, irx, isum,
           ohp, ohn, ohu, hip, hin, hiu, gpart, gsum, grd, grx, gry, eu, zbuf, lossb,
           mask_sems, send_sems, recv_sems):
    users = maskv.shape[1]
    quarter = maskv.shape[2]
    own_users = u0_ref.shape[1]
    sc = quarter // NS
    home = ohp.shape[2]

    z = lax.axis_index("emb")
    y = lax.axis_index("col")
    r = lax.axis_index("row")
    x = r // 2
    c = r % 2
    nz = 4

    def rel(m):
        xx = x if m < 2 else 1 - x
        cc = c if m % 2 == 0 else 1 - c
        return 2 * xx + cc

    dev_d = (z, y, rel(1))
    dev_x = (z, y, rel(2))
    dev_xd = (z, y, rel(3))
    dev_y = (z, 1 - y, r)
    dev_z = [((z + k) % nz, y, r) for k in (1, 2, 3)]

    cp = Copies(send_sems, recv_sems)

    mask_copies = {}
    for m in (3, 2, 1, 0):
        off = pl.multiple_of(rel(m) * quarter, quarter)
        mc = pltpu.make_async_copy(mask_hbm.at[:, pl.ds(off, quarter)], maskv.at[m], mask_sems.at[m])
        mc.start()
        mask_copies[m] = mc

    barrier = pltpu.get_barrier_semaphore()
    for dev in (dev_d, dev_x, dev_xd, dev_y, *dev_z):
        pl.semaphore_signal(barrier, inc=1, device_id=dev, device_id_type=MESH)
    pl.semaphore_wait(barrier, 7)

    y_off = pl.multiple_of(y * own_users, own_users)
    u0_y = cp.send(u0_ref, upan.at[0, :, pl.ds(y_off, own_users)], dev_y)
    upan[0, :, pl.ds(y_off, own_users)] = u0_ref[...]
    i0_x = cp.send(i0_ref, ipan.at[0, 2], dev_x)
    i0_d = cp.send(i0_ref, ipan.at[0, 1], dev_d)
    ipan[0, 0] = i0_ref[...]

    racc[...] = jnp.zeros_like(racc)

    def sums(m):
        def body(j, carry):
            off = pl.multiple_of(j * LB, LB)
            part = maskv[m, pl.ds(0, 8), pl.ds(off, LB)]
            for i in range(1, users // 8):
                part = part + maskv[m, pl.ds(8 * i, 8), pl.ds(off, LB)]
            csum[m, :, pl.ds(off, LB)] = jnp.sum(part.astype(F32), axis=0, keepdims=True)
            row = maskv[m, :, pl.ds(off, 128)]
            for g in range(1, LB // 128):
                row = row + maskv[m, :, pl.ds(pl.multiple_of(off + 128 * g, 128), 128)]
            racc[...] += row
            return carry
        lax.fori_loop(0, quarter // LB, body, 0)

    def one_hots(m):
        base = pl.multiple_of(rel(m) * home, home)
        for row, oh, hi in ((1, ohp, hip), (2, ohn, hin)):
            ids = trip_ref[pl.ds(row, 1), pl.ds(base, home)]
            owned = ids // quarter == y * NQ + r
            hi[m] = (ids % quarter) // GL
            low = jnp.where(owned, ids % GL, -1)
            for t in range(home // LB):
                lanes = low[:, t * LB:(t + 1) * LB]
                hit = lax.broadcasted_iota(jnp.int32, (GL, LB), 0) == lanes
                oh[m, :, t * LB:(t + 1) * LB] = jnp.where(hit, 1.0, 0.0).astype(BF16)

    csum_d, csum_x = {}, {}
    i0_f = None
    prev = None

    def chip_sums(m):
        csum_d[m].wait_recv()
        cch[m] = csum[m] + crd[m]
        csum_x[m ^ 2] = cp.send(cch.at[m], crx.at[m ^ 2], dev_x)

    for m in (3, 2, 1, 0):
        mask_copies[m].wait()
        sums(m)
        csum_d[m ^ 1] = cp.send(csum.at[m], crd.at[m ^ 1], dev_d)
        if m == 2:
            i0_x.wait_recv()
            i0_f = cp.send(ipan.at[0, 2], ipan.at[0, 3], dev_d)
            chip_sums(3)
            chip_sums(2)
    rows = jnp.transpose(racc[...].astype(F32), (1, 0))
    rsum[...] = jnp.sum(rows, axis=0, keepdims=True)
    rs_y = cp.send(rsum, rrecv, dev_y)
    chip_sums(1)
    chip_sums(0)

    rs_y.wait_recv()
    inv_row = lax.rsqrt(jnp.maximum(rsum[...] + rrecv[...], 1.0))
    invu[...] = jnp.transpose(jnp.broadcast_to(inv_row, (128, users)), (1, 0))
    u0_y.wait_recv()

    def build(m, s):
        def body(j, carry):
            iu = invu[...]
            for g in range(LB // 128):
                off = pl.multiple_of(s * sc + j * LB + g * 128, 128)
                blk = maskv[m, :, pl.ds(off, 128)]
                ii = invi[m, :, pl.ds(off, 128)]
                adj[m, :, pl.ds(off, 128)] = jnp.where(blk != 0, iu * ii, 0.0).astype(BF16)
            return carry
        lax.fori_loop(0, sc // LB, body, 0)

    def item_piece(k, m, s):
        sl = pl.ds(s * sc, sc)
        ipart[k, m, :, sl] = jnp.dot(upan[k], adj[m, :, sl], preferred_element_type=F32)

    def user_part(k, m):
        return lax.dot_general(ipan[k, m], adj[m], (((1,), (1,)), ((), ())), preferred_element_type=F32)

    def to_core(k, m, s):
        sl = pl.ds(s * sc, sc)
        return cp.send(ipart.at[k, m, :, sl], ird.at[k, (m ^ 1) // 2, :, sl], dev_d)

    def to_x(k, s, got):
        sl = pl.ds(s * sc, sc)
        got.wait_recv()
        isum[k, :, sl] = ipart[k, 2, :, sl] + ird[k, 1, :, sl]
        return cp.send(isum.at[k, :, sl], irx.at[k, :, sl], dev_x)

    def own_piece(k, s, got_d, got_x):
        sl = pl.ds(s * sc, sc)
        got_d.wait_recv()
        got_x.wait_recv()
        total = (ipart[k, 0, :, sl] + ird[k, 0, :, sl]) + irx[k, :, sl]
        ipan[k + 1, 0, :, sl] = total.astype(BF16)

    def gather_piece(k, s):
        sl = pl.ds(s * sc, sc)
        gx = cp.send(ipan.at[k, 0, :, sl], ipan.at[k, 2, :, sl], dev_x)
        gd = cp.send(ipan.at[k, 0, :, sl], ipan.at[k, 1, :, sl], dev_d)
        return gx, gd

    def forward_piece(k, s, gx):
        sl = pl.ds(s * sc, sc)
        gx.wait_recv()
        return cp.send(ipan.at[k, 2, :, sl], ipan.at[k, 3, :, sl], dev_d)

    def send_user(k, acc):
        upart[k] = acc
        return cp.send(upart.at[k], urecv.at[k], dev_y)

    def take_user(k, got):
        got.wait_recv()
        upan[k + 1] = (upart[k] + urecv[k]).astype(BF16)

    d1, x1 = {}, {}
    for m in (3, 2, 1, 0):
        csum_x[m].wait_recv()
        invi[m] = lax.rsqrt(jnp.maximum(cch[m] + crx[m], 1.0))
        for s in range(NS):
            build(m, s)
            item_piece(0, m, s)
            if m in (3, 1):
                d1[m ^ 1, s] = to_core(0, m, s)
            if m == 2:
                x1[s] = to_x(0, s, d1[2, s])
    i0_d.wait_recv()
    i0_f.wait_recv()
    acc = user_part(0, 0)
    for m in (1, 2, 3):
        acc = acc + user_part(0, m)
    u1 = send_user(0, acc)
    for m in (3, 2, 1, 0):
        one_hots(m)
    ubase = pl.multiple_of(r * home, home)
    uids = trip_ref[pl.ds(0, 1), pl.ds(ubase, home)]
    urow = uids // users
    hiu[...] = urow
    for t in range(home // LB):
        lanes = (uids % users)[:, t * LB:(t + 1) * LB]
        hit = lax.broadcasted_iota(jnp.int32, (GL, LB), 0) == lanes
        ohu[:, t * LB:(t + 1) * LB] = jnp.where(hit, 1.0, 0.0).astype(BF16)

    take_user(0, u1)
    d2, x2 = {}, {}
    for m in (3, 2, 1, 0):
        for s in range(NS):
            item_piece(1, m, s)
            if m in (3, 1):
                d2[m ^ 1, s] = to_core(1, m, s)
    g1 = {}
    for s in range(NS):
        own_piece(0, s, d1[0, s], x1[s])
        g1[s] = gather_piece(1, s)
    for s in range(NS):
        x2[s] = to_x(1, s, d2[2, s])
    f1 = {}
    for s in range(NS):
        f1[s] = forward_piece(1, s, g1[s][0])
    acc = user_part(1, 0)
    for s in range(NS):
        g1[s][1].wait_recv()
    acc = acc + user_part(1, 1)
    acc = acc + user_part(1, 2)
    for s in range(NS):
        f1[s].wait_recv()
    acc = acc + user_part(1, 3)
    u2 = send_user(1, acc)
    g2 = {}
    take_user(1, u2)
    d3, x3 = {}, {}
    for m in (3, 2, 1, 0):
        for s in range(NS):
            item_piece(2, m, s)
            if m in (3, 1):
                d3[m ^ 1, s] = to_core(2, m, s)
            if m == 2:
                x3[s] = to_x(2, s, d3[2, s])
    for s in range(NS):
        own_piece(1, s, d2[0, s], x2[s])
        g2[s] = gather_piece(2, s)
    f2 = {}
    for s in range(NS):
        f2[s] = forward_piece(2, s, g2[s][0])
    acc = user_part(2, 0)
    for s in range(NS):
        g2[s][1].wait_recv()
    acc = acc + user_part(2, 1)
    acc = acc + user_part(2, 2)
    for s in range(NS):
        f2[s].wait_recv()
    acc = acc + user_part(2, 3)
    u3 = send_user(2, acc)

    for s in range(NS):
        own_piece(2, s, d3[0, s], x3[s])
        sl = pl.ds(s * sc, sc)
        tot = ((ipan[0, 0, :, sl].astype(F32) + ipan[1, 0, :, sl].astype(F32))
               + ipan[2, 0, :, sl].astype(F32)) + ipan[3, 0, :, sl].astype(F32)
        outi_ref[:, sl] = (tot * (1.0 / (NUM_LAYERS + 1))).astype(BF16)
    table = jnp.concatenate(
        [outi_ref[:, g * GL:(g + 1) * GL] for g in range(quarter // GL)], axis=0)

    def pick(tab, oh, hi, n):
        got = jnp.dot(tab, oh, preferred_element_type=F32)
        rows16 = got.shape[0] // n
        out = jnp.where(hi == 0, got[:rows16], 0.0)
        for g in range(1, n):
            out = out + jnp.where(hi == g, got[g * rows16:(g + 1) * rows16], 0.0)
        return out

    def differences(m):
        for t in range(home // LB):
            sl = slice(t * LB, (t + 1) * LB)
            pos = pick(table, ohp[m, :, sl], hip[m, :, sl], quarter // GL)
            neg = pick(table, ohn[m, :, sl], hin[m, :, sl], quarter // GL)
            gpart[m, :, sl] = pos - neg

    differences(3)
    gd3 = cp.send(gpart.at[3], grd.at[1], dev_d)
    differences(2)
    gd3.wait_recv()
    gsum[1] = gpart[2] + grd[1]
    gx = cp.send(gsum.at[1], grx, dev_x)
    differences(1)
    gd1 = cp.send(gpart.at[1], grd.at[0], dev_d)
    differences(0)

    take_user(2, u3)
    ut = ((upan[0].astype(F32) + upan[1].astype(F32)) + upan[2].astype(F32)) + upan[3].astype(F32)
    eu[0] = (ut * (1.0 / (NUM_LAYERS + 1))).astype(BF16)
    outu_ref[...] = eu[0, :, pl.ds(y_off, own_users)]
    e1 = cp.send(eu.at[0], eu.at[1], dev_d)
    e2 = cp.send(eu.at[0], eu.at[2], dev_x)
    e3 = cp.send(eu.at[0], eu.at[3], dev_xd)

    gd1.wait_recv()
    gx.wait_recv()
    gsum[0] = (gpart[0] + grd[0]) + grx[...]
    gy = cp.send(gsum.at[0], gry, dev_y)

    e1.wait_recv()
    e2.wait_recv()
    e3.wait_recv()
    utab = jnp.concatenate([eu[m] for m in range(NQ)], axis=0)
    blk_id = hiu[...]
    place = jnp.where(blk_id // 2 == x, 0, 2) + jnp.where(blk_id % 2 == c, 0, 1)
    picked = []
    for t in range(home // LB):
        sl = slice(t * LB, (t + 1) * LB)
        picked.append(pick(utab, ohu[:, sl], place[:, sl], NQ))
    gy.wait_recv()
    for t in range(home // LB):
        sl = slice(t * LB, (t + 1) * LB)
        diff = gsum[0, :, sl] + gry[:, sl]
        zbuf[z, :, sl] = jnp.sum(picked[t] * diff, axis=0, keepdims=True)
    zc = [cp.send(zbuf.at[z], zbuf.at[z], dev) for dev in dev_z]
    for copy in zc:
        copy.wait_recv()
    score = ((zbuf[0] + zbuf[1]) + zbuf[2]) + zbuf[3]
    neg = -score
    lossb[r] = jnp.maximum(neg, 0.0) + jnp.log1p(jnp.exp(-jnp.abs(neg)))
    lc = [cp.send(lossb.at[r], lossb.at[r], dev) for dev in (dev_d, dev_x, dev_xd)]
    for copy in lc:
        copy.wait_recv()
    loss_ref[...] = lossb[...]
    cp.drain()


def solution(mesh):
    def local_fn(mask_blk, user_sh, item_sh, triples):
        users, items = mask_blk.shape
        cols, own_users = user_sh.shape[1], user_sh.shape[0]
        quarter = items // NQ
        home = triples.shape[0] // NQ
        vm = pltpu.VMEM
        nl = NUM_LAYERS
        scratch = [
            vm((NQ, users, quarter), jnp.int32), vm((NQ, users, quarter), BF16),
            vm((NQ, 1, quarter), F32), vm((NQ, 1, quarter), F32), vm((NQ, 1, quarter), F32),
            vm((NQ, 1, quarter), F32), vm((NQ, 1, quarter), F32),
            vm((users, 128), jnp.int32), vm((1, users), F32), vm((1, users), F32), vm((users, 128), F32),
            vm((nl + 1, cols, users), BF16), vm((nl, cols, users), F32), vm((nl, cols, users), F32),
            vm((nl + 1, NQ, cols, quarter), BF16), vm((nl, NQ, cols, quarter), F32),
            vm((nl, 2, cols, quarter), F32), vm((nl, cols, quarter), F32), vm((nl, cols, quarter), F32),
            vm((NQ, GL, home), BF16), vm((NQ, GL, home), BF16), vm((GL, home), BF16),
            vm((NQ, 1, home), jnp.int32), vm((NQ, 1, home), jnp.int32), vm((1, home), jnp.int32),
            vm((NQ, cols, home), F32), vm((2, cols, home), F32), vm((2, cols, home), F32),
            vm((cols, home), F32), vm((cols, home), F32),
            vm((NQ, cols, users), BF16), vm((4, 1, home), F32), vm((NQ, 1, home), F32),
            pltpu.SemaphoreType.DMA((NQ,)),
            pltpu.SemaphoreType.DMA((NUM_SEMS,)), pltpu.SemaphoreType.DMA((NUM_SEMS,)),
        ]
        vspec = pl.BlockSpec(memory_space=pltpu.VMEM)
        out_u, out_i, loss = pl.pallas_call(
            kernel,
            out_shape=[
                jax.ShapeDtypeStruct((cols, own_users), BF16),
                jax.ShapeDtypeStruct((cols, quarter), BF16),
                jax.ShapeDtypeStruct((NQ, 1, home), F32)],
            in_specs=[pl.BlockSpec(memory_space=pl.ANY), vspec, vspec, vspec],
            out_specs=[vspec, vspec, vspec],
            scratch_shapes=scratch,
            compiler_params=pltpu.CompilerParams(
                collective_id=0, has_side_effects=True, vmem_limit_bytes=60 * 1024 * 1024),
        )(mask_blk, user_sh.T, item_sh.T, triples.T)
        return out_u.T, out_i.T, loss.reshape(-1)

    return jax.shard_map(
        local_fn, mesh=mesh,
        in_specs=(P("row", "col"), P(("row", "col"), "emb"), P(("col", "row"), "emb"), P()),
        out_specs=(P(("row", "col"), "emb"), P(("col", "row"), "emb"), P()),
        check_vma=False)
```

```python
import functools

import jax
import jax.numpy as jnp
from jax import lax
from jax.experimental import pallas as pl
from jax.experimental.pallas import tpu as pltpu
from jax.sharding import PartitionSpec as P

NUM_LAYERS = 3
MESH = pl.DeviceIdType.MESH
F32 = jnp.float32
BF16 = jnp.bfloat16

NQ = 4
NS = 4
LB = 256
GL = 256


class Copies:
    def __init__(self, send_sems, recv_sems):
        self.send_sems, self.recv_sems, self.started = send_sems, recv_sems, []

    def send(self, src, dst, device):
        k = len(self.started)
        copy = pltpu.make_async_remote_copy(
            src_ref=src, dst_ref=dst, send_sem=self.send_sems.at[k],
            recv_sem=self.recv_sems.at[k], device_id=device, device_id_type=MESH)
        copy.start()
        self.started.append(copy)
        return copy

    def drain(self):
        for copy in self.started:
            copy.wait_send()


NUM_SEMS = 120


class Phase:
    def __init__(self):
        self.current = None

    def __call__(self, name):
        if self.current is not None:
            self.current.__exit__(None, None, None)
        self.current = None
        if name:
            self.current = jax.named_scope(name)
            self.current.__enter__()


def kernel(mask_hbm, u0_hbm, i0_hbm, trip_hbm, outu_ref, outi_ref, loss_ref,
           maskv, adj, csum, crd, crx, cch, invi, racc, rsum, rrecv, invu, trip_ref,
           upan, upart, urecv, ipan, ipart, ird, irx, isum,
           ohp, ohn, ohu, hip, hin, hiu, gpart, gsum, grd, grx, gry, eu, zbuf, lossb,
           in_sems, send_sems, recv_sems):
    users = maskv.shape[1]
    quarter = maskv.shape[2]
    own_users = u0_hbm.shape[1]
    sc = quarter // NS
    home = ohp.shape[2]
    hh = home // 2

    z = lax.axis_index("emb")
    y = lax.axis_index("col")
    r = lax.axis_index("row")
    x = r // 2
    c = r % 2
    nz = 4

    def rel(m):
        xx = x if m < 2 else 1 - x
        cc = c if m % 2 == 0 else 1 - c
        return 2 * xx + cc

    dev_d = (z, y, rel(1))
    dev_x = (z, y, rel(2))
    dev_xd = (z, y, rel(3))
    dev_y = (z, 1 - y, r)
    dev_z = [((z + k) % nz, y, r) for k in (1, 2, 3)]

    cp = Copies(send_sems, recv_sems)
    phase = Phase()
    phase("start")

    def load(src, dst, k):
        copy = pltpu.make_async_copy(src, dst, in_sems.at[k])
        copy.start()
        return copy

    y_off = pl.multiple_of(y * own_users, own_users)
    mask_copies = {}
    for m in (3, 2, 1, 0):
        off = pl.multiple_of(rel(m) * quarter, quarter)
        mask_copies[m] = load(mask_hbm.at[:, pl.ds(off, quarter)], maskv.at[m], m)
        if m == 3:
            u0_in = load(u0_hbm, upan.at[0, :, pl.ds(y_off, own_users)], 4)
            i0_in = load(i0_hbm, ipan.at[0, 0], 5)
            trip_in = load(trip_hbm, trip_ref, 6)

    barrier = pltpu.get_barrier_semaphore()
    for dev in (dev_d, dev_x, dev_xd, dev_y, *dev_z):
        pl.semaphore_signal(barrier, inc=1, device_id=dev, device_id_type=MESH)

    racc[...] = jnp.zeros_like(racc)

    def sums(m):
        def body(j, carry):
            off = pl.multiple_of(j * LB, LB)
            part = None
            for i in range(users // 16):
                rows = pl.ds(16 * i, 16)
                blk = maskv[m, rows, pl.ds(off, LB)]
                adj[m, rows, pl.ds(off, LB)] = blk.astype(F32).astype(BF16)
                two = blk[:8] + blk[8:]
                part = two if part is None else part + two
                row = blk[:, :128]
                for g in range(1, LB // 128):
                    row = row + blk[:, 128 * g:128 * (g + 1)]
                racc[rows, :] += row
            csum[m, :, pl.ds(off, LB)] = jnp.sum(part.astype(F32), axis=0, keepdims=True)
            return carry
        lax.fori_loop(0, quarter // LB, body, 0)

    def one_hots(m):
        base = pl.multiple_of(rel(m) * home, home)
        for row, oh, hi in ((1, ohp, hip), (2, ohn, hin)):
            ids = trip_ref[pl.ds(row, 1), pl.ds(base, home)]
            owned = ids // quarter == y * NQ + r
            hi[m] = (ids % quarter) // GL
            low = jnp.where(owned, ids % GL, -1)
            for t in range(home // LB):
                lanes = low[:, t * LB:(t + 1) * LB]
                hit = lax.broadcasted_iota(jnp.int32, (GL, LB), 0) == lanes
                oh[m, :, t * LB:(t + 1) * LB] = jnp.where(hit, 1.0, 0.0).astype(BF16)

    def user_one_hots():
        base = pl.multiple_of(r * home, home)
        uids = trip_ref[pl.ds(0, 1), pl.ds(base, home)]
        hiu[...] = uids // users
        for t in range(home // LB):
            lanes = (uids % users)[:, t * LB:(t + 1) * LB]
            hit = lax.broadcasted_iota(jnp.int32, (GL, LB), 0) == lanes
            ohu[:, t * LB:(t + 1) * LB] = jnp.where(hit, 1.0, 0.0).astype(BF16)

    csum_d, csum_x = {}, {}

    def chip_sums(m):
        csum_d[m].wait_recv()
        cch[m] = csum[m] + crd[m]
        csum_x[m ^ 2] = cp.send(cch.at[m], crx.at[m ^ 2], dev_x)

    def send_sums(m):
        csum_d[m ^ 1] = cp.send(csum.at[m], crd.at[m ^ 1], dev_d)

    for m in (3, 2):
        phase(f"mask_wait{m}")
        mask_copies[m].wait()
        phase(f"sums{m}")
        sums(m)
    phase("in_wait")
    u0_in.wait()
    i0_in.wait()
    trip_in.wait()
    phase("barrier")
    pl.semaphore_wait(barrier, 7)
    phase("layer0")
    send_sums(3)
    send_sums(2)
    u0_y = cp.send(upan.at[0, :, pl.ds(y_off, own_users)], upan.at[0, :, pl.ds(y_off, own_users)], dev_y)
    i0_x = cp.send(ipan.at[0, 0], ipan.at[0, 2], dev_x)
    i0_d = cp.send(ipan.at[0, 0], ipan.at[0, 1], dev_d)
    for m in (1, 0):
        phase(f"mask_wait{m}")
        mask_copies[m].wait()
        phase(f"sums{m}")
        sums(m)
        send_sums(m)
        if m == 1:
            phase("chip32")
            chip_sums(3)
            chip_sums(2)
    phase("rows")
    rows = jnp.transpose(racc[...].astype(F32), (1, 0))
    rsum[...] = jnp.sum(rows, axis=0, keepdims=True)
    rs_y = cp.send(rsum, rrecv, dev_y)
    one_hots(3)
    one_hots(2)
    phase("chip10")
    chip_sums(1)
    chip_sums(0)
    phase("onehots")
    one_hots(1)
    one_hots(0)
    user_one_hots()
    phase("i0_x_wait")
    i0_x.wait_recv()
    i0_f = cp.send(ipan.at[0, 2], ipan.at[0, 3], dev_d)
    u0_y.wait_recv()
    phase("rs_wait")
    rs_y.wait_recv()
    phase("invu")
    inv_row = lax.rsqrt(jnp.maximum(rsum[...] + rrecv[...], 1.0))
    invu[...] = jnp.transpose(jnp.broadcast_to(inv_row, (128, users)), (1, 0))
    phase("cx_wait")
    for m in (3, 2, 1, 0):
        csum_x[m].wait_recv()
        invi[m] = lax.rsqrt(jnp.maximum(cch[m] + crx[m], 1.0))

    def build(m, s):
        def body(j, carry):
            off = pl.multiple_of(s * sc + j * LB, LB)
            ii = invi[m, :, pl.ds(off, LB)]
            for i in range(users // 16):
                rows = pl.ds(16 * i, 16)
                iu = invu[rows, :]
                for g in range(LB // 128):
                    lanes = pl.ds(pl.multiple_of(off + 128 * g, 128), 128)
                    scale = (iu * ii[:, 128 * g:128 * (g + 1)]).astype(BF16)
                    adj[m, rows, lanes] = scale * adj[m, rows, lanes]
            return carry
        lax.fori_loop(0, sc // LB, body, 0)

    def item_piece(k, m, s):
        sl = pl.ds(s * sc, sc)
        ipart[k, m, :, sl] = jnp.dot(upan[k], adj[m, :, sl], preferred_element_type=F32)

    def user_part(k, m):
        return lax.dot_general(adj[m], ipan[k, m], (((1,), (1,)), ((), ())), preferred_element_type=F32)

    def to_core(k, m, s):
        sl = pl.ds(s * sc, sc)
        return cp.send(ipart.at[k, m, :, sl], ird.at[k, (m ^ 1) // 2, :, sl], dev_d)

    def to_x(k, s, got):
        sl = pl.ds(s * sc, sc)
        got.wait_recv()
        isum[k, :, sl] = ipart[k, 2, :, sl] + ird[k, 1, :, sl]
        return cp.send(isum.at[k, :, sl], irx.at[k, :, sl], dev_x)

    def own_piece(k, s, got_d, got_x):
        sl = pl.ds(s * sc, sc)
        got_d.wait_recv()
        got_x.wait_recv()
        total = (ipart[k, 0, :, sl] + ird[k, 0, :, sl]) + irx[k, :, sl]
        ipan[k + 1, 0, :, sl] = total.astype(BF16)

    def gather_piece(k, s):
        sl = pl.ds(s * sc, sc)
        gx = cp.send(ipan.at[k, 0, :, sl], ipan.at[k, 2, :, sl], dev_x)
        gd = cp.send(ipan.at[k, 0, :, sl], ipan.at[k, 1, :, sl], dev_d)
        return gx, gd

    def forward_piece(k, s, gx):
        sl = pl.ds(s * sc, sc)
        gx.wait_recv()
        return cp.send(ipan.at[k, 2, :, sl], ipan.at[k, 3, :, sl], dev_d)

    def send_user(k, acc):
        upart[k] = jnp.transpose(acc, (1, 0))
        return cp.send(upart.at[k], urecv.at[k], dev_y)

    def take_user(k, got):
        got.wait_recv()
        upan[k + 1] = (upart[k] + urecv[k]).astype(BF16)

    d, xs = [{}, {}, {}], [{}, {}, {}]
    g, f = {}, {}
    phase("build32")
    for s in range(NS):
        build(3, s)
        item_piece(0, 3, s)
        d[0][2, s] = to_core(0, 3, s)
        build(2, s)
        item_piece(0, 2, s)
        if s:
            xs[0][s - 1] = to_x(0, s - 1, d[0][2, s - 1])
    xs[0][NS - 1] = to_x(0, NS - 1, d[0][2, NS - 1])
    phase("upart0_32")
    i0_d.wait_recv()
    i0_f.wait_recv()
    acc = user_part(0, 3) + user_part(0, 2)
    phase("build10")
    for s in range(NS):
        build(1, s)
        item_piece(0, 1, s)
        d[0][0, s] = to_core(0, 1, s)
        build(0, s)
        item_piece(0, 0, s)

    def own_gather(k, s):
        own_piece(k, s, d[k][0, s], xs[k][s])
        g[k + 1, s] = gather_piece(k + 1, s)

    phase("own1_0")
    own_gather(0, 0)
    phase("upart0_1")
    acc = acc + user_part(0, 1)
    phase("own1_1")
    own_gather(0, 1)
    phase("upart0_0")
    acc = acc + user_part(0, 0)
    u1 = send_user(0, acc)
    phase("own1_2")
    own_gather(0, 2)
    phase("own1_3")
    own_gather(0, 3)
    phase("upart1_0")
    acc = user_part(1, 0)
    phase("upart1_1")
    for s in range(NS):
        g[1, s][1].wait_recv()
    acc = acc + user_part(1, 1)
    phase("u1_wait")
    take_user(0, u1)
    phase("items2_32")
    for s in range(NS):
        item_piece(1, 3, s)
        d[1][2, s] = to_core(1, 3, s)
        item_piece(1, 2, s)
        if s:
            xs[1][s - 1] = to_x(1, s - 1, d[1][2, s - 1])
        if s == 1:
            f[1, 0] = forward_piece(1, 0, g[1, 0][0])
        if s == 2:
            f[1, 1] = forward_piece(1, 1, g[1, 1][0])
    xs[1][NS - 1] = to_x(1, NS - 1, d[1][2, NS - 1])
    phase("fwd1")
    f[1, 2] = forward_piece(1, 2, g[1, 2][0])
    f[1, 3] = forward_piece(1, 3, g[1, 3][0])
    phase("upart1_2")
    acc = acc + user_part(1, 2)
    phase("f1_wait")
    for s in range(NS):
        f[1, s].wait_recv()
    phase("upart1_3")
    acc = acc + user_part(1, 3)
    u2 = send_user(1, acc)
    phase("items2_10")
    for s in range(NS):
        item_piece(1, 1, s)
        d[1][0, s] = to_core(1, 1, s)
        item_piece(1, 0, s)
    phase("u2_wait")
    take_user(1, u2)
    phase("items3_32")
    for s in range(NS):
        item_piece(2, 3, s)
        d[2][2, s] = to_core(2, 3, s)
        item_piece(2, 2, s)
        if s:
            xs[2][s - 1] = to_x(2, s - 1, d[2][2, s - 1])
    xs[2][NS - 1] = to_x(2, NS - 1, d[2][2, NS - 1])
    phase("own2")
    for s in range(NS):
        own_gather(1, s)
    phase("items3_10")
    for s in range(NS):
        item_piece(2, 1, s)
        d[2][0, s] = to_core(2, 1, s)
        item_piece(2, 0, s)
    phase("upart2_01")
    acc = user_part(2, 0)
    for s in range(NS):
        g[2, s][1].wait_recv()
    acc = acc + user_part(2, 1)

    phase("own3")
    for s in range(NS):
        own_piece(2, s, d[2][0, s], xs[2][s])
        sl = pl.ds(s * sc, sc)
        tot = ((ipan[0, 0, :, sl].astype(F32) + ipan[1, 0, :, sl].astype(F32))
               + ipan[2, 0, :, sl].astype(F32)) + ipan[3, 0, :, sl].astype(F32)
        outi_ref[:, sl] = (tot * (1.0 / (NUM_LAYERS + 1))).astype(BF16)
    phase("table")
    table = jnp.concatenate(
        [outi_ref[:, g0 * GL:(g0 + 1) * GL] for g0 in range(quarter // GL)], axis=0)

    def pick(tab, oh, hi, n):
        got = jnp.dot(tab, oh, preferred_element_type=F32)
        rows16 = got.shape[0] // n
        out = jnp.where(hi == 0, got[:rows16], 0.0)
        for g0 in range(1, n):
            out = out + jnp.where(hi == g0, got[g0 * rows16:(g0 + 1) * rows16], 0.0)
        return out

    def differences(m, h):
        for t in range(hh // LB):
            sl = slice(h * hh + t * LB, h * hh + (t + 1) * LB)
            pos = pick(table, ohp[m, :, sl], hip[m, :, sl], quarter // GL)
            neg = pick(table, ohn[m, :, sl], hin[m, :, sl], quarter // GL)
            gpart[m, :, sl] = pos - neg

    half = [pl.ds(0, hh), pl.ds(hh, hh)]
    gd3, gd1, gx, gy = {}, {}, {}, {}
    phase("diff3")
    for h in (0, 1):
        differences(3, h)
        gd3[h] = cp.send(gpart.at[3, :, half[h]], grd.at[1, :, half[h]], dev_d)
    phase("diff2")
    for h in (0, 1):
        differences(2, h)
        gd3[h].wait_recv()
        gsum[1, :, half[h]] = gpart[2, :, half[h]] + grd[1, :, half[h]]
        gx[h] = cp.send(gsum.at[1, :, half[h]], grx.at[:, half[h]], dev_x)
    phase("diff1")
    for h in (0, 1):
        differences(1, h)
        gd1[h] = cp.send(gpart.at[1, :, half[h]], grd.at[0, :, half[h]], dev_d)
    phase("fwd2")
    for s in range(NS):
        f[2, s] = forward_piece(2, s, g[2, s][0])
    phase("upart2_2")
    acc = acc + user_part(2, 2)
    phase("f2_wait")
    for s in range(NS):
        f[2, s].wait_recv()
    phase("upart2_3")
    acc = acc + user_part(2, 3)
    u3 = send_user(2, acc)
    phase("diff0")
    for h in (0, 1):
        differences(0, h)
    phase("g_wait")
    for h in (0, 1):
        gd1[h].wait_recv()
        gx[h].wait_recv()
        gsum[0, :, half[h]] = (gpart[0, :, half[h]] + grd[0, :, half[h]]) + grx[:, half[h]]
        gy[h] = cp.send(gsum.at[0, :, half[h]], gry.at[:, half[h]], dev_y)

    phase("u3_wait")
    take_user(2, u3)
    phase("finalu")
    ut = ((upan[0].astype(F32) + upan[1].astype(F32)) + upan[2].astype(F32)) + upan[3].astype(F32)
    eu[0] = (ut * (1.0 / (NUM_LAYERS + 1))).astype(BF16)
    e1 = cp.send(eu.at[0], eu.at[1], dev_d)
    e2 = cp.send(eu.at[0], eu.at[2], dev_x)
    e3 = cp.send(eu.at[0], eu.at[3], dev_xd)
    outu_ref[...] = eu[0, :, pl.ds(y_off, own_users)]

    phase("e_wait")
    e1.wait_recv()
    e2.wait_recv()
    e3.wait_recv()
    phase("picku")
    utab = jnp.concatenate([eu[m] for m in range(NQ)], axis=0)
    blk_id = hiu[...]
    place = jnp.where(blk_id // 2 == x, 0, 2) + jnp.where(blk_id % 2 == c, 0, 1)
    picked = []
    for t in range(home // LB):
        sl = slice(t * LB, (t + 1) * LB)
        picked.append(pick(utab, ohu[:, sl], place[:, sl], NQ))
    phase("gy_wait")
    gy[0].wait_recv()
    gy[1].wait_recv()
    phase("dot")
    for t in range(home // LB):
        sl = slice(t * LB, (t + 1) * LB)
        diff = gsum[0, :, sl] + gry[:, sl]
        zbuf[z, :, sl] = jnp.sum(picked[t] * diff, axis=0, keepdims=True)
    zc = [cp.send(zbuf.at[z], zbuf.at[z], dev) for dev in dev_z]
    phase("z_wait")
    for copy in zc:
        copy.wait_recv()
    phase("loss")
    score = ((zbuf[0] + zbuf[1]) + zbuf[2]) + zbuf[3]
    neg = -score
    lossb[r] = jnp.maximum(neg, 0.0) + jnp.log1p(jnp.exp(-jnp.abs(neg)))
    lc = [cp.send(lossb.at[r], lossb.at[r], dev) for dev in (dev_d, dev_x, dev_xd)]
    phase("loss_wait")
    for copy in lc:
        copy.wait_recv()
    phase("end")
    loss_ref[...] = lossb[...]
    phase("drain")
    cp.drain()
    phase(None)


def emit(u_in, i_in, l_in, u_out, i_out, l_out):
    u_out[...] = u_in[...]
    i_out[...] = i_in[...]
    l_out[...] = l_in[...]


def solution(mesh):
    def local_fn(mask_blk, user_sh, item_sh, triples):
        users, items = mask_blk.shape
        cols, own_users = user_sh.shape[1], user_sh.shape[0]
        quarter = items // NQ
        home = triples.shape[0] // NQ
        vm = pltpu.VMEM
        nl = NUM_LAYERS
        scratch = [
            vm((NQ, users, quarter), jnp.int32), vm((NQ, users, quarter), BF16),
            vm((NQ, 1, quarter), F32), vm((NQ, 1, quarter), F32), vm((NQ, 1, quarter), F32),
            vm((NQ, 1, quarter), F32), vm((NQ, 1, quarter), F32),
            vm((users, 128), jnp.int32), vm((1, users), F32), vm((1, users), F32), vm((users, 128), F32),
            vm(triples.shape[::-1], jnp.int32),
            vm((nl + 1, cols, users), BF16), vm((nl, cols, users), F32), vm((nl, cols, users), F32),
            vm((nl + 1, NQ, cols, quarter), BF16), vm((nl, NQ, cols, quarter), F32),
            vm((nl, 2, cols, quarter), F32), vm((nl, cols, quarter), F32), vm((nl, cols, quarter), F32),
            vm((NQ, GL, home), BF16), vm((NQ, GL, home), BF16), vm((GL, home), BF16),
            vm((NQ, 1, home), jnp.int32), vm((NQ, 1, home), jnp.int32), vm((1, home), jnp.int32),
            vm((NQ, cols, home), F32), vm((2, cols, home), F32), vm((2, cols, home), F32),
            vm((cols, home), F32), vm((cols, home), F32),
            vm((NQ, cols, users), BF16), vm((4, 1, home), F32), vm((NQ, 1, home), F32),
            pltpu.SemaphoreType.DMA((NQ + 3,)),
            pltpu.SemaphoreType.DMA((NUM_SEMS,)), pltpu.SemaphoreType.DMA((NUM_SEMS,)),
        ]
        vspec = pl.BlockSpec(memory_space=pltpu.VMEM)
        out_u, out_i, loss = pl.pallas_call(
            kernel,
            out_shape=[
                jax.ShapeDtypeStruct((cols, own_users), BF16),
                jax.ShapeDtypeStruct((cols, quarter), BF16),
                jax.ShapeDtypeStruct((NQ, 1, home), F32)],
            in_specs=[pl.BlockSpec(memory_space=pl.ANY)] * 4,
            out_specs=[vspec, vspec, vspec],
            scratch_shapes=scratch,
            compiler_params=pltpu.CompilerParams(
                collective_id=0, has_side_effects=True, vmem_limit_bytes=60 * 1024 * 1024),
        )(mask_blk, user_sh.T, item_sh.T, triples.T)
        out_u, out_i, loss = pl.pallas_call(
            emit,
            out_shape=[
                jax.ShapeDtypeStruct((cols, own_users), BF16),
                jax.ShapeDtypeStruct((cols, quarter), BF16),
                jax.ShapeDtypeStruct((NQ, 1, home), F32)],
            in_specs=[vspec] * 3, out_specs=[vspec] * 3,
        )(out_u, out_i, loss)
        return out_u.T, out_i.T, loss.reshape(-1)

    return jax.shard_map(
        local_fn, mesh=mesh,
        in_specs=(P("row", "col"), P(("row", "col"), "emb"), P(("col", "row"), "emb"), P()),
        out_specs=(P(("row", "col"), "emb"), P(("col", "row"), "emb"), P()),
        check_vma=False)
```

```python
import functools

import jax
import jax.numpy as jnp
from jax import lax
from jax.experimental import pallas as pl
from jax.experimental.pallas import tpu as pltpu
from jax.sharding import PartitionSpec as P

NUM_LAYERS = 3
MESH = pl.DeviceIdType.MESH
F32 = jnp.float32
BF16 = jnp.bfloat16

NQ = 4
NM = 2
NS = 4
LB = 256
GL = 256


class Copies:
    def __init__(self, send_sems, recv_sems):
        self.send_sems, self.recv_sems, self.started = send_sems, recv_sems, []

    def send(self, src, dst, device):
        k = len(self.started)
        copy = pltpu.make_async_remote_copy(
            src_ref=src, dst_ref=dst, send_sem=self.send_sems.at[k],
            recv_sem=self.recv_sems.at[k], device_id=device, device_id_type=MESH)
        copy.start()
        self.started.append(copy)
        return copy

    def drain(self):
        for copy in self.started:
            copy.wait_send()


NUM_SEMS = 120


class Phase:
    def __init__(self):
        self.current = None

    def __call__(self, name):
        if self.current is not None:
            self.current.__exit__(None, None, None)
        self.current = None
        if name:
            self.current = jax.named_scope(name)
            self.current.__enter__()


def kernel(mask_hbm, u0_hbm, i0_hbm, trip_hbm, outu_ref, outi_ref, loss_ref,
           maskv, maskb, adj, csum, crd, crx, cch, invi, racc, rsum, rrecv, invu, trip_ref,
           upan, upart, urecv, ipan, ipart, ird, irx, isum,
           ohp, ohn, ohu, hip, hin, hiu, gpart, gsum, grd, grx, gry, eu, zbuf, lossb,
           in_sems, send_sems, recv_sems):
    users = maskv.shape[1]
    quarter = maskv.shape[2]
    own_users = u0_hbm.shape[1]
    sc = quarter // NS
    home = gpart.shape[2]
    hh = home // 2

    z = lax.axis_index("emb")
    y = lax.axis_index("col")
    r = lax.axis_index("row")
    x = r // 2
    c = r % 2
    nz = 4

    def rel(m):
        xx = x if m < 2 else 1 - x
        cc = c if m % 2 == 0 else 1 - c
        return 2 * xx + cc

    dev_d = (z, y, rel(1))
    dev_x = (z, y, rel(2))
    dev_xd = (z, y, rel(3))
    dev_y = (z, 1 - y, r)
    dev_z = [((z + k) % nz, y, r) for k in (1, 2, 3)]

    cp = Copies(send_sems, recv_sems)
    phase = Phase()
    phase("start")

    def load(src, dst, k):
        copy = pltpu.make_async_copy(src, dst, in_sems.at[k])
        copy.start()
        return copy

    y_off = pl.multiple_of(y * own_users, own_users)
    mask_copies = {}
    mh = quarter // NM
    for m in (3, 2, 1, 0):
        for h in range(NM):
            off = pl.multiple_of(rel(m) * quarter + h * mh, mh)
            mask_copies[m, h] = load(
                mask_hbm.at[:, pl.ds(off, mh)], maskv.at[m, :, pl.ds(h * mh, mh)], m * NM + h)
        if m == 3:
            u0_in = load(u0_hbm, upan.at[0, :, pl.ds(y_off, own_users)], NQ * NM)
            i0_in = load(i0_hbm, ipan.at[0, 0], NQ * NM + 1)
            trip_in = load(trip_hbm, trip_ref, NQ * NM + 2)

    barrier = pltpu.get_barrier_semaphore()
    for dev in (dev_d, dev_x, dev_xd, dev_y, *dev_z):
        pl.semaphore_signal(barrier, inc=1, device_id=dev, device_id_type=MESH)

    racc[...] = jnp.zeros_like(racc)

    def sums(m):
        for h in range(NM):
            mask_copies[m, h].wait()

            def body(j, carry):
                off = pl.multiple_of(h * mh + j * LB, LB)
                tile = h * (mh // 128) + j * (LB // 128)
                part = None
                for i in range(users // 16):
                    rows = pl.ds(16 * i, 16)
                    blk = maskv[m, rows, pl.ds(off, LB)]
                    ones = blk.astype(F32).astype(BF16)
                    for g in range(LB // 128):
                        maskb[m, tile + g, rows, :] = ones[:, 128 * g:128 * (g + 1)]
                    two = blk[:8] + blk[8:]
                    part = two if part is None else part + two
                    row = blk[:, :128]
                    for g in range(1, LB // 128):
                        row = row + blk[:, 128 * g:128 * (g + 1)]
                    racc[rows, :] += row
                csum[m, :, pl.ds(off, LB)] = jnp.sum(part.astype(F32), axis=0, keepdims=True)
                return carry
            lax.fori_loop(0, mh // LB, body, 0)

    def one_hot(lanes):
        hit = lax.broadcasted_iota(jnp.int32, (GL, 128), 0) == lanes
        return jnp.where(hit, 1.0, 0.0).astype(BF16)

    def hot_block(oh, t):
        n = LB // 128
        return jnp.concatenate([oh[t * n + i] for i in range(n)], axis=1)

    def one_hots(m):
        base = pl.multiple_of(rel(m) * home, home)
        for row, oh, hi in ((1, ohp, hip), (2, ohn, hin)):
            ids = trip_ref[pl.ds(row, 1), pl.ds(base, home)]
            owned = ids // quarter == y * NQ + r
            hi[m] = (ids % quarter) // GL
            low = jnp.where(owned, ids % GL, -1)
            for t in range(home // 128):
                oh[m, t] = one_hot(low[:, t * 128:(t + 1) * 128])

    def user_one_hots():
        base = pl.multiple_of(r * home, home)
        uids = trip_ref[pl.ds(0, 1), pl.ds(base, home)]
        hiu[...] = uids // users
        low = uids % users
        for t in range(home // 128):
            ohu[t] = one_hot(low[:, t * 128:(t + 1) * 128])

    csum_d, csum_x = {}, {}

    def chip_sums(m):
        csum_d[m].wait_recv()
        cch[m] = csum[m] + crd[m]
        csum_x[m ^ 2] = cp.send(cch.at[m], crx.at[m ^ 2], dev_x)

    def send_sums(m):
        csum_d[m ^ 1] = cp.send(csum.at[m], crd.at[m ^ 1], dev_d)

    phase("sums32")
    sums(3)
    sums(2)
    u0_in.wait()
    i0_in.wait()
    trip_in.wait()
    phase("barrier")
    pl.semaphore_wait(barrier, 7)
    phase("sums10")
    send_sums(3)
    send_sums(2)
    u0_y = cp.send(upan.at[0, :, pl.ds(y_off, own_users)], upan.at[0, :, pl.ds(y_off, own_users)], dev_y)
    i0_d = cp.send(ipan.at[0, 0], ipan.at[0, 1], dev_d)
    sums(1)
    send_sums(1)
    chip_sums(3)
    chip_sums(2)
    sums(0)
    send_sums(0)
    phase("rows")
    rows = jnp.transpose(racc[...].astype(F32), (1, 0))
    rsum[...] = jnp.sum(rows, axis=0, keepdims=True)
    rs_y = cp.send(rsum, rrecv, dev_y)
    chip_sums(1)
    one_hots(3)
    phase("chip0")
    chip_sums(0)
    i0_x = cp.send(ipan.at[0, 0], ipan.at[0, 2], dev_x)
    phase("onehots")
    one_hots(2)
    one_hots(1)
    phase("rs_wait")
    u0_y.wait_recv()
    rs_y.wait_recv()
    inv_row = lax.rsqrt(jnp.maximum(rsum[...] + rrecv[...], 1.0))
    invu[...] = jnp.transpose(jnp.broadcast_to(inv_row, (128, users)), (1, 0))
    phase("cx_wait")
    for m in (3, 2, 1, 0):
        csum_x[m].wait_recv()
        invi[m] = lax.rsqrt(jnp.maximum(cch[m] + crx[m], 1.0))

    def build(m, s):
        for g in range(sc // 128):
            lanes = slice(s * sc + 128 * g, s * sc + 128 * (g + 1))
            scale = (invu[...] * invi[m, :, lanes]).astype(BF16)
            tile = s * (sc // 128) + g
            adj[m, tile] = scale * maskb[m, tile]

    def block(m, s, n, rows):
        first, count = s * (sc // 128), n * (sc // 128)
        return jnp.concatenate([adj[m, first + t, rows, :] for t in range(count)], axis=1)

    def item_piece(k, m, s):
        sl = pl.ds(s * sc, sc)
        ipart[k, m, :, sl] = jnp.dot(upan[k], block(m, s, 1, slice(0, users)), preferred_element_type=F32)

    def user_piece(k, m, s, n, acc=None):
        out = []
        for h in (0, 1):
            part = lax.dot_general(
                ipan[k, m, :, s * sc:(s + n) * sc], block(m, s, n, slice(h * own_users, (h + 1) * own_users)),
                (((1,), (1,)), ((), ())), preferred_element_type=F32)
            out.append(part if acc is None else acc[h] + part)
        return out

    def to_core(k, m, s):
        sl = pl.ds(s * sc, sc)
        return cp.send(ipart.at[k, m, :, sl], ird.at[k, (m ^ 1) // 2, :, sl], dev_d)

    def to_x(k, s, got):
        sl = pl.ds(s * sc, sc)
        got.wait_recv()
        isum[k, :, sl] = ipart[k, 2, :, sl] + ird[k, 1, :, sl]
        return cp.send(isum.at[k, :, sl], irx.at[k, :, sl], dev_x)

    def own_piece(k, s, got_d, got_x):
        sl = pl.ds(s * sc, sc)
        got_d.wait_recv()
        got_x.wait_recv()
        total = (ipart[k, 0, :, sl] + ird[k, 0, :, sl]) + irx[k, :, sl]
        ipan[k + 1, 0, :, sl] = total.astype(BF16)

    def gather_piece(k, s):
        sl = pl.ds(s * sc, sc)
        gx = cp.send(ipan.at[k, 0, :, sl], ipan.at[k, 2, :, sl], dev_x)
        gd = cp.send(ipan.at[k, 0, :, sl], ipan.at[k, 1, :, sl], dev_d)
        return gx, gd

    def forward_piece(k, s, gx):
        sl = pl.ds(s * sc, sc)
        gx.wait_recv()
        return cp.send(ipan.at[k, 2, :, sl], ipan.at[k, 3, :, sl], dev_d)

    def send_user(k, acc):
        for h in (0, 1):
            upart[k, :, h * own_users:(h + 1) * own_users] = acc[h]
        return cp.send(upart.at[k], urecv.at[k], dev_y)

    def take_user(k, got):
        got.wait_recv()
        upan[k + 1] = (upart[k] + urecv[k]).astype(BF16)

    d, xs = [{}, {}, {}], [{}, {}, {}]
    g, f = {}, {}

    def own_gather(k, s):
        own_piece(k, s, d[k][0, s], xs[k][s])
        g[k + 1, s] = gather_piece(k + 1, s)

    def core_send(k, m, s):
        d[k][m ^ 1, s] = to_core(k, m, s)

    def x_send(k, s):
        xs[k][s] = to_x(k, s, d[k][2, s])

    def forward(k, s):
        f[k, s] = forward_piece(k, s, g[k, s][0])

    phase("build32")
    build(3, 0)
    for s in range(NS):
        item_piece(0, 3, s)
        build(2, s)
        core_send(0, 3, s)
        item_piece(0, 2, s)
        if s + 1 < NS:
            build(3, s + 1)
        if s:
            x_send(0, s - 1)
    phase("build10")
    build(1, 0)
    x_send(0, NS - 1)
    for s in range(NS):
        item_piece(0, 1, s)
        build(0, s)
        core_send(0, 1, s)
        item_piece(0, 0, s)
        if s + 1 < NS:
            build(1, s + 1)
    phase("upart0")
    i0_d.wait_recv()
    acc = user_piece(0, 1, 0, NS, user_piece(0, 0, 0, NS))
    i0_x.wait_recv()
    i0_f = cp.send(ipan.at[0, 2], ipan.at[0, 3], dev_d)
    phase("own1_0")
    own_gather(0, 0)
    phase("upart0b")
    acc = user_piece(0, 2, 0, NS, acc)
    i0_f.wait_recv()
    acc = user_piece(0, 3, 0, NS, acc)
    u1 = send_user(0, acc)
    phase("own1_1")
    own_gather(0, 1)
    one_hots(0)
    phase("own1_2")
    own_gather(0, 2)
    user_one_hots()
    phase("own1_3")
    own_gather(0, 3)
    phase("u1_wait")
    take_user(0, u1)
    phase("items2_32")

    def items_32(k):
        item_piece(k, 3, 0)
        item_piece(k, 3, 1)
        item_piece(k, 3, 2)
        core_send(k, 3, 0)
        core_send(k, 3, 1)
        item_piece(k, 3, 3)
        item_piece(k, 2, 0)
        core_send(k, 3, 2)
        core_send(k, 3, 3)
        item_piece(k, 2, 1)
        item_piece(k, 2, 2)
        item_piece(k, 2, 3)

    items_32(1)
    phase("fwd1_0")
    forward(1, 0)
    phase("items2_10")
    item_piece(1, 1, 0)
    item_piece(1, 1, 1)
    x_send(1, 0)
    x_send(1, 1)
    item_piece(1, 1, 2)
    item_piece(1, 1, 3)
    x_send(1, 2)
    x_send(1, 3)
    phase("fwd1_1")
    forward(1, 1)
    item_piece(1, 0, 0)
    for s in range(NS):
        core_send(1, 1, s)
    item_piece(1, 0, 1)
    item_piece(1, 0, 2)
    item_piece(1, 0, 3)
    phase("upart1_0")
    acc = user_piece(1, 0, 0, NS)
    phase("fwd1_2")
    forward(1, 2)
    for s in range(NS):
        g[1, s][1].wait_recv()
    acc = user_piece(1, 1, 0, NS, acc)
    phase("fwd1_3")
    forward(1, 3)
    acc = user_piece(1, 2, 0, NS, acc)
    f[1, 0].wait_recv()
    f[1, 1].wait_recv()
    acc = user_piece(1, 3, 0, 2, acc)
    phase("f1_wait")
    f[1, 2].wait_recv()
    f[1, 3].wait_recv()
    acc = user_piece(1, 3, 2, 2, acc)
    u2 = send_user(1, acc)
    phase("own2_01")
    own_gather(1, 0)
    own_gather(1, 1)
    phase("u2_wait")
    take_user(1, u2)
    phase("items3_32")
    items_32(2)
    phase("items3_10")
    item_piece(2, 1, 0)
    item_piece(2, 1, 1)
    x_send(2, 0)
    x_send(2, 1)
    item_piece(2, 1, 2)
    item_piece(2, 1, 3)
    x_send(2, 2)
    x_send(2, 3)
    item_piece(2, 0, 0)
    for s in range(NS):
        core_send(2, 1, s)
    item_piece(2, 0, 1)
    item_piece(2, 0, 2)
    item_piece(2, 0, 3)
    phase("own2_23")
    own_gather(1, 2)
    own_gather(1, 3)
    phase("upart2_01")
    acc = user_piece(2, 0, 0, NS)
    for s in range(NS):
        g[2, s][1].wait_recv()
    acc = user_piece(2, 1, 0, NS, acc)
    phase("fwd2_01")
    forward(2, 0)
    forward(2, 1)
    acc = user_piece(2, 2, 0, 2, acc)
    f[2, 0].wait_recv()
    f[2, 1].wait_recv()
    acc = user_piece(2, 3, 0, 2, acc)

    def pick(tab, oh, hi, n):
        got = jnp.dot(tab, oh, preferred_element_type=F32)
        rows16 = got.shape[0] // n
        out = jnp.where(hi == 0, got[:rows16], 0.0)
        for g0 in range(1, n):
            out = out + jnp.where(hi == g0, got[g0 * rows16:(g0 + 1) * rows16], 0.0)
        return out

    def final_piece(s):
        own_piece(2, s, d[2][0, s], xs[2][s])
        sl = pl.ds(s * sc, sc)
        tot = ((ipan[0, 0, :, sl].astype(F32) + ipan[1, 0, :, sl].astype(F32))
               + ipan[2, 0, :, sl].astype(F32)) + ipan[3, 0, :, sl].astype(F32)
        outi_ref[:, sl] = (tot * (1.0 / (NUM_LAYERS + 1))).astype(BF16)

    half = [pl.ds(0, hh), pl.ds(hh, hh)]

    def differences(m, h):
        for t in range(h * (hh // LB), (h + 1) * (hh // LB)):
            sl = slice(t * LB, (t + 1) * LB)
            pos = pick(table, hot_block(ohp.at[m], t), hip[m, :, sl], quarter // GL)
            neg = pick(table, hot_block(ohn.at[m], t), hin[m, :, sl], quarter // GL)
            gpart[m, :, sl] = pos - neg

    phase("own3")
    for s in range(NS):
        final_piece(s)
    table = jnp.concatenate(
        [outi_ref[:, g0 * GL:(g0 + 1) * GL] for g0 in range(quarter // GL)], axis=0)
    gd3, gd1, gx, gy = {}, {}, {}, {}
    phase("diff3")
    differences(3, 0)
    gd3[0] = cp.send(gpart.at[3, :, half[0]], grd.at[1, :, half[0]], dev_d)
    differences(3, 1)
    gd3[1] = cp.send(gpart.at[3, :, half[1]], grd.at[1, :, half[1]], dev_d)
    differences(2, 0)
    differences(2, 1)
    phase("gd3_wait")
    for h in (0, 1):
        gd3[h].wait_recv()
        gsum[1, :, half[h]] = gpart[2, :, half[h]] + grd[1, :, half[h]]
        gx[h] = cp.send(gsum.at[1, :, half[h]], grx.at[:, half[h]], dev_x)
    phase("diff1")
    differences(1, 0)
    differences(1, 1)
    for h in (0, 1):
        gd1[h] = cp.send(gpart.at[1, :, half[h]], grd.at[0, :, half[h]], dev_d)
    differences(0, 0)
    differences(0, 1)
    phase("fwd2_23")
    forward(2, 2)
    forward(2, 3)
    acc = user_piece(2, 2, 2, 2, acc)
    phase("f2_wait")
    f[2, 2].wait_recv()
    f[2, 3].wait_recv()
    acc = user_piece(2, 3, 2, 2, acc)
    u3 = send_user(2, acc)
    phase("g_wait")
    for h in (0, 1):
        gd1[h].wait_recv()
        gx[h].wait_recv()
        gsum[0, :, half[h]] = (gpart[0, :, half[h]] + grd[0, :, half[h]]) + grx[:, half[h]]
        gy[h] = cp.send(gsum.at[0, :, half[h]], gry.at[:, half[h]], dev_y)

    phase("u3_wait")
    take_user(2, u3)
    phase("finalu")
    ut = ((upan[0].astype(F32) + upan[1].astype(F32)) + upan[2].astype(F32)) + upan[3].astype(F32)
    eu[0] = (ut * (1.0 / (NUM_LAYERS + 1))).astype(BF16)
    e1 = cp.send(eu.at[0], eu.at[1], dev_d)
    e2 = cp.send(eu.at[0], eu.at[2], dev_x)
    e3 = cp.send(eu.at[0], eu.at[3], dev_xd)
    outu_ref[...] = eu[0, :, pl.ds(y_off, own_users)]

    phase("e_wait")
    e1.wait_recv()
    e2.wait_recv()
    e3.wait_recv()
    phase("picku")
    utab = jnp.concatenate([eu[m] for m in range(NQ)], axis=0)
    blk_id = hiu[...]
    place = jnp.where(blk_id // 2 == x, 0, 2) + jnp.where(blk_id % 2 == c, 0, 1)
    picked = []
    for t in range(home // LB):
        picked.append(pick(utab, hot_block(ohu, t), place[:, t * LB:(t + 1) * LB], NQ))
    phase("gy_wait")
    gy[0].wait_recv()
    gy[1].wait_recv()
    phase("dot")
    for t in range(home // LB):
        sl = slice(t * LB, (t + 1) * LB)
        diff = gsum[0, :, sl] + gry[:, sl]
        zbuf[z, :, sl] = jnp.sum(picked[t] * diff, axis=0, keepdims=True)
    zc = [cp.send(zbuf.at[z], zbuf.at[z], dev) for dev in dev_z]
    phase("z_wait")
    for copy in zc:
        copy.wait_recv()
    phase("loss")
    score = ((zbuf[0] + zbuf[1]) + zbuf[2]) + zbuf[3]
    neg = -score
    lossb[r] = jnp.maximum(neg, 0.0) + jnp.log1p(jnp.exp(-jnp.abs(neg)))
    lc = [cp.send(lossb.at[r], lossb.at[r], dev) for dev in (dev_d, dev_x, dev_xd)]
    phase("loss_wait")
    for copy in lc:
        copy.wait_recv()
    phase("end")
    loss_ref[...] = lossb[...]
    phase("drain")
    cp.drain()
    phase(None)


def emit(u_in, i_in, l_in, u_out, i_out, l_out):
    u_out[...] = u_in[...]
    i_out[...] = i_in[...]
    l_out[...] = l_in[...]


def solution(mesh):
    def local_fn(mask_blk, user_sh, item_sh, triples):
        users, items = mask_blk.shape
        cols, own_users = user_sh.shape[1], user_sh.shape[0]
        quarter = items // NQ
        home = triples.shape[0] // NQ
        vm = pltpu.VMEM
        nl = NUM_LAYERS
        scratch = [
            vm((NQ, users, quarter), jnp.int32), vm((NQ, quarter // 128, users, 128), BF16),
            vm((NQ, quarter // 128, users, 128), BF16),
            vm((NQ, 1, quarter), F32), vm((NQ, 1, quarter), F32), vm((NQ, 1, quarter), F32),
            vm((NQ, 1, quarter), F32), vm((NQ, 1, quarter), F32),
            vm((users, 128), jnp.int32), vm((1, users), F32), vm((1, users), F32), vm((users, 128), F32),
            vm(triples.shape[::-1], jnp.int32),
            vm((nl + 1, cols, users), BF16), vm((nl, cols, users), F32), vm((nl, cols, users), F32),
            vm((nl + 1, NQ, cols, quarter), BF16), vm((nl, NQ, cols, quarter), F32),
            vm((nl, 2, cols, quarter), F32), vm((nl, cols, quarter), F32), vm((nl, cols, quarter), F32),
            vm((NQ, home // 128, GL, 128), BF16), vm((NQ, home // 128, GL, 128), BF16),
            vm((home // 128, GL, 128), BF16),
            vm((NQ, 1, home), jnp.int32), vm((NQ, 1, home), jnp.int32), vm((1, home), jnp.int32),
            vm((NQ, cols, home), F32), vm((2, cols, home), F32), vm((2, cols, home), F32),
            vm((cols, home), F32), vm((cols, home), F32),
            vm((NQ, cols, users), BF16), vm((4, 1, home), F32), vm((NQ, 1, home), F32),
            pltpu.SemaphoreType.DMA((NQ * NM + 3,)),
            pltpu.SemaphoreType.DMA((NUM_SEMS,)), pltpu.SemaphoreType.DMA((NUM_SEMS,)),
        ]
        vspec = pl.BlockSpec(memory_space=pltpu.VMEM)
        out_u, out_i, loss = pl.pallas_call(
            kernel,
            out_shape=[
                jax.ShapeDtypeStruct((cols, own_users), BF16),
                jax.ShapeDtypeStruct((cols, quarter), BF16),
                jax.ShapeDtypeStruct((NQ, 1, home), F32)],
            in_specs=[pl.BlockSpec(memory_space=pl.ANY)] * 4,
            out_specs=[vspec, vspec, vspec],
            scratch_shapes=scratch,
            compiler_params=pltpu.CompilerParams(
                collective_id=0, has_side_effects=True, vmem_limit_bytes=60 * 1024 * 1024),
        )(mask_blk, user_sh.T, item_sh.T, triples.T)
        out_u, out_i, loss = pl.pallas_call(
            emit,
            out_shape=[
                jax.ShapeDtypeStruct((cols, own_users), BF16),
                jax.ShapeDtypeStruct((cols, quarter), BF16),
                jax.ShapeDtypeStruct((NQ, 1, home), F32)],
            in_specs=[vspec] * 3, out_specs=[vspec] * 3,
        )(out_u, out_i, loss)
        return out_u.T, out_i.T, loss.reshape(-1)

    return jax.shard_map(
        local_fn, mesh=mesh,
        in_specs=(P("row", "col"), P(("row", "col"), "emb"), P(("col", "row"), "emb"), P()),
        out_specs=(P(("row", "col"), "emb"), P(("col", "row"), "emb"), P()),
        check_vma=False)
```

```python
import functools

import jax
import jax.numpy as jnp
from jax import lax
from jax.experimental import pallas as pl
from jax.experimental.pallas import tpu as pltpu
from jax.sharding import PartitionSpec as P

NUM_LAYERS = 3
MESH = pl.DeviceIdType.MESH
F32 = jnp.float32
BF16 = jnp.bfloat16

NQ = 4
NM = 2
NS = 4
LB = 256
GL = 256
LANES = 128
ROWS = 16


class Copies:
    def __init__(self, send_sems, recv_sems):
        self.send_sems, self.recv_sems, self.started = send_sems, recv_sems, []

    def send(self, src, dst, device):
        k = len(self.started)
        copy = pltpu.make_async_remote_copy(
            src_ref=src, dst_ref=dst, send_sem=self.send_sems.at[k],
            recv_sem=self.recv_sems.at[k], device_id=device, device_id_type=MESH)
        copy.start()
        self.started.append(copy)
        return copy

    def drain(self):
        for copy in self.started:
            copy.wait_send()


VMEM_LIMIT = 60 * 2 ** 20
NUM_SEMS = 86
NUM_LOADS = NQ * NM + NS + 2


class Phase:
    def __init__(self):
        self.current = None

    def __call__(self, name):
        if self.current is not None:
            self.current.__exit__(None, None, None)
        self.current = None
        if name:
            self.current = jax.named_scope(name)
            self.current.__enter__()


def kernel(mask_hbm, u0_hbm, i0_hbm, trip_hbm, outu_ref, outi_ref, loss_ref,
           maskv, maskb, adj, csum, crd, crx, cch, invi, racc, rsum, rrecv, invu, trip_ref,
           upan, upart, urecv, ipan, ipart, ird, irx, isum,
           ohp, ohn, ohu, hip, hin, hiu, gpart, gsum, grd, grx, gry, eu, zbuf,
           in_sems, send_sems, recv_sems):
    users, quarter = maskv.shape[1:]
    own_users = u0_hbm.shape[1]
    sc = ipan.shape[-1]
    home = gpart.shape[-1]
    hh = home // 2
    mh = quarter // NM
    pieces, halves = range(NS), range(2)
    own, core, other, both = range(NQ)
    order = (both, other, core, own)

    z, y, r = lax.axis_index("emb"), lax.axis_index("col"), lax.axis_index("row")
    x, c = r // 2, r % 2
    nz = zbuf.shape[0]

    def rel(m):
        xx = x if m in (own, core) else 1 - x
        cc = c if m in (own, other) else 1 - c
        return 2 * xx + cc

    dev_d, dev_x, dev_xd = [(z, y, rel(m)) for m in (core, other, both)]
    dev_y = (z, 1 - y, r)
    score_devs = [((z + k) % nz, y, rel(m)) for k in range(nz) for m in range(NQ) if k or m]

    cp = Copies(send_sems, recv_sems)
    phase = Phase()
    phase("start")
    loads = []

    def load(src, dst):
        copy = pltpu.make_async_copy(src, dst, in_sems.at[len(loads)])
        copy.start()
        loads.append(copy)
        return copy

    y_off = pl.multiple_of(y * own_users, own_users)
    own_u = pl.ds(y_off, own_users)
    mask_copies, small = {}, []
    for m in order:
        for h in range(NM):
            off = pl.multiple_of(rel(m) * quarter + h * mh, mh)
            mask_copies[m, h] = load(mask_hbm.at[:, pl.ds(off, mh)], maskv.at[m, :, pl.ds(h * mh, mh)])
        if m == both:
            small.append(load(u0_hbm, upan.at[0, :, own_u]))
            small += [load(i0_hbm.at[:, pl.ds(s * sc, sc)], ipan.at[0, own, s]) for s in pieces]
            small.append(load(trip_hbm, trip_ref))

    barrier = pltpu.get_barrier_semaphore()
    for dev in (dev_y, *score_devs):
        pl.semaphore_signal(barrier, inc=1, device_id=dev, device_id_type=MESH)

    racc[...] = jnp.zeros_like(racc)

    def sums(m):
        for h in range(NM):
            mask_copies[m, h].wait()

            def body(j, carry):
                off = pl.multiple_of(h * mh + j * LB, LB)
                tile = h * (mh // LANES) + j * (LB // LANES)
                part = None
                for i in range(users // ROWS):
                    rows = pl.ds(ROWS * i, ROWS)
                    blk = maskv[m, rows, pl.ds(off, LB)]
                    ones = blk.astype(F32).astype(BF16)
                    row = None
                    for g in range(LB // LANES):
                        lanes = slice(LANES * g, LANES * (g + 1))
                        maskb[m, tile + g, rows, :] = ones[:, lanes]
                        row = blk[:, lanes] if row is None else row + blk[:, lanes]
                    racc[rows, :] += row
                    two = blk[:ROWS // 2] + blk[ROWS // 2:]
                    part = two if part is None else part + two
                csum[m, :, pl.ds(off, LB)] = jnp.sum(part.astype(F32), axis=0, keepdims=True)
                return carry
            lax.fori_loop(0, mh // LB, body, 0)

    def one_hot(lanes):
        hit = lax.broadcasted_iota(jnp.int32, (GL, LANES), 0) == lanes
        return jnp.where(hit, 1.0, 0.0).astype(BF16)

    def hot_block(oh, t):
        n = LB // LANES
        return jnp.concatenate([oh[t * n + i] for i in range(n)], axis=1)

    def one_hots(m):
        base = pl.multiple_of(rel(m) * home, home)
        for row, oh, hi in ((1, ohp, hip), (2, ohn, hin)):
            ids = trip_ref[pl.ds(row, 1), pl.ds(base, home)]
            owned = ids // quarter == y * NQ + r
            hi[m] = (ids % quarter) // GL
            low = jnp.where(owned, ids % GL, -1)
            for t in range(home // LANES):
                oh[m, t] = one_hot(low[:, t * LANES:(t + 1) * LANES])

    def user_one_hots():
        base = pl.multiple_of(r * home, home)
        uids = trip_ref[pl.ds(0, 1), pl.ds(base, home)]
        hiu[...] = uids // users
        low = uids % users
        for t in range(home // LANES):
            ohu[t] = one_hot(low[:, t * LANES:(t + 1) * LANES])

    csum_d, csum_x = {}, {}

    def chip_sums(m):
        csum_d[m].wait_recv()
        cch[m] = csum[m] + crd[m]
        csum_x[m ^ other] = cp.send(cch.at[m], crx.at[m ^ other], dev_x)

    def send_sums(m):
        csum_d[m ^ core] = cp.send(csum.at[m], crd.at[m ^ core], dev_d)

    phase("sums32")
    sums(both)
    sums(other)
    for copy in small:
        copy.wait()
    phase("barrier")
    pl.semaphore_wait(barrier, 1 + len(score_devs))
    phase("sums10")
    send_sums(both)
    send_sums(other)
    u0_y = cp.send(upan.at[0, :, own_u], upan.at[0, :, own_u], dev_y)
    i0_d = cp.send(ipan.at[0, own], ipan.at[0, core], dev_d)
    sums(core)
    send_sums(core)
    chip_sums(both)
    chip_sums(other)
    sums(own)
    send_sums(own)
    phase("rows")
    rows = jnp.transpose(racc[...].astype(F32), (1, 0))
    rsum[...] = jnp.sum(rows, axis=0, keepdims=True)
    rs_y = cp.send(rsum, rrecv, dev_y)
    chip_sums(core)
    one_hots(both)
    phase("chip0")
    chip_sums(own)
    i0_x = cp.send(ipan.at[0, own], ipan.at[0, other], dev_x)
    phase("onehots")
    one_hots(other)
    one_hots(core)
    phase("rs_wait")
    u0_y.wait_recv()
    rs_y.wait_recv()
    inv_row = lax.rsqrt(jnp.maximum(rsum[...] + rrecv[...], 1.0))
    invu[...] = jnp.transpose(jnp.broadcast_to(inv_row, (LANES, users)), (1, 0))
    phase("cx_wait")
    for m in order:
        csum_x[m].wait_recv()
        invi[m] = lax.rsqrt(jnp.maximum(cch[m] + crx[m], 1.0))

    tiles = sc // LANES

    def build(m, s):
        for tile in range(s * tiles, (s + 1) * tiles):
            scale = (invu[...] * invi[m, :, tile * LANES:(tile + 1) * LANES]).astype(BF16)
            adj[m, tile] = scale * maskb[m, tile]

    def block(m, s, n, rows):
        return jnp.concatenate([adj[m, t, rows, :] for t in range(s * tiles, (s + n) * tiles)], axis=1)

    def items(k, m, some=pieces):
        for s in some:
            ipart[k, m, s] = jnp.dot(upan[k], block(m, s, 1, slice(0, users)), preferred_element_type=F32)

    def user_part(k, m, acc=None, s=0, n=NS):
        table = jnp.concatenate([ipan[k, m, s + i] for i in range(n)], axis=1)
        out = []
        for h in halves:
            part = lax.dot_general(
                table, block(m, s, n, slice(h * own_users, (h + 1) * own_users)),
                (((1,), (1,)), ((), ())), preferred_element_type=F32)
            out.append(part if acc is None else acc[h] + part)
        return out

    d, xs, g, gd, f = {}, {}, {}, {}, {}

    def core_send(k, s):
        d[k, s] = cp.send(ipart.at[k, both, s], ird.at[k, 1, s], dev_d)

    def core_send_own(k):
        d[k] = cp.send(ipart.at[k, core], ird.at[k, 0], dev_d)

    def x_send(k, s):
        d[k, s].wait_recv()
        isum[k, s] = ipart[k, other, s] + ird[k, 1, s]
        xs[k, s] = cp.send(isum.at[k, s], irx.at[k, s], dev_x)

    def own_piece(k, s):
        if s == 0:
            d[k].wait_recv()
        xs[k, s].wait_recv()
        total = (ipart[k, own, s] + ird[k, 0, s]) + irx[k, s]
        ipan[k + 1, own, s] = total.astype(BF16)

    def own_gather(k, s):
        own_piece(k, s)
        g[k + 1, s] = cp.send(ipan.at[k + 1, own, s], ipan.at[k + 1, other, s], dev_x)
        if s == NS - 1:
            gd[k + 1] = cp.send(ipan.at[k + 1, own], ipan.at[k + 1, core], dev_d)

    def forward(k, s):
        g[k, s].wait_recv()
        f[k, s] = cp.send(ipan.at[k, other, s], ipan.at[k, both, s], dev_d)

    def send_user(k, acc):
        for h in halves:
            upart[k, :, h * own_users:(h + 1) * own_users] = acc[h]
        return cp.send(upart.at[k], urecv.at[k], dev_y)

    def take_user(k, got):
        got.wait_recv()
        upan[k + 1] = (upart[k] + urecv[k]).astype(BF16)

    last = NS - 1
    phase("build32")
    for s in pieces:
        build(both, s)
        items(0, both, [s])
        build(other, s)
        core_send(0, s)
        items(0, other, [s])
        if s > 1:
            x_send(0, s - 2)
    phase("build10")
    for s in pieces:
        build(core, s)
        if s in (1, last):
            x_send(0, NS - 2 + s // 2)
    for s in pieces:
        build(own, s)
    phase("upart0")
    i0_d.wait_recv()
    acc = user_part(0, core, user_part(0, own))
    i0_x.wait_recv()
    i0_f = cp.send(ipan.at[0, other], ipan.at[0, both], dev_d)
    acc = user_part(0, other, acc)
    phase("upart0b")
    i0_f.wait_recv()
    acc = user_part(0, both, acc)
    u1 = send_user(0, acc)
    phase("items1_10")
    items(0, core)
    core_send_own(0)
    items(0, own)
    one_hots(own)
    user_one_hots()
    for s in range(last):
        phase(f"own1_{s}")
        own_gather(0, s)
    phase("u1_wait")
    take_user(0, u1)

    def items_x(k):
        items(k, both)
        items(k, other, [0])
        for s in pieces:
            core_send(k, s)
        items(k, other, range(1, NS))

    phase("items2_32")
    items_x(1)
    phase("own1_last")
    own_gather(0, last)
    phase("x2")
    for s in pieces:
        x_send(1, s)
    phase("items2_10")
    items(1, core)
    core_send_own(1)
    items(1, own)
    phase("fwd1_0")
    forward(1, 0)
    acc = user_part(1, own)
    phase("fwd1_1")
    forward(1, 1)
    gd[1].wait_recv()
    acc = user_part(1, core, acc)
    phase("fwd1_2")
    forward(1, 2)
    acc = user_part(1, other, acc, 0, last)
    phase("fwd1_3")
    forward(1, last)
    acc = user_part(1, other, acc, last, 1)
    for s in range(last):
        f[1, s].wait_recv()
    acc = user_part(1, both, acc, 0, last)
    phase("f1_wait")
    f[1, last].wait_recv()
    acc = user_part(1, both, acc, last, 1)
    u2 = send_user(1, acc)
    phase("own2_01")
    own_gather(1, 0)
    own_gather(1, 1)
    phase("u2_wait")
    take_user(1, u2)
    phase("items3_32")
    items_x(2)
    items(2, core)
    phase("x3")
    for s in pieces:
        x_send(2, s)
    core_send_own(2)
    phase("own2_2")
    own_gather(1, 2)
    items(2, own)
    phase("own2_3")
    own_gather(1, last)
    phase("upart2_01")
    acc = user_part(2, own)
    gd[2].wait_recv()
    acc = user_part(2, core, acc)
    phase("fwd2_01")
    for s in halves:
        forward(2, s)
    acc = user_part(2, other, acc, 0, 2)
    for s in halves:
        f[2, s].wait_recv()
    acc = user_part(2, both, acc, 0, 2)

    def mean4(a, b, e, h):
        tot = ((a.astype(F32) + b.astype(F32)) + e.astype(F32)) + h.astype(F32)
        return (tot * (1.0 / (NUM_LAYERS + 1))).astype(BF16)

    def pick(tab, oh, hi, first):
        got = jnp.dot(tab, oh, preferred_element_type=F32)
        n = got.shape[0] // ROWS
        out = jnp.where(hi == first, got[:ROWS], 0.0)
        for i in range(1, n):
            out = out + jnp.where(hi == first + i, got[i * ROWS:(i + 1) * ROWS], 0.0)
        return out

    def final_piece(s):
        own_piece(2, s)
        outi_ref[:, s * sc:(s + 1) * sc] = mean4(*[ipan[k, own, s] for k in range(NUM_LAYERS + 1)])

    half = [pl.ds(h * hh, hh) for h in halves]

    def differences(m, h, first, n):
        groups = range(first * sc // GL, (first + n) * sc // GL)
        table = jnp.concatenate([outi_ref[:, i * GL:(i + 1) * GL] for i in groups], axis=0)
        for t in range(h * (hh // LB), (h + 1) * (hh // LB)):
            sl = slice(t * LB, (t + 1) * LB)
            pos = pick(table, hot_block(ohp.at[m], t), hip[m, :, sl], groups[0])
            neg = pick(table, hot_block(ohn.at[m], t), hin[m, :, sl], groups[0])
            gpart[m, :, sl] = pos - neg if first == 0 else (gpart[m, :, sl] + pos) - neg

    phase("own3")
    for s in range(last):
        final_piece(s)
    phase("diff_012")
    for m in order:
        for h in halves:
            differences(m, h, 0, last)
    phase("own3_last")
    final_piece(last)
    gd3, gd1, gx, gy = {}, {}, {}, {}
    phase("diff3")
    for h in halves:
        differences(both, h, last, 1)
        gd3[h] = cp.send(gpart.at[both, :, half[h]], grd.at[1, :, half[h]], dev_d)
    for h in halves:
        differences(other, h, last, 1)
    for h in halves:
        differences(core, h, last, 1)
    gd1 = cp.send(gpart.at[core], grd.at[0], dev_d)
    phase("gd3_wait")
    for h in halves:
        gd3[h].wait_recv()
        gsum[1, :, half[h]] = gpart[other, :, half[h]] + grd[1, :, half[h]]
        gx[h] = cp.send(gsum.at[1, :, half[h]], grx.at[:, half[h]], dev_x)
    phase("diff0")
    for h in halves:
        differences(own, h, last, 1)
    phase("fwd2_23")
    for s in (2, last):
        forward(2, s)
    acc = user_part(2, other, acc, 2, NS - 2)
    phase("f2_wait")
    for s in (2, last):
        f[2, s].wait_recv()
    acc = user_part(2, both, acc, 2, NS - 2)
    u3 = send_user(2, acc)
    phase("g_wait")
    gd1.wait_recv()
    for h in halves:
        gx[h].wait_recv()
        gsum[0, :, half[h]] = (gpart[own, :, half[h]] + grd[0, :, half[h]]) + grx[:, half[h]]
        gy[h] = cp.send(gsum.at[0, :, half[h]], gry.at[:, half[h]], dev_y)

    phase("u3_wait")
    take_user(2, u3)
    phase("finalu")
    eu[own] = mean4(*[upan[k] for k in range(NUM_LAYERS + 1)])
    ec = [cp.send(eu.at[own], eu.at[m], dev) for m, dev in ((core, dev_d), (other, dev_x), (both, dev_xd))]
    outu_ref[...] = eu[own, :, own_u]

    phase("e_wait")
    for copy in ec:
        copy.wait_recv()
    phase("picku")
    utab = jnp.concatenate([eu[m] for m in range(NQ)], axis=0)
    place = jnp.where(hiu[...] // 2 == x, own, other) + jnp.where(hiu[...] % 2 == c, own, core)
    picked = [pick(utab, hot_block(ohu, t), place[:, t * LB:(t + 1) * LB], own) for t in range(home // LB)]
    phase("gy_wait")
    for h in halves:
        gy[h].wait_recv()
    phase("dot")
    for t in range(home // LB):
        sl = slice(t * LB, (t + 1) * LB)
        diff = gsum[0, :, sl] + gry[:, sl]
        zbuf[z, r, :, sl] = jnp.sum(picked[t] * diff, axis=0, keepdims=True)
    zc = [cp.send(zbuf.at[z, r], zbuf.at[z, r], dev) for dev in score_devs]
    phase("z_wait")
    for copy in zc:
        copy.wait_recv()
    phase("loss")
    for q in range(NQ):
        neg = -(((zbuf[0, q] + zbuf[1, q]) + zbuf[2, q]) + zbuf[3, q])
        loss_ref[q] = jnp.maximum(neg, 0.0) + jnp.log1p(jnp.exp(-jnp.abs(neg)))
    phase("drain")
    cp.drain()
    phase(None)
    assert len(cp.started) == NUM_SEMS and len(loads) == NUM_LOADS


def solution(mesh):
    def local_fn(mask_blk, user_sh, item_sh, triples):
        users, items = mask_blk.shape
        cols, own_users = user_sh.shape[1], user_sh.shape[0]
        quarter = items // NQ
        home = triples.shape[0] // NQ
        vm, sem = pltpu.VMEM, pltpu.SemaphoreType.DMA
        nl = NUM_LAYERS
        sc = quarter // NS
        tiles = (NQ, quarter // LANES, users, LANES)
        per_item, hots = (NQ, 1, quarter), (NQ, home // LANES, GL, LANES)
        triple_row = (NQ, 1, home)
        scratch = [
            vm((NQ, users, quarter), jnp.int32), vm(tiles, BF16), vm(tiles, BF16),
            *[vm(per_item, F32)] * 5,
            vm((users, LANES), jnp.int32), vm((1, users), F32), vm((1, users), F32), vm((users, LANES), F32),
            vm(triples.shape[::-1], jnp.int32),
            vm((nl + 1, cols, users), BF16), vm((nl, cols, users), F32), vm((nl, cols, users), F32),
            vm((nl + 1, NQ, NS, cols, sc), BF16), vm((nl, NQ, NS, cols, sc), F32),
            vm((nl, 2, NS, cols, sc), F32), vm((nl, NS, cols, sc), F32), vm((nl, NS, cols, sc), F32),
            vm(hots, BF16), vm(hots, BF16), vm(hots[1:], BF16),
            vm(triple_row, jnp.int32), vm(triple_row, jnp.int32), vm(triple_row[1:], jnp.int32),
            vm((NQ, cols, home), F32), vm((2, cols, home), F32), vm((2, cols, home), F32),
            vm((cols, home), F32), vm((cols, home), F32),
            vm((NQ, cols, users), BF16), vm((mesh.shape["emb"], *triple_row), F32),
            sem((NUM_LOADS,)), sem((NUM_SEMS,)), sem((NUM_SEMS,)),
        ]
        vspec = pl.BlockSpec(memory_space=pltpu.VMEM)
        out_u, out_i, loss = pl.pallas_call(
            kernel,
            out_shape=[
                jax.ShapeDtypeStruct((cols, own_users), BF16),
                jax.ShapeDtypeStruct((cols, quarter), BF16),
                jax.ShapeDtypeStruct((NQ, 1, home), F32)],
            in_specs=[pl.BlockSpec(memory_space=pltpu.HBM)] * 4,
            out_specs=[vspec, vspec, vspec],
            scratch_shapes=scratch,
            compiler_params=pltpu.CompilerParams(
                collective_id=0, has_side_effects=True, vmem_limit_bytes=VMEM_LIMIT),
        )(mask_blk, user_sh.T, item_sh.T, triples.T)
        return out_u.T, out_i.T, loss.reshape(-1)

    return jax.shard_map(
        local_fn, mesh=mesh,
        in_specs=(P("row", "col"), P(("row", "col"), "emb"), P(("col", "row"), "emb"), P()),
        out_specs=(P(("row", "col"), "emb"), P(("col", "row"), "emb"), P()),
        check_vma=False)
```

```python
import functools

import jax
import jax.numpy as jnp
from jax import lax
from jax.experimental import pallas as pl
from jax.experimental.pallas import tpu as pltpu
from jax.sharding import PartitionSpec as P

NUM_LAYERS = 3
MESH = pl.DeviceIdType.MESH
F32 = jnp.float32
BF16 = jnp.bfloat16

NQ = 4
NM = 2
NS = 4
LB = 256
GL = 256
LANES = 128
ROWS = 16


class Copies:
    def __init__(self, send_sems, recv_sems):
        self.send_sems, self.recv_sems, self.started = send_sems, recv_sems, []

    def send(self, src, dst, device):
        k = len(self.started)
        copy = pltpu.make_async_remote_copy(
            src_ref=src, dst_ref=dst, send_sem=self.send_sems.at[k],
            recv_sem=self.recv_sems.at[k], device_id=device, device_id_type=MESH)
        copy.start()
        self.started.append(copy)
        return copy

    def drain(self):
        for copy in self.started:
            copy.wait_send()


VMEM_LIMIT = 52 * 2 ** 20
NUM_SEMS = 86
NUM_LOADS = NQ * NM + NS + 2


class Phase:
    def __init__(self):
        self.current = None

    def __call__(self, name):
        if self.current is not None:
            self.current.__exit__(None, None, None)
        self.current = None
        if name:
            self.current = jax.named_scope(name)
            self.current.__enter__()


def kernel(mask_hbm, u0_hbm, i0_hbm, trip_hbm, outu_ref, outi_ref, loss_ref,
           maskv, maskb, adj, csum, crd, crx, cch, invi, racc, rsum, rrecv, invu, trip_ref,
           upan, upart, urecv, ipan, ipart, ird, irx, isum,
           ohp, ohn, ohu, hip, hin, hiu, gpart, gsum, grd, grx, gry, eu, zbuf,
           in_sems, send_sems, recv_sems):
    users, quarter = maskv.shape[1:]
    own_users = u0_hbm.shape[1]
    sc = ipan.shape[-1]
    home = gpart.shape[-1]
    hh = home // 2
    mh = quarter // NM
    pieces, halves = range(NS), range(2)
    own, core, other, both = range(NQ)
    order = (both, other, core, own)

    z, y, r = lax.axis_index("emb"), lax.axis_index("col"), lax.axis_index("row")
    x, c = r // 2, r % 2
    nz = zbuf.shape[0]

    def rel(m):
        xx = x if m in (own, core) else 1 - x
        cc = c if m in (own, other) else 1 - c
        return 2 * xx + cc

    dev_d, dev_x, dev_xd = [(z, y, rel(m)) for m in (core, other, both)]
    dev_y = (z, 1 - y, r)
    score_devs = [((z + k) % nz, y, rel(m)) for k in range(nz) for m in range(NQ) if k or m]

    cp = Copies(send_sems, recv_sems)
    phase = Phase()
    phase("start")
    loads = []

    def load(src, dst):
        copy = pltpu.make_async_copy(src, dst, in_sems.at[len(loads)])
        copy.start()
        loads.append(copy)
        return copy

    y_off = pl.multiple_of(y * own_users, own_users)
    own_u = pl.ds(y_off, own_users)
    mask_copies, small = {}, []
    for m in order:
        for h in range(NM):
            off = pl.multiple_of(rel(m) * quarter + h * mh, mh)
            mask_copies[m, h] = load(mask_hbm.at[:, pl.ds(off, mh)], maskv.at[m, :, pl.ds(h * mh, mh)])
        if m == both:
            small.append(load(u0_hbm, upan.at[0, :, own_u]))
            small += [load(i0_hbm.at[:, pl.ds(s * sc, sc)], ipan.at[0, own, s]) for s in pieces]
            small.append(load(trip_hbm, trip_ref))

    barrier = pltpu.get_barrier_semaphore()
    for dev in (dev_y, *score_devs):
        pl.semaphore_signal(barrier, inc=1, device_id=dev, device_id_type=MESH)

    racc[...] = jnp.zeros_like(racc)

    def sums(m):
        for h in range(NM):
            mask_copies[m, h].wait()

            def body(j, carry):
                off = pl.multiple_of(h * mh + j * LB, LB)
                tile = h * (mh // LANES) + j * (LB // LANES)
                part = None
                for i in range(users // ROWS):
                    rows = pl.ds(ROWS * i, ROWS)
                    blk = maskv[m, rows, pl.ds(off, LB)]
                    ones = blk.astype(F32).astype(BF16)
                    row = None
                    for g in range(LB // LANES):
                        lanes = slice(LANES * g, LANES * (g + 1))
                        maskb[m, tile + g, rows, :] = ones[:, lanes]
                        row = blk[:, lanes] if row is None else row + blk[:, lanes]
                    racc[rows, :] += row
                    two = blk[:ROWS // 2] + blk[ROWS // 2:]
                    part = two if part is None else part + two
                csum[m, :, pl.ds(off, LB)] = jnp.sum(part.astype(F32), axis=0, keepdims=True)
                return carry
            lax.fori_loop(0, mh // LB, body, 0)

    def one_hot(lanes):
        hit = lax.broadcasted_iota(jnp.int32, (GL, LANES), 0) == lanes
        return jnp.where(hit, 1.0, 0.0).astype(BF16)

    def hot_block(oh, t):
        n = LB // LANES
        return jnp.concatenate([oh[t * n + i] for i in range(n)], axis=1)

    def one_hots(m):
        base = pl.multiple_of(rel(m) * home, home)
        for row, oh, hi in ((1, ohp, hip), (2, ohn, hin)):
            ids = trip_ref[pl.ds(row, 1), pl.ds(base, home)]
            owned = ids // quarter == y * NQ + r
            hi[m] = (ids % quarter) // GL
            low = jnp.where(owned, ids % GL, -1)
            for t in range(home // LANES):
                oh[m, t] = one_hot(low[:, t * LANES:(t + 1) * LANES])

    def user_one_hots():
        base = pl.multiple_of(r * home, home)
        uids = trip_ref[pl.ds(0, 1), pl.ds(base, home)]
        hiu[...] = uids // users
        low = uids % users
        for t in range(home // LANES):
            ohu[t] = one_hot(low[:, t * LANES:(t + 1) * LANES])

    csum_d, csum_x = {}, {}

    def chip_sums(m):
        csum_d[m].wait_recv()
        cch[m] = csum[m] + crd[m]
        csum_x[m ^ other] = cp.send(cch.at[m], crx.at[m ^ other], dev_x)

    def send_sums(m):
        csum_d[m ^ core] = cp.send(csum.at[m], crd.at[m ^ core], dev_d)

    phase("sums32")
    sums(both)
    sums(other)
    for copy in small:
        copy.wait()
    phase("barrier")
    pl.semaphore_wait(barrier, 1 + len(score_devs))
    phase("sums10")
    send_sums(both)
    send_sums(other)
    u0_y = cp.send(upan.at[0, :, own_u], upan.at[0, :, own_u], dev_y)
    i0_d = cp.send(ipan.at[0, own], ipan.at[0, core], dev_d)
    sums(core)
    send_sums(core)
    chip_sums(both)
    chip_sums(other)
    sums(own)
    send_sums(own)
    phase("rows")
    rows = jnp.transpose(racc[...].astype(F32), (1, 0))
    rsum[...] = jnp.sum(rows, axis=0, keepdims=True)
    rs_y = cp.send(rsum, rrecv, dev_y)
    chip_sums(core)
    one_hots(both)
    phase("chip0")
    chip_sums(own)
    i0_x = cp.send(ipan.at[0, own], ipan.at[0, other], dev_x)
    phase("onehots")
    one_hots(other)
    one_hots(core)
    phase("rs_wait")
    u0_y.wait_recv()
    rs_y.wait_recv()
    inv_row = lax.rsqrt(jnp.maximum(rsum[...] + rrecv[...], 1.0))
    invu[...] = jnp.transpose(jnp.broadcast_to(inv_row, (LANES, users)), (1, 0))
    phase("cx_wait")
    for m in order:
        csum_x[m].wait_recv()
        invi[m] = lax.rsqrt(jnp.maximum(cch[m] + crx[m], 1.0))

    tiles = sc // LANES

    def build(m, s):
        for tile in range(s * tiles, (s + 1) * tiles):
            scale = (invu[...] * invi[m, :, tile * LANES:(tile + 1) * LANES]).astype(BF16)
            adj[m, tile] = scale * maskb[m, tile]

    def block(m, s, n, rows):
        return jnp.concatenate([adj[m, t, rows, :] for t in range(s * tiles, (s + n) * tiles)], axis=1)

    def items(k, m, some=pieces):
        for s in some:
            ipart[k, m, s] = jnp.dot(upan[k], block(m, s, 1, slice(0, users)), preferred_element_type=F32)

    def user_part(k, m, acc=None, s=0, n=NS):
        table = jnp.concatenate([ipan[k, m, s + i] for i in range(n)], axis=1)
        out = []
        for h in halves:
            part = lax.dot_general(
                table, block(m, s, n, slice(h * own_users, (h + 1) * own_users)),
                (((1,), (1,)), ((), ())), preferred_element_type=F32)
            out.append(part if acc is None else acc[h] + part)
        return out

    d, xs, g, gd, f = {}, {}, {}, {}, {}

    def core_send(k, s):
        d[k, s] = cp.send(ipart.at[k, both, s], ird.at[k, 1, s], dev_d)

    def core_send_own(k):
        d[k] = cp.send(ipart.at[k, core], ird.at[k, 0], dev_d)

    def x_send(k, s):
        d[k, s].wait_recv()
        isum[k, s] = ipart[k, other, s] + ird[k, 1, s]
        xs[k, s] = cp.send(isum.at[k, s], irx.at[k, s], dev_x)

    def own_piece(k, s):
        if s == 0:
            d[k].wait_recv()
        xs[k, s].wait_recv()
        total = (ipart[k, own, s] + ird[k, 0, s]) + irx[k, s]
        ipan[k + 1, own, s] = total.astype(BF16)

    def own_gather(k, s):
        own_piece(k, s)
        g[k + 1, s] = cp.send(ipan.at[k + 1, own, s], ipan.at[k + 1, other, s], dev_x)
        if s == NS - 1:
            gd[k + 1] = cp.send(ipan.at[k + 1, own], ipan.at[k + 1, core], dev_d)

    def forward(k, s):
        g[k, s].wait_recv()
        f[k, s] = cp.send(ipan.at[k, other, s], ipan.at[k, both, s], dev_d)

    def send_user(k, acc):
        for h in halves:
            upart[k, :, h * own_users:(h + 1) * own_users] = acc[h]
        return cp.send(upart.at[k], urecv.at[k], dev_y)

    def take_user(k, got):
        got.wait_recv()
        upan[k + 1] = (upart[k] + urecv[k]).astype(BF16)

    last = NS - 1
    phase("build32")
    for s in pieces:
        build(both, s)
        items(0, both, [s])
        build(other, s)
        core_send(0, s)
        items(0, other, [s])
        if s > 1:
            x_send(0, s - 2)
    phase("build10")
    for s in pieces:
        build(core, s)
        if s in (1, last):
            x_send(0, NS - 2 + s // 2)
    for s in pieces:
        build(own, s)
    phase("upart0")
    i0_d.wait_recv()
    acc = user_part(0, core, user_part(0, own))
    i0_x.wait_recv()
    i0_f = cp.send(ipan.at[0, other], ipan.at[0, both], dev_d)
    acc = user_part(0, other, acc)
    phase("upart0b")
    i0_f.wait_recv()
    acc = user_part(0, both, acc)
    u1 = send_user(0, acc)
    phase("items1_10")
    items(0, core)
    core_send_own(0)
    items(0, own)
    one_hots(own)
    user_one_hots()
    for s in range(last):
        phase(f"own1_{s}")
        own_gather(0, s)
    phase("u1_wait")
    take_user(0, u1)

    def items_x(k):
        items(k, both)
        items(k, other, [0])
        for s in pieces:
            core_send(k, s)
        items(k, other, range(1, NS))

    phase("items2_32")
    items_x(1)
    phase("own1_last")
    own_gather(0, last)
    phase("x2")
    for s in pieces:
        x_send(1, s)
    phase("items2_10")
    items(1, core)
    core_send_own(1)
    items(1, own)
    phase("fwd1_0")
    forward(1, 0)
    acc = user_part(1, own)
    phase("fwd1_1")
    forward(1, 1)
    gd[1].wait_recv()
    acc = user_part(1, core, acc)
    phase("fwd1_2")
    forward(1, 2)
    acc = user_part(1, other, acc, 0, last)
    phase("fwd1_3")
    forward(1, last)
    acc = user_part(1, other, acc, last, 1)
    for s in range(last):
        f[1, s].wait_recv()
    acc = user_part(1, both, acc, 0, last)
    phase("f1_wait")
    f[1, last].wait_recv()
    acc = user_part(1, both, acc, last, 1)
    u2 = send_user(1, acc)
    phase("own2_01")
    own_gather(1, 0)
    own_gather(1, 1)
    phase("u2_wait")
    take_user(1, u2)
    phase("items3_32")
    items_x(2)
    items(2, core)
    phase("x3")
    for s in pieces:
        x_send(2, s)
    core_send_own(2)
    phase("own2_2")
    own_gather(1, 2)
    items(2, own)
    phase("own2_3")
    own_gather(1, last)
    phase("upart2_01")
    acc = user_part(2, own)
    gd[2].wait_recv()
    acc = user_part(2, core, acc)
    phase("fwd2_01")
    for s in halves:
        forward(2, s)
    acc = user_part(2, other, acc, 0, 2)
    for s in halves:
        f[2, s].wait_recv()
    acc = user_part(2, both, acc, 0, 2)

    def mean4(a, b, e, h):
        tot = ((a.astype(F32) + b.astype(F32)) + e.astype(F32)) + h.astype(F32)
        return (tot * (1.0 / (NUM_LAYERS + 1))).astype(BF16)

    def pick(tab, oh, hi, first):
        got = jnp.dot(tab, oh, preferred_element_type=F32)
        n = got.shape[0] // ROWS
        out = jnp.where(hi == first, got[:ROWS], 0.0)
        for i in range(1, n):
            out = out + jnp.where(hi == first + i, got[i * ROWS:(i + 1) * ROWS], 0.0)
        return out

    def final_piece(s):
        own_piece(2, s)
        outi_ref[:, s * sc:(s + 1) * sc] = mean4(*[ipan[k, own, s] for k in range(NUM_LAYERS + 1)])

    half = [pl.ds(h * hh, hh) for h in halves]

    def differences(m, h, first, n):
        groups = range(first * sc // GL, (first + n) * sc // GL)
        table = jnp.concatenate([outi_ref[:, i * GL:(i + 1) * GL] for i in groups], axis=0)
        for t in range(h * (hh // LB), (h + 1) * (hh // LB)):
            sl = slice(t * LB, (t + 1) * LB)
            pos = pick(table, hot_block(ohp.at[m], t), hip[m, :, sl], groups[0])
            neg = pick(table, hot_block(ohn.at[m], t), hin[m, :, sl], groups[0])
            gpart[m, :, sl] = pos - neg if first == 0 else (gpart[m, :, sl] + pos) - neg

    phase("own3")
    for s in range(last):
        final_piece(s)
    phase("diff_012")
    for m in order:
        for h in halves:
            differences(m, h, 0, last)
    phase("own3_last")
    final_piece(last)
    gd3, gd1, gx, gy = {}, {}, {}, {}
    phase("diff3")
    for h in halves:
        differences(both, h, last, 1)
        gd3[h] = cp.send(gpart.at[both, :, half[h]], grd.at[1, :, half[h]], dev_d)
    for h in halves:
        differences(other, h, last, 1)
    for h in halves:
        differences(core, h, last, 1)
    gd1 = cp.send(gpart.at[core], grd.at[0], dev_d)
    phase("gd3_wait")
    for h in halves:
        gd3[h].wait_recv()
        gsum[1, :, half[h]] = gpart[other, :, half[h]] + grd[1, :, half[h]]
        gx[h] = cp.send(gsum.at[1, :, half[h]], grx.at[:, half[h]], dev_x)
    phase("diff0")
    for h in halves:
        differences(own, h, last, 1)
    phase("fwd2_23")
    for s in (2, last):
        forward(2, s)
    acc = user_part(2, other, acc, 2, NS - 2)
    phase("f2_wait")
    for s in (2, last):
        f[2, s].wait_recv()
    acc = user_part(2, both, acc, 2, NS - 2)
    u3 = send_user(2, acc)
    phase("g_wait")
    gd1.wait_recv()
    for h in halves:
        gx[h].wait_recv()
        gsum[0, :, half[h]] = (gpart[own, :, half[h]] + grd[0, :, half[h]]) + grx[:, half[h]]
        gy[h] = cp.send(gsum.at[0, :, half[h]], gry.at[:, half[h]], dev_y)

    phase("u3_wait")
    take_user(2, u3)
    phase("finalu")
    eu[own] = mean4(*[upan[k] for k in range(NUM_LAYERS + 1)])
    ec = [cp.send(eu.at[own], eu.at[m], dev) for m, dev in ((core, dev_d), (other, dev_x), (both, dev_xd))]
    outu_ref[...] = eu[own, :, own_u]

    phase("e_wait")
    for copy in ec:
        copy.wait_recv()
    phase("picku")
    utab = jnp.concatenate([eu[m] for m in range(NQ)], axis=0)
    place = jnp.where(hiu[...] // 2 == x, own, other) + jnp.where(hiu[...] % 2 == c, own, core)
    picked = [pick(utab, hot_block(ohu, t), place[:, t * LB:(t + 1) * LB], own) for t in range(home // LB)]
    phase("gy_wait")
    for h in halves:
        gy[h].wait_recv()
    phase("dot")
    for t in range(home // LB):
        sl = slice(t * LB, (t + 1) * LB)
        diff = gsum[0, :, sl] + gry[:, sl]
        zbuf[z, r, :, sl] = jnp.sum(picked[t] * diff, axis=0, keepdims=True)
    zc = [cp.send(zbuf.at[z, r], zbuf.at[z, r], dev) for dev in score_devs]
    phase("z_wait")
    for copy in zc:
        copy.wait_recv()
    phase("loss")
    for q in range(NQ):
        neg = -(((zbuf[0, q] + zbuf[1, q]) + zbuf[2, q]) + zbuf[3, q])
        loss_ref[q] = jnp.maximum(neg, 0.0) + jnp.log1p(jnp.exp(-jnp.abs(neg)))
    phase("drain")
    cp.drain()
    phase(None)
    assert len(cp.started) == NUM_SEMS and len(loads) == NUM_LOADS


def emit(*refs):
    n = len(refs) // 2
    sems = refs[-1]
    copies = [pltpu.make_async_copy(src, dst, sems.at[i]) for i, (src, dst) in enumerate(zip(refs[:n], refs[n:]))]
    for copy in copies:
        copy.start()
    for copy in copies:
        copy.wait()


def solution(mesh):
    def local_fn(mask_blk, user_sh, item_sh, triples):
        users, items = mask_blk.shape
        cols, own_users = user_sh.shape[1], user_sh.shape[0]
        quarter = items // NQ
        home = triples.shape[0] // NQ
        vm, sem = pltpu.VMEM, pltpu.SemaphoreType.DMA
        nl = NUM_LAYERS
        sc = quarter // NS
        tiles = (NQ, quarter // LANES, users, LANES)
        per_item, hots = (NQ, 1, quarter), (NQ, home // LANES, GL, LANES)
        triple_row = (NQ, 1, home)
        scratch = [
            vm((NQ, users, quarter), jnp.int32), vm(tiles, BF16), vm(tiles, BF16),
            *[vm(per_item, F32)] * 5,
            vm((users, LANES), jnp.int32), vm((1, users), F32), vm((1, users), F32), vm((users, LANES), F32),
            vm(triples.shape[::-1], jnp.int32),
            vm((nl + 1, cols, users), BF16), vm((nl, cols, users), F32), vm((nl, cols, users), F32),
            vm((nl + 1, NQ, NS, cols, sc), BF16), vm((nl, NQ, NS, cols, sc), F32),
            vm((nl, 2, NS, cols, sc), F32), vm((nl, NS, cols, sc), F32), vm((nl, NS, cols, sc), F32),
            vm(hots, BF16), vm(hots, BF16), vm(hots[1:], BF16),
            vm(triple_row, jnp.int32), vm(triple_row, jnp.int32), vm(triple_row[1:], jnp.int32),
            vm((NQ, cols, home), F32), vm((2, cols, home), F32), vm((2, cols, home), F32),
            vm((cols, home), F32), vm((cols, home), F32),
            vm((NQ, cols, users), BF16), vm((mesh.shape["emb"], *triple_row), F32),
            sem((NUM_LOADS,)), sem((NUM_SEMS,)), sem((NUM_SEMS,)),
        ]
        vspec = pl.BlockSpec(memory_space=pltpu.VMEM)
        out_u, out_i, loss = pl.pallas_call(
            kernel,
            out_shape=[
                jax.ShapeDtypeStruct((cols, own_users), BF16),
                jax.ShapeDtypeStruct((cols, quarter), BF16),
                jax.ShapeDtypeStruct((NQ, 1, home), F32)],
            in_specs=[pl.BlockSpec(memory_space=pltpu.HBM)] * 4,
            out_specs=[vspec, vspec, vspec],
            scratch_shapes=scratch,
            compiler_params=pltpu.CompilerParams(
                collective_id=0, has_side_effects=True, vmem_limit_bytes=VMEM_LIMIT),
        )(*[pltpu.with_memory_space_constraint(a, pltpu.HBM) for a in (mask_blk, user_sh.T, item_sh.T, triples.T)])
        out_u, out_i, loss = pl.pallas_call(
            emit,
            out_shape=[jax.ShapeDtypeStruct(a.shape, a.dtype) for a in (out_u, out_i, loss)],
            in_specs=[vspec] * 3, out_specs=[pl.BlockSpec(memory_space=pltpu.HBM)] * 3,
            scratch_shapes=[sem((3,))],
            compiler_params=pltpu.CompilerParams(vmem_limit_bytes=2 ** 20),
        )(out_u, out_i, loss)
        return out_u.T, out_i.T, loss.reshape(-1)

    return jax.shard_map(
        local_fn, mesh=mesh,
        in_specs=(P("row", "col"), P(("row", "col"), "emb"), P(("col", "row"), "emb"), P()),
        out_specs=(P(("row", "col"), "emb"), P(("col", "row"), "emb"), P()),
        check_vma=False)
```

```python
import functools

import jax
import jax.numpy as jnp
from jax import lax
from jax.experimental import pallas as pl
from jax.experimental.pallas import tpu as pltpu
from jax.sharding import PartitionSpec as P

NUM_LAYERS = 3
MESH = pl.DeviceIdType.MESH
F32 = jnp.float32
BF16 = jnp.bfloat16

NQ = 4
NM = 2
NS = 4
LB = 256
GL = 256
LANES = 128
ROWS = 16


class Copies:
    def __init__(self, send_sems, recv_sems):
        self.send_sems, self.recv_sems = send_sems, recv_sems
        self.recvs, self.groups, self.single = 0, {}, []

    def recv_sem(self):
        self.recvs += 1
        return self.recv_sems.at[self.recvs - 1]

    def send(self, src, dst, device, group=None, whole=None, recv_sem=None):
        count = len(self.groups) + len(self.single)
        if group is None:
            sem = self.send_sems.at[count]
        else:
            if group not in self.groups:
                self.groups[group] = (self.send_sems.at[count], whole)
            sem = self.groups[group][0]
        copy = pltpu.make_async_remote_copy(
            src_ref=src, dst_ref=dst, send_sem=sem,
            recv_sem=self.recv_sem() if recv_sem is None else recv_sem,
            device_id=device, device_id_type=MESH)
        copy.start()
        if group is None:
            self.single.append(copy)
        return copy

    def drain(self):
        for copy in self.single:
            copy.wait_send()
        for sem, whole in self.groups.values():
            wait_bytes(whole, sem)


def wait_bytes(ref, sem):
    pltpu.make_async_copy(ref, ref, sem).wait()


VMEM_LIMIT = 52 * 2 ** 20
NUM_SENDS = 35
NUM_RECVS = 71
NUM_LOADS = NQ * NM + NS + 2


class Phase:
    def __init__(self):
        self.current = None

    def __call__(self, name):
        if self.current is not None:
            self.current.__exit__(None, None, None)
        self.current = None
        if name:
            self.current = jax.named_scope(name)
            self.current.__enter__()


def kernel(mask_hbm, u0_hbm, i0_hbm, trip_hbm, outu_ref, outi_ref, loss_ref,
           maskv, maskb, adj, csum, crd, crx, cch, invi, racc, rsum, rrecv, invu, trip_ref,
           upan, upart, urecv, ipan, ipart, ird, irx, isum,
           ohp, ohn, ohu, hip, hin, hiu, gpart, gsum, grd, grx, gry, grxy, eu, zbuf,
           in_sems, send_sems, recv_sems):
    users, quarter = maskv.shape[1:]
    own_users = u0_hbm.shape[1]
    sc = ipan.shape[-1]
    home = gpart.shape[-1]
    hh = home // 2
    mh = quarter // NM
    pieces, halves = range(NS), range(2)
    own, core, other, both = range(NQ)
    order = (both, other, core, own)

    z, y, r = lax.axis_index("emb"), lax.axis_index("col"), lax.axis_index("row")
    x, c = r // 2, r % 2
    nz = zbuf.shape[0] // NQ
    slot = z * NQ + r

    def rel(m):
        xx = x if m in (own, core) else 1 - x
        cc = c if m in (own, other) else 1 - c
        return 2 * xx + cc

    dev_d, dev_x, dev_xd = [(z, y, rel(m)) for m in (core, other, both)]
    dev_y, dev_xy = (z, 1 - y, r), (z, 1 - y, rel(other))
    score_devs = [((z + k) % nz, y, rel(m)) for k in range(nz) for m in range(NQ) if k or m]

    cp = Copies(send_sems, recv_sems)
    phase = Phase()
    phase("start")
    loads = []

    def load(src, dst):
        copy = pltpu.make_async_copy(src, dst, in_sems.at[len(loads)])
        copy.start()
        loads.append(copy)
        return copy

    y_off = pl.multiple_of(y * own_users, own_users)
    own_u = pl.ds(y_off, own_users)
    mask_copies, small = {}, []
    for m in order:
        for h in range(NM):
            off = pl.multiple_of(rel(m) * quarter + h * mh, mh)
            mask_copies[m, h] = load(mask_hbm.at[:, pl.ds(off, mh)], maskv.at[m, :, pl.ds(h * mh, mh)])
        if m == both:
            small.append(load(u0_hbm, upan.at[0, :, own_u]))
            small += [load(i0_hbm.at[:, pl.ds(s * sc, sc)], ipan.at[0, own, s]) for s in pieces]
            small.append(load(trip_hbm, trip_ref))

    barrier = pltpu.get_barrier_semaphore()
    for dev in (dev_y, dev_xy, *score_devs):
        pl.semaphore_signal(barrier, inc=1, device_id=dev, device_id_type=MESH)

    racc[...] = jnp.zeros_like(racc)

    def sums(m):
        for h in range(NM):
            mask_copies[m, h].wait()

            def body(j, carry):
                off = pl.multiple_of(h * mh + j * LB, LB)
                tile = h * (mh // LANES) + j * (LB // LANES)
                part = None
                for i in range(users // ROWS):
                    rows = pl.ds(ROWS * i, ROWS)
                    blk = maskv[m, rows, pl.ds(off, LB)]
                    ones = blk.astype(F32).astype(BF16)
                    row = None
                    for g in range(LB // LANES):
                        lanes = slice(LANES * g, LANES * (g + 1))
                        maskb[m, tile + g, rows, :] = ones[:, lanes]
                        row = blk[:, lanes] if row is None else row + blk[:, lanes]
                    racc[rows, :] += row
                    two = blk[:ROWS // 2] + blk[ROWS // 2:]
                    part = two if part is None else part + two
                csum[m, :, pl.ds(off, LB)] = jnp.sum(part.astype(F32), axis=0, keepdims=True)
                return carry
            lax.fori_loop(0, mh // LB, body, 0)

    def one_hot(lanes):
        hit = lax.broadcasted_iota(jnp.int32, (GL, LANES), 0) == lanes
        return jnp.where(hit, 1.0, 0.0).astype(BF16)

    def hot_block(oh, t):
        n = LB // LANES
        return jnp.concatenate([oh[t * n + i] for i in range(n)], axis=1)

    def one_hots(m):
        base = pl.multiple_of(rel(m) * home, home)
        for row, oh, hi in ((1, ohp, hip), (2, ohn, hin)):
            ids = trip_ref[pl.ds(row, 1), pl.ds(base, home)]
            owned = ids // quarter == y * NQ + r
            hi[m] = (ids % quarter) // GL
            low = jnp.where(owned, ids % GL, -1)
            for t in range(home // LANES):
                oh[m, t] = one_hot(low[:, t * LANES:(t + 1) * LANES])

    def user_one_hots():
        base = pl.multiple_of(r * home, home)
        uids = trip_ref[pl.ds(0, 1), pl.ds(base, home)]
        hiu[...] = uids // users
        low = uids % users
        for t in range(home // LANES):
            ohu[t] = one_hot(low[:, t * LANES:(t + 1) * LANES])

    csum_d, csum_x = {}, {}

    def chip_sums(m):
        csum_d[m].wait_recv()
        cch[m] = csum[m] + crd[m]
        csum_x[m ^ other] = cp.send(cch.at[m], crx.at[m ^ other], dev_x, "chip", cch)

    def send_sums(m):
        csum_d[m ^ core] = cp.send(csum.at[m], crd.at[m ^ core], dev_d, "sums", csum)

    phase("sums32")
    sums(both)
    sums(other)
    for copy in small:
        copy.wait()
    phase("barrier")
    pl.semaphore_wait(barrier, 2 + len(score_devs))
    phase("sums10")
    send_sums(both)
    send_sums(other)
    u0_y = cp.send(upan.at[0, :, own_u], upan.at[0, :, own_u], dev_y)
    i0_d = cp.send(ipan.at[0, own], ipan.at[0, core], dev_d)
    sums(core)
    send_sums(core)
    chip_sums(both)
    chip_sums(other)
    sums(own)
    send_sums(own)
    phase("rows")
    rows = jnp.transpose(racc[...].astype(F32), (1, 0))
    rsum[...] = jnp.sum(rows, axis=0, keepdims=True)
    rs_y = cp.send(rsum, rrecv, dev_y)
    chip_sums(core)
    one_hots(both)
    phase("chip0")
    chip_sums(own)
    i0_x = cp.send(ipan.at[0, own], ipan.at[0, other], dev_x)
    phase("onehots")
    one_hots(other)
    one_hots(core)
    phase("rs_wait")
    u0_y.wait_recv()
    rs_y.wait_recv()
    inv_row = lax.rsqrt(jnp.maximum(rsum[...] + rrecv[...], 1.0))
    invu[...] = jnp.transpose(jnp.broadcast_to(inv_row, (LANES, users)), (1, 0))
    phase("cx_wait")
    for m in order:
        csum_x[m].wait_recv()
        invi[m] = lax.rsqrt(jnp.maximum(cch[m] + crx[m], 1.0))

    tiles = sc // LANES

    def build(m, s):
        for tile in range(s * tiles, (s + 1) * tiles):
            scale = (invu[...] * invi[m, :, tile * LANES:(tile + 1) * LANES]).astype(BF16)
            adj[m, tile] = scale * maskb[m, tile]

    def block(m, s, n, rows):
        return jnp.concatenate([adj[m, t, rows, :] for t in range(s * tiles, (s + n) * tiles)], axis=1)

    def items(k, m, some=pieces):
        for s in some:
            ipart[k, m, s] = jnp.dot(upan[k], block(m, s, 1, slice(0, users)), preferred_element_type=F32)

    def user_part(k, m, acc=None, s=0, n=NS):
        table = jnp.concatenate([ipan[k, m, s + i] for i in range(n)], axis=1)
        out = []
        for h in halves:
            part = lax.dot_general(
                table, block(m, s, n, slice(h * own_users, (h + 1) * own_users)),
                (((1,), (1,)), ((), ())), preferred_element_type=F32)
            out.append(part if acc is None else acc[h] + part)
        return out

    d, xs, g, gd, f = {}, {}, {}, {}, {}

    def core_send(k, s):
        d[k, s] = cp.send(ipart.at[k, both, s], ird.at[k, 1, s], dev_d, ("core", k), ipart.at[k, both])

    def core_send_own(k):
        d[k] = cp.send(ipart.at[k, core], ird.at[k, 0], dev_d)

    def x_send(k, s):
        d[k, s].wait_recv()
        isum[k, s] = ipart[k, other, s] + ird[k, 1, s]
        xs[k, s] = cp.send(isum.at[k, s], irx.at[k, s], dev_x, ("x", k), isum.at[k])

    def own_piece(k, s):
        if s == 0:
            d[k].wait_recv()
        xs[k, s].wait_recv()
        total = (ipart[k, own, s] + ird[k, 0, s]) + irx[k, s]
        ipan[k + 1, own, s] = total.astype(BF16)

    def own_gather(k, s):
        own_piece(k, s)
        g[k + 1, s] = cp.send(
            ipan.at[k + 1, own, s], ipan.at[k + 1, other, s], dev_x, ("gather", k), ipan.at[k + 1, own])
        if s == NS - 1:
            gd[k + 1] = cp.send(ipan.at[k + 1, own], ipan.at[k + 1, core], dev_d)

    def forward(k, s):
        g[k, s].wait_recv()
        f[k, s] = cp.send(ipan.at[k, other, s], ipan.at[k, both, s], dev_d, ("forward", k), ipan.at[k, other])

    def send_user(k, acc):
        for h in halves:
            upart[k, :, h * own_users:(h + 1) * own_users] = acc[h]
        return cp.send(upart.at[k], urecv.at[k], dev_y)

    def take_user(k, got):
        got.wait_recv()
        upan[k + 1] = (upart[k] + urecv[k]).astype(BF16)

    last = NS - 1
    phase("build32")
    for s in pieces:
        build(both, s)
        items(0, both, [s])
        build(other, s)
        core_send(0, s)
        items(0, other, [s])
        if s > 1:
            x_send(0, s - 2)
    phase("build10")
    for s in pieces:
        build(core, s)
        if s in (1, last):
            x_send(0, NS - 2 + s // 2)
    for s in pieces:
        build(own, s)
    phase("upart0")
    i0_d.wait_recv()
    acc = user_part(0, core, user_part(0, own))
    i0_x.wait_recv()
    i0_f = cp.send(ipan.at[0, other], ipan.at[0, both], dev_d)
    acc = user_part(0, other, acc)
    phase("upart0b")
    i0_f.wait_recv()
    acc = user_part(0, both, acc)
    u1 = send_user(0, acc)
    phase("items1_10")
    items(0, core)
    core_send_own(0)
    items(0, own)
    one_hots(own)
    user_one_hots()
    for s in range(last):
        phase(f"own1_{s}")
        own_gather(0, s)
    phase("u1_wait")
    take_user(0, u1)

    def items_x(k):
        items(k, both)
        items(k, other, [0])
        for s in pieces:
            core_send(k, s)
        items(k, other, range(1, NS))

    phase("items2_32")
    items_x(1)
    phase("own1_last")
    own_gather(0, last)
    phase("x2")
    for s in pieces:
        x_send(1, s)
    phase("items2_10")
    items(1, core)
    core_send_own(1)
    items(1, own)
    phase("fwd1_0")
    forward(1, 0)
    acc = user_part(1, own)
    phase("fwd1_1")
    forward(1, 1)
    gd[1].wait_recv()
    acc = user_part(1, core, acc)
    phase("fwd1_2")
    forward(1, 2)
    acc = user_part(1, other, acc, 0, last)
    phase("fwd1_3")
    forward(1, last)
    acc = user_part(1, other, acc, last, 1)
    for s in range(last):
        f[1, s].wait_recv()
    acc = user_part(1, both, acc, 0, last)
    phase("f1_wait")
    f[1, last].wait_recv()
    acc = user_part(1, both, acc, last, 1)
    u2 = send_user(1, acc)
    phase("own2_01")
    own_gather(1, 0)
    own_gather(1, 1)
    phase("u2_wait")
    take_user(1, u2)
    phase("items3_32")
    items_x(2)
    items(2, core)
    phase("x3")
    x_send(2, 0)
    core_send_own(2)
    phase("own2_2")
    own_gather(1, 2)
    phase("own2_3")
    own_gather(1, last)
    for s in range(1, NS):
        x_send(2, s)
    phase("items3_own")
    items(2, own)
    phase("upart2_01")
    acc = user_part(2, own)
    gd[2].wait_recv()
    acc = user_part(2, core, acc)
    phase("fwd2_01")
    for s in halves:
        forward(2, s)
    acc = user_part(2, other, acc, 0, 2)
    for s in halves:
        f[2, s].wait_recv()
    acc = user_part(2, both, acc, 0, 2)
    phase("fwd2_23")
    for s in (2, last):
        forward(2, s)
    acc = user_part(2, other, acc, 2, NS - 2)
    phase("f2_wait")
    for s in (2, last):
        f[2, s].wait_recv()
    acc = user_part(2, both, acc, 2, NS - 2)
    u3 = send_user(2, acc)

    def mean4(a, b, e, h):
        tot = ((a.astype(F32) + b.astype(F32)) + e.astype(F32)) + h.astype(F32)
        return (tot * (1.0 / (NUM_LAYERS + 1))).astype(BF16)

    def pick(tab, oh, hi, first):
        got = jnp.dot(tab, oh, preferred_element_type=F32)
        n = got.shape[0] // ROWS
        out = jnp.where(hi == first, got[:ROWS], 0.0)
        for i in range(1, n):
            out = out + jnp.where(hi == first + i, got[i * ROWS:(i + 1) * ROWS], 0.0)
        return out

    def final_piece(s):
        own_piece(2, s)
        outi_ref[:, s * sc:(s + 1) * sc] = mean4(*[ipan[k, own, s] for k in range(NUM_LAYERS + 1)])

    half = [pl.ds(h * hh, hh) for h in halves]

    def differences(m, h, first, n):
        groups = range(first * sc // GL, (first + n) * sc // GL)
        table = jnp.concatenate([outi_ref[:, i * GL:(i + 1) * GL] for i in groups], axis=0)
        for t in range(h * (hh // LB), (h + 1) * (hh // LB)):
            sl = slice(t * LB, (t + 1) * LB)
            pos = pick(table, hot_block(ohp.at[m], t), hip[m, :, sl], groups[0])
            neg = pick(table, hot_block(ohn.at[m], t), hin[m, :, sl], groups[0])
            gpart[m, :, sl] = pos - neg if first == 0 else (gpart[m, :, sl] + pos) - neg

    phase("own3")
    for s in range(last):
        final_piece(s)
    phase("diff_012")
    for m in order:
        for h in halves:
            differences(m, h, 0, last)
    phase("u3_wait")
    take_user(2, u3)
    phase("finalu")
    eu[own] = mean4(*[upan[k] for k in range(NUM_LAYERS + 1)])
    others = eu.at[pl.ds(core, NQ - 1)]
    eu_sem = cp.recv_sem()
    for m, dev in ((core, dev_d), (other, dev_x), (both, dev_xd)):
        cp.send(eu.at[own], eu.at[m], dev, "eu", others, eu_sem)
    outu_ref[...] = eu[own, :, own_u]

    phase("own3_last")
    final_piece(last)
    gd3, gx, gxy = {}, {}, {}
    phase("diff3")
    for h in halves:
        differences(both, h, last, 1)
        gd3[h] = cp.send(gpart.at[both, :, half[h]], grd.at[1, :, half[h]], dev_d)
    for h in halves:
        differences(other, h, last, 1)
    for h in halves:
        differences(core, h, last, 1)
    gd1 = cp.send(gpart.at[core], grd.at[0], dev_d)
    phase("gd3_wait")
    for h in halves:
        gd3[h].wait_recv()
        gsum[1, :, half[h]] = gpart[other, :, half[h]] + grd[1, :, half[h]]
        gx[h] = cp.send(gsum.at[1, :, half[h]], grx.at[:, half[h]], dev_x)
        gxy[h] = cp.send(gsum.at[1, :, half[h]], grxy.at[:, half[h]], dev_xy)
    phase("diff0")
    for h in halves:
        differences(own, h, last, 1)
    phase("gd1_wait")
    gd1.wait_recv()
    gsum[0] = gpart[own] + grd[0]
    gy = cp.send(gsum.at[0], gry, dev_y)
    phase("e_wait")
    wait_bytes(others, eu_sem)
    phase("picku")
    utab = jnp.concatenate([eu[m] for m in range(NQ)], axis=0)
    place = jnp.where(hiu[...] // 2 == x, own, other) + jnp.where(hiu[...] % 2 == c, own, core)
    picked = [pick(utab, hot_block(ohu, t), place[:, t * LB:(t + 1) * LB], own) for t in range(home // LB)]
    phase("gy_wait")
    gy.wait_recv()
    for h in halves:
        gx[h].wait_recv()
        gxy[h].wait_recv()
    phase("dot")
    for t in range(home // LB):
        sl = slice(t * LB, (t + 1) * LB)
        diff = (gsum[0, :, sl] + grx[:, sl]) + (gry[:, sl] + grxy[:, sl])
        zbuf[slot, :, sl] = jnp.sum(picked[t] * diff, axis=0, keepdims=True)
    rest = zbuf.at[pl.ds(0, len(score_devs))]
    z_sem = cp.recv_sem()
    for dev in score_devs:
        cp.send(zbuf.at[slot], zbuf.at[slot], dev, "score", rest, z_sem)
    phase("z_wait")
    wait_bytes(rest, z_sem)
    phase("loss")
    for q in range(NQ):
        neg = -sum(zbuf[k * NQ + q] for k in range(nz))
        loss_ref[q] = jnp.maximum(neg, 0.0) + jnp.log1p(jnp.exp(-jnp.abs(neg)))
    phase("drain")
    cp.drain()
    phase(None)
    assert (len(cp.groups) + len(cp.single), cp.recvs, len(loads)) == (NUM_SENDS, NUM_RECVS, NUM_LOADS)


def emit(*refs):
    n = len(refs) // 2
    sems = refs[-1]
    copies = [pltpu.make_async_copy(src, dst, sems.at[i]) for i, (src, dst) in enumerate(zip(refs[:n], refs[n:]))]
    for copy in copies:
        copy.start()
    for copy in copies:
        copy.wait()


def solution(mesh):
    def local_fn(mask_blk, user_sh, item_sh, triples):
        users, items = mask_blk.shape
        cols, own_users = user_sh.shape[1], user_sh.shape[0]
        quarter = items // NQ
        home = triples.shape[0] // NQ
        vm, sem = pltpu.VMEM, pltpu.SemaphoreType.DMA
        nl = NUM_LAYERS
        sc = quarter // NS
        tiles = (NQ, quarter // LANES, users, LANES)
        per_item, hots = (NQ, 1, quarter), (NQ, home // LANES, GL, LANES)
        triple_row = (NQ, 1, home)
        scratch = [
            vm((NQ, users, quarter), jnp.int32), vm(tiles, BF16), vm(tiles, BF16),
            *[vm(per_item, F32)] * 5,
            vm((users, LANES), jnp.int32), vm((1, users), F32), vm((1, users), F32), vm((users, LANES), F32),
            vm(triples.shape[::-1], jnp.int32),
            vm((nl + 1, cols, users), BF16), vm((nl, cols, users), F32), vm((nl, cols, users), F32),
            vm((nl + 1, NQ, NS, cols, sc), BF16), vm((nl, NQ, NS, cols, sc), F32),
            vm((nl, 2, NS, cols, sc), F32), vm((nl, NS, cols, sc), F32), vm((nl, NS, cols, sc), F32),
            vm(hots, BF16), vm(hots, BF16), vm(hots[1:], BF16),
            vm(triple_row, jnp.int32), vm(triple_row, jnp.int32), vm(triple_row[1:], jnp.int32),
            vm((NQ, cols, home), F32), vm((2, cols, home), F32), vm((2, cols, home), F32),
            *[vm((cols, home), F32)] * 3,
            vm((NQ, cols, users), BF16), vm((mesh.shape["emb"] * NQ, 1, home), F32),
            sem((NUM_LOADS,)), sem((NUM_SENDS,)), sem((NUM_RECVS,)),
        ]
        vspec = pl.BlockSpec(memory_space=pltpu.VMEM)
        out_u, out_i, loss = pl.pallas_call(
            kernel,
            out_shape=[
                jax.ShapeDtypeStruct((cols, own_users), BF16),
                jax.ShapeDtypeStruct((cols, quarter), BF16),
                jax.ShapeDtypeStruct((NQ, 1, home), F32)],
            in_specs=[pl.BlockSpec(memory_space=pltpu.HBM)] * 4,
            out_specs=[vspec, vspec, vspec],
            scratch_shapes=scratch,
            compiler_params=pltpu.CompilerParams(
                collective_id=0, has_side_effects=True, vmem_limit_bytes=VMEM_LIMIT),
        )(*[pltpu.with_memory_space_constraint(a, pltpu.HBM) for a in (mask_blk, user_sh.T, item_sh.T, triples.T)])
        out_u, out_i, loss = pl.pallas_call(
            emit,
            out_shape=[jax.ShapeDtypeStruct(a.shape, a.dtype) for a in (out_u, out_i, loss)],
            in_specs=[vspec] * 3, out_specs=[pl.BlockSpec(memory_space=pltpu.HBM)] * 3,
            scratch_shapes=[sem((3,))],
            compiler_params=pltpu.CompilerParams(vmem_limit_bytes=2 ** 20),
        )(out_u, out_i, loss)
        return out_u.T, out_i.T, loss.reshape(-1)

    return jax.shard_map(
        local_fn, mesh=mesh,
        in_specs=(P("row", "col"), P(("row", "col"), "emb"), P(("col", "row"), "emb"), P()),
        out_specs=(P(("row", "col"), "emb"), P(("col", "row"), "emb"), P()),
        check_vma=False)
```

```python
import functools

import jax
import jax.numpy as jnp
from jax import lax
from jax.experimental import pallas as pl
from jax.experimental.pallas import tpu as pltpu
from jax.sharding import PartitionSpec as P

NUM_LAYERS = 3
MESH = pl.DeviceIdType.MESH
F32 = jnp.float32
BF16 = jnp.bfloat16

NQ = 4
NM = 2
NS = 4
LB = 256
GL = 256
LANES = 128
ROWS = 16


class Copies:
    def __init__(self, send_sems, recv_sems):
        self.send_sems, self.recv_sems = send_sems, recv_sems
        self.recvs, self.groups, self.single = 0, {}, []

    def recv_sem(self):
        self.recvs += 1
        return self.recv_sems.at[self.recvs - 1]

    def send(self, src, dst, device, group=None, whole=None, recv_sem=None):
        count = len(self.groups) + len(self.single)
        if group is None:
            sem = self.send_sems.at[count]
        else:
            if group not in self.groups:
                self.groups[group] = (self.send_sems.at[count], whole)
            sem = self.groups[group][0]
        copy = pltpu.make_async_remote_copy(
            src_ref=src, dst_ref=dst, send_sem=sem,
            recv_sem=self.recv_sem() if recv_sem is None else recv_sem,
            device_id=device, device_id_type=MESH)
        copy.start()
        if group is None:
            self.single.append(copy)
        return copy

    def drain(self):
        for copy in self.single:
            copy.wait_send()
        for sem, whole in self.groups.values():
            wait_bytes(whole, sem)


def wait_bytes(ref, sem):
    pltpu.make_async_copy(ref, ref, sem).wait()


VMEM_LIMIT = 52 * 2 ** 20
NUM_SENDS = 35
NUM_RECVS = 71
NUM_LOADS = NQ * NM + NS + 2


class Phase:
    def __init__(self):
        self.current = None

    def __call__(self, name):
        if self.current is not None:
            self.current.__exit__(None, None, None)
        self.current = None
        if name:
            self.current = jax.named_scope(name)
            self.current.__enter__()


def kernel(mask_hbm, u0_hbm, i0_hbm, trip_hbm, outu_ref, outi_ref, loss_ref,
           maskv, maskb, adj, csum, crd, crx, cch, invi, racc, rsum, rrecv, invu, trip_ref,
           upan, upart, urecv, ipan, ipart, ird, irx, isum,
           ohp, ohn, ohu, hip, hin, hiu, gpart, gsum, grd, grx, gry, grxy, eu, zbuf,
           in_sems, send_sems, recv_sems):
    users, quarter = maskv.shape[1:]
    own_users = u0_hbm.shape[1]
    sc = ipan.shape[-1]
    home = gpart.shape[-1]
    hh = home // 2
    mh = quarter // NM
    pieces, halves = range(NS), range(2)
    own, core, other, both = range(NQ)
    order = (both, other, core, own)

    z, y, r = lax.axis_index("emb"), lax.axis_index("col"), lax.axis_index("row")
    x, c = r // 2, r % 2
    nz = zbuf.shape[0] // NQ
    slot = z * NQ + r

    def rel(m):
        xx = x if m in (own, core) else 1 - x
        cc = c if m in (own, other) else 1 - c
        return 2 * xx + cc

    dev_d, dev_x, dev_xd = [(z, y, rel(m)) for m in (core, other, both)]
    dev_y, dev_xy = (z, 1 - y, r), (z, 1 - y, rel(other))
    score_devs = [((z + k) % nz, y, rel(m)) for k in range(nz) for m in range(NQ) if k or m]

    cp = Copies(send_sems, recv_sems)
    phase = Phase()
    phase("start")
    loads = []

    def load(src, dst):
        copy = pltpu.make_async_copy(src, dst, in_sems.at[len(loads)])
        copy.start()
        loads.append(copy)
        return copy

    y_off = pl.multiple_of(y * own_users, own_users)
    own_u = pl.ds(y_off, own_users)
    mask_copies, small = {}, []
    for m in order:
        for h in range(NM):
            off = pl.multiple_of(rel(m) * quarter + h * mh, mh)
            mask_copies[m, h] = load(mask_hbm.at[:, pl.ds(off, mh)], maskv.at[m, :, pl.ds(h * mh, mh)])
        if m == both:
            small.append(load(u0_hbm, upan.at[0, :, own_u]))
            small += [load(i0_hbm.at[:, pl.ds(s * sc, sc)], ipan.at[0, own, s]) for s in pieces]
            small.append(load(trip_hbm, trip_ref))

    barrier = pltpu.get_barrier_semaphore()
    for dev in (dev_y, dev_xy, *score_devs):
        pl.semaphore_signal(barrier, inc=1, device_id=dev, device_id_type=MESH)

    racc[...] = jnp.zeros_like(racc)

    def sums(m):
        for h in range(NM):
            mask_copies[m, h].wait()

            def body(j, carry):
                off = pl.multiple_of(h * mh + j * LB, LB)
                tile = h * (mh // LANES) + j * (LB // LANES)
                part = None
                for i in range(users // ROWS):
                    rows = pl.ds(ROWS * i, ROWS)
                    blk = maskv[m, rows, pl.ds(off, LB)]
                    ones = blk.astype(F32).astype(BF16)
                    row = None
                    for g in range(LB // LANES):
                        lanes = slice(LANES * g, LANES * (g + 1))
                        maskb[m, tile + g, rows, :] = ones[:, lanes]
                        row = blk[:, lanes] if row is None else row + blk[:, lanes]
                    racc[rows, :] += row
                    two = blk[:ROWS // 2] + blk[ROWS // 2:]
                    part = two if part is None else part + two
                csum[m, :, pl.ds(off, LB)] = jnp.sum(part.astype(F32), axis=0, keepdims=True)
                return carry
            lax.fori_loop(0, mh // LB, body, 0)

    def one_hot(lanes):
        hit = lax.broadcasted_iota(jnp.int32, (GL, LANES), 0) == lanes
        return jnp.where(hit, 1.0, 0.0).astype(BF16)

    def hot_block(oh, t):
        n = LB // LANES
        return jnp.concatenate([oh[t * n + i] for i in range(n)], axis=1)

    def one_hots(m):
        base = pl.multiple_of(rel(m) * home, home)
        for row, oh, hi in ((1, ohp, hip), (2, ohn, hin)):
            ids = trip_ref[pl.ds(row, 1), pl.ds(base, home)]
            owned = ids // quarter == y * NQ + r
            hi[m] = (ids % quarter) // GL
            low = jnp.where(owned, ids % GL, -1)
            for t in range(home // LANES):
                oh[m, t] = one_hot(low[:, t * LANES:(t + 1) * LANES])

    def user_one_hots():
        base = pl.multiple_of(r * home, home)
        uids = trip_ref[pl.ds(0, 1), pl.ds(base, home)]
        hiu[...] = uids // users
        low = uids % users
        for t in range(home // LANES):
            ohu[t] = one_hot(low[:, t * LANES:(t + 1) * LANES])

    csum_d, csum_x = {}, {}

    def chip_sums(m):
        csum_d[m].wait_recv()
        cch[m] = csum[m] + crd[m]
        csum_x[m ^ other] = cp.send(cch.at[m], crx.at[m ^ other], dev_x, "chip", cch)

    def send_sums(m):
        csum_d[m ^ core] = cp.send(csum.at[m], crd.at[m ^ core], dev_d, "sums", csum)

    phase("sums32")
    sums(both)
    sums(other)
    for copy in small:
        copy.wait()
    phase("barrier")
    pl.semaphore_wait(barrier, 2 + len(score_devs))
    phase("sums10")
    send_sums(both)
    send_sums(other)
    u0_y = cp.send(upan.at[0, :, own_u], upan.at[0, :, own_u], dev_y)
    i0_d = cp.send(ipan.at[0, own], ipan.at[0, core], dev_d)
    sums(core)
    send_sums(core)
    chip_sums(both)
    chip_sums(other)
    sums(own)
    send_sums(own)
    phase("rows")
    rows = jnp.transpose(racc[...].astype(F32), (1, 0))
    rsum[...] = jnp.sum(rows, axis=0, keepdims=True)
    rs_y = cp.send(rsum, rrecv, dev_y)
    chip_sums(core)
    one_hots(both)
    phase("chip0")
    chip_sums(own)
    i0_x = cp.send(ipan.at[0, own], ipan.at[0, other], dev_x)
    phase("onehots")
    one_hots(other)
    one_hots(core)
    phase("rs_wait")
    u0_y.wait_recv()
    rs_y.wait_recv()
    inv_row = lax.rsqrt(jnp.maximum(rsum[...] + rrecv[...], 1.0))
    invu[...] = jnp.transpose(jnp.broadcast_to(inv_row, (LANES, users)), (1, 0))
    phase("cx_wait")
    for m in order:
        csum_x[m].wait_recv()
        invi[m] = lax.rsqrt(jnp.maximum(cch[m] + crx[m], 1.0))

    tiles = sc // LANES

    def build(m, s):
        for tile in range(s * tiles, (s + 1) * tiles):
            scale = (invu[...] * invi[m, :, tile * LANES:(tile + 1) * LANES]).astype(BF16)
            adj[m, tile] = scale * maskb[m, tile]

    def block(m, s, n, rows):
        return jnp.concatenate([adj[m, t, rows, :] for t in range(s * tiles, (s + n) * tiles)], axis=1)

    def items(k, m, some=pieces):
        for s in some:
            ipart[k, m, s] = jnp.dot(upan[k], block(m, s, 1, slice(0, users)), preferred_element_type=F32)

    def user_part(k, m, acc=None, s=0, n=NS):
        table = jnp.concatenate([ipan[k, m, s + i] for i in range(n)], axis=1)
        out = []
        for h in halves:
            part = lax.dot_general(
                table, block(m, s, n, slice(h * own_users, (h + 1) * own_users)),
                (((1,), (1,)), ((), ())), preferred_element_type=F32)
            out.append(part if acc is None else acc[h] + part)
        return out

    d, xs, g, gd, f = {}, {}, {}, {}, {}

    def core_send(k, s):
        d[k, s] = cp.send(ipart.at[k, both, s], ird.at[k, 1, s], dev_d, ("core", k), ipart.at[k, both])

    def core_send_own(k):
        d[k] = cp.send(ipart.at[k, core], ird.at[k, 0], dev_d)

    def x_send(k, s):
        d[k, s].wait_recv()
        isum[k, s] = ipart[k, other, s] + ird[k, 1, s]
        xs[k, s] = cp.send(isum.at[k, s], irx.at[k, s], dev_x, ("x", k), isum.at[k])

    def own_piece(k, s):
        if s == 0:
            d[k].wait_recv()
        xs[k, s].wait_recv()
        total = (ipart[k, own, s] + ird[k, 0, s]) + irx[k, s]
        ipan[k + 1, own, s] = total.astype(BF16)

    def own_gather(k, s):
        own_piece(k, s)
        g[k + 1, s] = cp.send(
            ipan.at[k + 1, own, s], ipan.at[k + 1, other, s], dev_x, ("gather", k), ipan.at[k + 1, own])
        if s == NS - 1:
            gd[k + 1] = cp.send(ipan.at[k + 1, own], ipan.at[k + 1, core], dev_d)

    def forward(k, s):
        g[k, s].wait_recv()
        f[k, s] = cp.send(ipan.at[k, other, s], ipan.at[k, both, s], dev_d, ("forward", k), ipan.at[k, other])

    def send_user(k, acc):
        for h in halves:
            upart[k, :, h * own_users:(h + 1) * own_users] = acc[h]
        return cp.send(upart.at[k], urecv.at[k], dev_y)

    def take_user(k, got):
        got.wait_recv()
        upan[k + 1] = (upart[k] + urecv[k]).astype(BF16)

    last = NS - 1
    phase("build32")
    for s in pieces:
        build(both, s)
        items(0, both, [s])
        build(other, s)
        core_send(0, s)
        items(0, other, [s])
        if s > 1:
            x_send(0, s - 2)
    phase("build10")
    for s in pieces:
        build(core, s)
        if s in (1, last):
            x_send(0, NS - 2 + s // 2)
    for s in pieces:
        build(own, s)
    phase("i0_x_wait")
    i0_x.wait_recv()
    i0_f = cp.send(ipan.at[0, other], ipan.at[0, both], dev_d)
    phase("upart0")
    i0_d.wait_recv()
    acc = user_part(0, core, user_part(0, own))
    acc = user_part(0, other, acc)
    phase("upart0b")
    i0_f.wait_recv()
    acc = user_part(0, both, acc)
    u1 = send_user(0, acc)
    phase("items1_10")
    items(0, core)
    core_send_own(0)
    items(0, own)
    one_hots(own)
    user_one_hots()
    for s in range(last):
        phase(f"own1_{s}")
        own_gather(0, s)
    phase("u1_wait")
    take_user(0, u1)

    def items_x(k):
        items(k, both)
        items(k, other, [0])
        for s in pieces:
            core_send(k, s)
        items(k, other, range(1, NS))

    phase("items2_32")
    items_x(1)
    phase("own1_last")
    own_gather(0, last)
    phase("items2_10")
    items(1, core)
    core_send_own(1)
    items(1, own)
    phase("x2")
    for s in pieces:
        x_send(1, s)
    phase("fwd1_0")
    forward(1, 0)
    acc = user_part(1, own)
    phase("fwd1_1")
    forward(1, 1)
    gd[1].wait_recv()
    acc = user_part(1, core, acc)
    phase("fwd1_2")
    forward(1, 2)
    acc = user_part(1, other, acc, 0, last)
    phase("fwd1_3")
    forward(1, last)
    acc = user_part(1, other, acc, last, 1)
    for s in range(last):
        f[1, s].wait_recv()
    acc = user_part(1, both, acc, 0, last)
    phase("f1_wait")
    f[1, last].wait_recv()
    acc = user_part(1, both, acc, last, 1)
    u2 = send_user(1, acc)
    phase("own2_01")
    own_gather(1, 0)
    own_gather(1, 1)
    phase("u2_wait")
    take_user(1, u2)
    phase("items3_32")
    items_x(2)
    items(2, core)
    phase("x3")
    x_send(2, 0)
    core_send_own(2)
    phase("own2_2")
    own_gather(1, 2)
    phase("own2_3")
    own_gather(1, last)
    for s in range(1, NS):
        x_send(2, s)
    phase("items3_own")
    items(2, own)
    phase("upart2_01")
    acc = user_part(2, own)
    gd[2].wait_recv()
    acc = user_part(2, core, acc)
    phase("fwd2_01")
    for s in halves:
        forward(2, s)
    acc = user_part(2, other, acc, 0, 2)
    for s in halves:
        f[2, s].wait_recv()
    acc = user_part(2, both, acc, 0, 2)
    phase("fwd2_23")
    for s in (2, last):
        forward(2, s)
    acc = user_part(2, other, acc, 2, NS - 2)
    phase("f2_wait")
    for s in (2, last):
        f[2, s].wait_recv()
    acc = user_part(2, both, acc, 2, NS - 2)
    u3 = send_user(2, acc)

    def mean4(a, b, e, h):
        tot = ((a.astype(F32) + b.astype(F32)) + e.astype(F32)) + h.astype(F32)
        return (tot * (1.0 / (NUM_LAYERS + 1))).astype(BF16)

    def pick(tab, oh, hi, first):
        got = jnp.dot(tab, oh, preferred_element_type=F32)
        n = got.shape[0] // ROWS
        out = jnp.where(hi == first, got[:ROWS], 0.0)
        for i in range(1, n):
            out = out + jnp.where(hi == first + i, got[i * ROWS:(i + 1) * ROWS], 0.0)
        return out

    def final_piece(s):
        own_piece(2, s)
        outi_ref[:, s * sc:(s + 1) * sc] = mean4(*[ipan[k, own, s] for k in range(NUM_LAYERS + 1)])

    half = [pl.ds(h * hh, hh) for h in halves]

    def differences(m, h, first, n):
        groups = range(first * sc // GL, (first + n) * sc // GL)
        table = jnp.concatenate([outi_ref[:, i * GL:(i + 1) * GL] for i in groups], axis=0)
        for t in range(h * (hh // LB), (h + 1) * (hh // LB)):
            sl = slice(t * LB, (t + 1) * LB)
            pos = pick(table, hot_block(ohp.at[m], t), hip[m, :, sl], groups[0])
            neg = pick(table, hot_block(ohn.at[m], t), hin[m, :, sl], groups[0])
            gpart[m, :, sl] = pos - neg if first == 0 else (gpart[m, :, sl] + pos) - neg

    phase("own3")
    for s in range(last):
        final_piece(s)
    phase("diff_012")
    for m in order:
        for h in halves:
            differences(m, h, 0, last)
    phase("u3_wait")
    take_user(2, u3)
    phase("finalu")
    eu[own] = mean4(*[upan[k] for k in range(NUM_LAYERS + 1)])
    others = eu.at[pl.ds(core, NQ - 1)]
    eu_sem = cp.recv_sem()
    for m, dev in ((core, dev_d), (other, dev_x), (both, dev_xd)):
        cp.send(eu.at[own], eu.at[m], dev, "eu", others, eu_sem)
    outu_ref[...] = eu[own, :, own_u]

    phase("own3_last")
    final_piece(last)
    gd3, gx, gxy = {}, {}, {}
    phase("diff3")
    for h in halves:
        differences(both, h, last, 1)
        gd3[h] = cp.send(gpart.at[both, :, half[h]], grd.at[1, :, half[h]], dev_d)
    for h in halves:
        differences(other, h, last, 1)
    for h in halves:
        differences(core, h, last, 1)
    gd1 = cp.send(gpart.at[core], grd.at[0], dev_d)
    phase("gd3_wait")
    for h in halves:
        gd3[h].wait_recv()
        gsum[1, :, half[h]] = gpart[other, :, half[h]] + grd[1, :, half[h]]
        gx[h] = cp.send(gsum.at[1, :, half[h]], grx.at[:, half[h]], dev_x)
        gxy[h] = cp.send(gsum.at[1, :, half[h]], grxy.at[:, half[h]], dev_xy)
    phase("diff0")
    for h in halves:
        differences(own, h, last, 1)
    phase("gd1_wait")
    gd1.wait_recv()
    gsum[0] = gpart[own] + grd[0]
    gy = cp.send(gsum.at[0], gry, dev_y)
    phase("e_wait")
    wait_bytes(others, eu_sem)
    phase("picku")
    utab = jnp.concatenate([eu[m] for m in range(NQ)], axis=0)
    place = jnp.where(hiu[...] // 2 == x, own, other) + jnp.where(hiu[...] % 2 == c, own, core)
    picked = [pick(utab, hot_block(ohu, t), place[:, t * LB:(t + 1) * LB], own) for t in range(home // LB)]
    phase("gy_wait")
    gy.wait_recv()
    for h in halves:
        gx[h].wait_recv()
        gxy[h].wait_recv()
    phase("dot")
    for t in range(home // LB):
        sl = slice(t * LB, (t + 1) * LB)
        diff = (gsum[0, :, sl] + grx[:, sl]) + (gry[:, sl] + grxy[:, sl])
        zbuf[slot, :, sl] = jnp.sum(picked[t] * diff, axis=0, keepdims=True)
    rest = zbuf.at[pl.ds(0, len(score_devs))]
    z_sem = cp.recv_sem()
    for dev in score_devs:
        cp.send(zbuf.at[slot], zbuf.at[slot], dev, "score", rest, z_sem)
    phase("z_wait")
    wait_bytes(rest, z_sem)
    phase("loss")
    for q in range(NQ):
        neg = -sum(zbuf[k * NQ + q] for k in range(nz))
        loss_ref[q] = jnp.maximum(neg, 0.0) + jnp.log1p(jnp.exp(-jnp.abs(neg)))
    phase("drain")
    cp.drain()
    phase(None)
    assert (len(cp.groups) + len(cp.single), cp.recvs, len(loads)) == (NUM_SENDS, NUM_RECVS, NUM_LOADS)


def emit(*refs):
    n = len(refs) // 2
    sems = refs[-1]
    copies = [pltpu.make_async_copy(src, dst, sems.at[i]) for i, (src, dst) in enumerate(zip(refs[:n], refs[n:]))]
    for copy in copies:
        copy.start()
    for copy in copies:
        copy.wait()


def solution(mesh):
    def local_fn(mask_blk, user_sh, item_sh, triples):
        users, items = mask_blk.shape
        cols, own_users = user_sh.shape[1], user_sh.shape[0]
        quarter = items // NQ
        home = triples.shape[0] // NQ
        vm, sem = pltpu.VMEM, pltpu.SemaphoreType.DMA
        nl = NUM_LAYERS
        sc = quarter // NS
        tiles = (NQ, quarter // LANES, users, LANES)
        per_item, hots = (NQ, 1, quarter), (NQ, home // LANES, GL, LANES)
        triple_row = (NQ, 1, home)
        scratch = [
            vm((NQ, users, quarter), jnp.int32), vm(tiles, BF16), vm(tiles, BF16),
            *[vm(per_item, F32)] * 5,
            vm((users, LANES), jnp.int32), vm((1, users), F32), vm((1, users), F32), vm((users, LANES), F32),
            vm(triples.shape[::-1], jnp.int32),
            vm((nl + 1, cols, users), BF16), vm((nl, cols, users), F32), vm((nl, cols, users), F32),
            vm((nl + 1, NQ, NS, cols, sc), BF16), vm((nl, NQ, NS, cols, sc), F32),
            vm((nl, 2, NS, cols, sc), F32), vm((nl, NS, cols, sc), F32), vm((nl, NS, cols, sc), F32),
            vm(hots, BF16), vm(hots, BF16), vm(hots[1:], BF16),
            vm(triple_row, jnp.int32), vm(triple_row, jnp.int32), vm(triple_row[1:], jnp.int32),
            vm((NQ, cols, home), F32), vm((2, cols, home), F32), vm((2, cols, home), F32),
            *[vm((cols, home), F32)] * 3,
            vm((NQ, cols, users), BF16), vm((mesh.shape["emb"] * NQ, 1, home), F32),
            sem((NUM_LOADS,)), sem((NUM_SENDS,)), sem((NUM_RECVS,)),
        ]
        vspec = pl.BlockSpec(memory_space=pltpu.VMEM)
        out_u, out_i, loss = pl.pallas_call(
            kernel,
            out_shape=[
                jax.ShapeDtypeStruct((cols, own_users), BF16),
                jax.ShapeDtypeStruct((cols, quarter), BF16),
                jax.ShapeDtypeStruct((NQ, 1, home), F32)],
            in_specs=[pl.BlockSpec(memory_space=pltpu.HBM)] * 4,
            out_specs=[vspec, vspec, vspec],
            scratch_shapes=scratch,
            compiler_params=pltpu.CompilerParams(
                collective_id=0, has_side_effects=True, vmem_limit_bytes=VMEM_LIMIT),
        )(*[pltpu.with_memory_space_constraint(a, pltpu.HBM) for a in (mask_blk, user_sh.T, item_sh.T, triples.T)])
        out_u, out_i, loss = pl.pallas_call(
            emit,
            out_shape=[jax.ShapeDtypeStruct(a.shape, a.dtype) for a in (out_u, out_i, loss)],
            in_specs=[vspec] * 3, out_specs=[pl.BlockSpec(memory_space=pltpu.HBM)] * 3,
            scratch_shapes=[sem((3,))],
            compiler_params=pltpu.CompilerParams(vmem_limit_bytes=2 ** 20),
        )(out_u, out_i, loss)
        return out_u.T, out_i.T, loss.reshape(-1)

    return jax.shard_map(
        local_fn, mesh=mesh,
        in_specs=(P("row", "col"), P(("row", "col"), "emb"), P(("col", "row"), "emb"), P()),
        out_specs=(P(("row", "col"), "emb"), P(("col", "row"), "emb"), P()),
        check_vma=False)
```

```python
import functools

import jax
import jax.numpy as jnp
from jax import lax
from jax.experimental import pallas as pl
from jax.experimental.pallas import tpu as pltpu
from jax.sharding import PartitionSpec as P

NUM_LAYERS = 3
MESH = pl.DeviceIdType.MESH
F32 = jnp.float32
BF16 = jnp.bfloat16

NY = 2
NQ = 4
NM = 2
NS = 4
LB = 256
GL = 256
LANES = 128
ROWS = 16


class Copies:
    def __init__(self, send_sems, recv_sems):
        self.send_sems, self.recv_sems = send_sems, recv_sems
        self.recvs, self.groups, self.single = 0, {}, []

    def recv_sem(self):
        self.recvs += 1
        return self.recv_sems.at[self.recvs - 1]

    def send(self, src, dst, device, group=None, whole=None, recv_sem=None):
        count = len(self.groups) + len(self.single)
        if group is None:
            sem = self.send_sems.at[count]
        else:
            if group not in self.groups:
                self.groups[group] = (self.send_sems.at[count], whole)
            sem = self.groups[group][0]
        copy = pltpu.make_async_remote_copy(
            src_ref=src, dst_ref=dst, send_sem=sem,
            recv_sem=self.recv_sem() if recv_sem is None else recv_sem,
            device_id=device, device_id_type=MESH)
        copy.start()
        if group is None:
            self.single.append(copy)
        return copy

    def drain(self):
        for copy in self.single:
            copy.wait_send()
        for sem, whole in self.groups.values():
            wait_bytes(whole, sem)


def wait_bytes(ref, sem):
    pltpu.make_async_copy(ref, ref, sem).wait()


VMEM_LIMIT = 52 * 2 ** 20
NUM_SENDS = 33
NUM_RECVS = 69
NUM_LOADS = NQ * NM + NS + 2


class Phase:
    def __init__(self):
        self.current = None

    def __call__(self, name):
        if self.current is not None:
            self.current.__exit__(None, None, None)
        self.current = None
        if name:
            self.current = jax.named_scope(name)
            self.current.__enter__()


def kernel(mask_hbm, u0_hbm, i0_hbm, trip_hbm, outu_ref, outi_ref, loss_ref,
           maskv, maskb, adj, csum, crd, crx, cch, invi, racc, rsum, rrecv, invu, trip_ref,
           upan, upart, urecv, ipan, ipart, ird, irx, isum,
           ohp, ohn, ohu, hip, hin, hiu, gpart, gsum, grd, grx, eu, zbuf,
           in_sems, send_sems, recv_sems):
    users, quarter = maskv.shape[1:]
    own_users = u0_hbm.shape[1]
    sc = ipan.shape[-1]
    hh = gpart.shape[-1]
    home = NY * hh
    mh = quarter // NM
    pieces, halves = range(NS), range(2)
    own, core, other, both = range(NQ)
    order = (both, other, core, own)

    z, y, r = lax.axis_index("emb"), lax.axis_index("col"), lax.axis_index("row")
    x, c = r // 2, r % 2
    nz = zbuf.shape[0] // (NQ * NY)
    slot = (z * NQ + r) * NY + y

    def rel(m):
        xx = x if m in (own, core) else 1 - x
        cc = c if m in (own, other) else 1 - c
        return 2 * xx + cc

    dev_d, dev_x, dev_xd = [(z, y, rel(m)) for m in (core, other, both)]
    dev_y, dev_xy = (z, 1 - y, r), (z, 1 - y, rel(other))
    score_devs = [((z + k) % nz, yy, rel(m)) for k in range(nz) for yy in (y, 1 - y) for m in range(NQ)][1:]

    cp = Copies(send_sems, recv_sems)
    phase = Phase()
    phase("start")
    loads = []

    def load(src, dst):
        copy = pltpu.make_async_copy(src, dst, in_sems.at[len(loads)])
        copy.start()
        loads.append(copy)
        return copy

    y_off = pl.multiple_of(y * own_users, own_users)
    own_u = pl.ds(y_off, own_users)
    mask_copies, small = {}, []
    for m in order:
        for h in range(NM):
            off = pl.multiple_of(rel(m) * quarter + h * mh, mh)
            mask_copies[m, h] = load(mask_hbm.at[:, pl.ds(off, mh)], maskv.at[m, :, pl.ds(h * mh, mh)])
        if m == both:
            small.append(load(u0_hbm, upan.at[0, :, own_u]))
            small += [load(i0_hbm.at[:, pl.ds(s * sc, sc)], ipan.at[0, own, s]) for s in pieces]
            small.append(load(trip_hbm, trip_ref))

    barrier = pltpu.get_barrier_semaphore()
    for dev in score_devs:
        pl.semaphore_signal(barrier, inc=1, device_id=dev, device_id_type=MESH)

    racc[...] = jnp.zeros_like(racc)

    def sums(m):
        for h in range(NM):
            mask_copies[m, h].wait()

            def body(j, carry):
                off = pl.multiple_of(h * mh + j * LB, LB)
                tile = h * (mh // LANES) + j * (LB // LANES)
                part = None
                for i in range(users // ROWS):
                    rows = pl.ds(ROWS * i, ROWS)
                    blk = maskv[m, rows, pl.ds(off, LB)]
                    ones = blk.astype(F32).astype(BF16)
                    row = None
                    for g in range(LB // LANES):
                        lanes = slice(LANES * g, LANES * (g + 1))
                        maskb[m, tile + g, rows, :] = ones[:, lanes]
                        row = blk[:, lanes] if row is None else row + blk[:, lanes]
                    racc[rows, :] += row
                    two = blk[:ROWS // 2] + blk[ROWS // 2:]
                    part = two if part is None else part + two
                csum[m, :, pl.ds(off, LB)] = jnp.sum(part.astype(F32), axis=0, keepdims=True)
                return carry
            lax.fori_loop(0, mh // LB, body, 0)

    def one_hot(lanes):
        hit = lax.broadcasted_iota(jnp.int32, (GL, LANES), 0) == lanes
        return jnp.where(hit, 1.0, 0.0).astype(BF16)

    def hot_block(oh, t):
        n = LB // LANES
        return jnp.concatenate([oh[t * n + i] for i in range(n)], axis=1)

    def one_hots(m):
        base = pl.multiple_of(rel(m) * home, home)
        for row, oh, hi in ((1, ohp, hip), (2, ohn, hin)):
            ids = trip_ref[pl.ds(row, 1), pl.ds(base, home)]
            owned = ids // quarter == y * NQ + r
            hi[m] = (ids % quarter) // GL
            low = jnp.where(owned, ids % GL, -1)
            for t in range(home // LANES):
                oh[m, t] = one_hot(low[:, t * LANES:(t + 1) * LANES])

    def user_one_hots():
        base = pl.multiple_of((r * NY + y) * hh, hh)
        uids = trip_ref[pl.ds(0, 1), pl.ds(base, hh)]
        hiu[...] = uids // users
        low = uids % users
        for t in range(hh // LANES):
            ohu[t] = one_hot(low[:, t * LANES:(t + 1) * LANES])

    csum_d, csum_x = {}, {}

    def chip_sums(m):
        csum_d[m].wait_recv()
        cch[m] = csum[m] + crd[m]
        csum_x[m ^ other] = cp.send(cch.at[m], crx.at[m ^ other], dev_x, "chip", cch)

    def send_sums(m):
        csum_d[m ^ core] = cp.send(csum.at[m], crd.at[m ^ core], dev_d, "sums", csum)

    phase("sums32")
    sums(both)
    sums(other)
    for copy in small:
        copy.wait()
    phase("barrier")
    pl.semaphore_wait(barrier, len(score_devs))
    phase("sums10")
    send_sums(both)
    send_sums(other)
    u0_y = cp.send(upan.at[0, :, own_u], upan.at[0, :, own_u], dev_y)
    i0_d = cp.send(ipan.at[0, own], ipan.at[0, core], dev_d)
    sums(core)
    send_sums(core)
    chip_sums(both)
    chip_sums(other)
    sums(own)
    send_sums(own)
    phase("rows")
    rows = jnp.transpose(racc[...].astype(F32), (1, 0))
    rsum[...] = jnp.sum(rows, axis=0, keepdims=True)
    rs_y = cp.send(rsum, rrecv, dev_y)
    chip_sums(core)
    one_hots(both)
    phase("chip0")
    chip_sums(own)
    i0_x = cp.send(ipan.at[0, own], ipan.at[0, other], dev_x)
    phase("onehots")
    one_hots(other)
    one_hots(core)
    phase("rs_wait")
    u0_y.wait_recv()
    rs_y.wait_recv()
    inv_row = lax.rsqrt(jnp.maximum(rsum[...] + rrecv[...], 1.0))
    invu[...] = jnp.transpose(jnp.broadcast_to(inv_row, (LANES, users)), (1, 0))
    phase("cx_wait")
    for m in order:
        csum_x[m].wait_recv()
        invi[m] = lax.rsqrt(jnp.maximum(cch[m] + crx[m], 1.0))

    tiles = sc // LANES

    def build(m, s):
        for tile in range(s * tiles, (s + 1) * tiles):
            scale = (invu[...] * invi[m, :, tile * LANES:(tile + 1) * LANES]).astype(BF16)
            adj[m, tile] = scale * maskb[m, tile]

    def block(m, s, n, rows):
        return jnp.concatenate([adj[m, t, rows, :] for t in range(s * tiles, (s + n) * tiles)], axis=1)

    def items(k, m, some=pieces):
        for s in some:
            ipart[k, m, s] = jnp.dot(upan[k], block(m, s, 1, slice(0, users)), preferred_element_type=F32)

    def user_part(k, m, acc=None, s=0, n=NS):
        table = jnp.concatenate([ipan[k, m, s + i] for i in range(n)], axis=1)
        out = []
        for h in halves:
            part = lax.dot_general(
                table, block(m, s, n, slice(h * own_users, (h + 1) * own_users)),
                (((1,), (1,)), ((), ())), preferred_element_type=F32)
            out.append(part if acc is None else acc[h] + part)
        return out

    d, xs, g, gd, f = {}, {}, {}, {}, {}

    def core_send(k, s):
        d[k, s] = cp.send(ipart.at[k, both, s], ird.at[k, 1, s], dev_d, ("core", k), ipart.at[k, both])

    def core_send_own(k):
        d[k] = cp.send(ipart.at[k, core], ird.at[k, 0], dev_d)

    def x_send(k, s):
        d[k, s].wait_recv()
        isum[k, s] = ipart[k, other, s] + ird[k, 1, s]
        xs[k, s] = cp.send(isum.at[k, s], irx.at[k, s], dev_x, ("x", k), isum.at[k])

    def own_piece(k, s):
        if s == 0:
            d[k].wait_recv()
        xs[k, s].wait_recv()
        total = (ipart[k, own, s] + ird[k, 0, s]) + irx[k, s]
        ipan[k + 1, own, s] = total.astype(BF16)

    def own_gather(k, s):
        own_piece(k, s)
        g[k + 1, s] = cp.send(
            ipan.at[k + 1, own, s], ipan.at[k + 1, other, s], dev_x, ("gather", k), ipan.at[k + 1, own])
        if s == NS - 1:
            gd[k + 1] = cp.send(ipan.at[k + 1, own], ipan.at[k + 1, core], dev_d)

    def forward(k, s):
        g[k, s].wait_recv()
        f[k, s] = cp.send(ipan.at[k, other, s], ipan.at[k, both, s], dev_d, ("forward", k), ipan.at[k, other])

    def send_user(k, acc):
        for h in halves:
            upart[k, :, h * own_users:(h + 1) * own_users] = acc[h]
        return cp.send(upart.at[k], urecv.at[k], dev_y)

    def take_user(k, got):
        got.wait_recv()
        upan[k + 1] = (upart[k] + urecv[k]).astype(BF16)

    last = NS - 1
    phase("build32")
    for s in pieces:
        build(both, s)
        items(0, both, [s])
        build(other, s)
        core_send(0, s)
        items(0, other, [s])
        if s > 1:
            x_send(0, s - 2)
    phase("build10")
    for s in pieces:
        build(core, s)
        if s in (1, last):
            x_send(0, NS - 2 + s // 2)
    for s in pieces:
        build(own, s)
    phase("i0_x_wait")
    i0_x.wait_recv()
    i0_f = cp.send(ipan.at[0, other], ipan.at[0, both], dev_d)
    phase("upart0")
    i0_d.wait_recv()
    acc = user_part(0, core, user_part(0, own))
    acc = user_part(0, other, acc)
    phase("upart0b")
    i0_f.wait_recv()
    acc = user_part(0, both, acc)
    u1 = send_user(0, acc)
    phase("items1_10")
    items(0, core)
    core_send_own(0)
    items(0, own)
    one_hots(own)
    user_one_hots()
    for s in range(last):
        phase(f"own1_{s}")
        own_gather(0, s)
    phase("u1_wait")
    take_user(0, u1)

    def items_x(k):
        items(k, both)
        items(k, other, [0])
        for s in pieces:
            core_send(k, s)
        items(k, other, range(1, NS))

    phase("items2_32")
    items_x(1)
    phase("own1_last")
    own_gather(0, last)
    phase("items2_10")
    items(1, core)
    core_send_own(1)
    items(1, own)
    phase("x2")
    for s in pieces:
        x_send(1, s)
    phase("fwd1_0")
    forward(1, 0)
    acc = user_part(1, own)
    phase("fwd1_1")
    forward(1, 1)
    gd[1].wait_recv()
    acc = user_part(1, core, acc)
    phase("fwd1_2")
    forward(1, 2)
    acc = user_part(1, other, acc, 0, last)
    phase("fwd1_3")
    forward(1, last)
    acc = user_part(1, other, acc, last, 1)
    for s in range(last):
        f[1, s].wait_recv()
    acc = user_part(1, both, acc, 0, last)
    phase("f1_wait")
    f[1, last].wait_recv()
    acc = user_part(1, both, acc, last, 1)
    u2 = send_user(1, acc)
    phase("own2_01")
    own_gather(1, 0)
    own_gather(1, 1)
    phase("u2_wait")
    take_user(1, u2)
    phase("items3_32")
    items_x(2)
    items(2, core)
    phase("x3")
    x_send(2, 0)
    core_send_own(2)
    phase("own2_2")
    own_gather(1, 2)
    phase("own2_3")
    own_gather(1, last)
    for s in range(1, NS):
        x_send(2, s)
    phase("items3_own")
    items(2, own)
    phase("upart2_01")
    acc = user_part(2, own)
    gd[2].wait_recv()
    acc = user_part(2, core, acc)
    phase("fwd2_01")
    for s in halves:
        forward(2, s)
    acc = user_part(2, other, acc, 0, 2)
    for s in halves:
        f[2, s].wait_recv()
    acc = user_part(2, both, acc, 0, 2)
    phase("fwd2_23")
    for s in (2, last):
        forward(2, s)
    acc = user_part(2, other, acc, 2, NS - 2)
    phase("f2_wait")
    for s in (2, last):
        f[2, s].wait_recv()
    acc = user_part(2, both, acc, 2, NS - 2)
    u3 = send_user(2, acc)

    def mean4(a, b, e, h):
        tot = ((a.astype(F32) + b.astype(F32)) + e.astype(F32)) + h.astype(F32)
        return (tot * (1.0 / (NUM_LAYERS + 1))).astype(BF16)

    def pick(tab, oh, hi, first):
        got = jnp.dot(tab, oh, preferred_element_type=F32)
        n = got.shape[0] // ROWS
        out = jnp.where(hi == first, got[:ROWS], 0.0)
        for i in range(1, n):
            out = out + jnp.where(hi == first + i, got[i * ROWS:(i + 1) * ROWS], 0.0)
        return out

    def final_piece(s):
        own_piece(2, s)
        outi_ref[:, s * sc:(s + 1) * sc] = mean4(*[ipan[k, own, s] for k in range(NUM_LAYERS + 1)])

    def differences(m, h, first, n):
        groups = range(first * sc // GL, (first + n) * sc // GL)
        table = jnp.concatenate([outi_ref[:, i * GL:(i + 1) * GL] for i in groups], axis=0)
        for t in range(h * (hh // LB), (h + 1) * (hh // LB)):
            sl = slice(t * LB, (t + 1) * LB)
            pos = pick(table, hot_block(ohp.at[m], t), hip[m, :, sl], groups[0])
            neg = pick(table, hot_block(ohn.at[m], t), hin[m, :, sl], groups[0])
            out = slice(t * LB - h * hh, (t + 1) * LB - h * hh)
            gpart[m, h, :, out] = pos - neg if first == 0 else (gpart[m, h, :, out] + pos) - neg

    phase("own3")
    for s in range(last):
        final_piece(s)
    phase("diff_012")
    for m in order:
        for h in halves:
            differences(m, h, 0, last)
    phase("u3_wait")
    take_user(2, u3)
    phase("finalu")
    eu[own] = mean4(*[upan[k] for k in range(NUM_LAYERS + 1)])
    others = eu.at[pl.ds(core, NQ - 1)]
    eu_sem = cp.recv_sem()
    for m, dev in ((core, dev_d), (other, dev_x), (both, dev_xd)):
        cp.send(eu.at[own], eu.at[m], dev, "eu", others, eu_sem)
    outu_ref[...] = eu[own, :, own_u]

    phase("own3_last")
    final_piece(last)
    gd3 = {}
    phase("diff3")
    for h in halves:
        differences(both, h, last, 1)
        gd3[h] = cp.send(gpart.at[both, h], grd.at[1, h], dev_d)
    for h in halves:
        differences(other, h, last, 1)
    for h in halves:
        differences(core, h, last, 1)
    gd1 = cp.send(gpart.at[core], grd.at[0], dev_d)
    phase("gd3_wait")
    for h in halves:
        gd3[h].wait_recv()

    def home_send(i, m, h, dev):
        gsum[i] = gpart[m, h] + grd[m // 2, h]
        return cp.send(gsum.at[i], grx.at[i], dev)

    gx = [home_send(0, other, 1 - y, dev_xy), home_send(1, other, y, dev_x)]
    phase("diff0")
    for h in halves:
        differences(own, h, last, 1)
    phase("gd1_wait")
    gd1.wait_recv()
    gx.append(home_send(2, own, 1 - y, dev_y))
    phase("e_wait")
    wait_bytes(others, eu_sem)
    phase("picku")
    utab = jnp.concatenate([eu[m] for m in range(NQ)], axis=0)
    place = jnp.where(hiu[...] // 2 == x, own, other) + jnp.where(hiu[...] % 2 == c, own, core)
    picked = [pick(utab, hot_block(ohu, t), place[:, t * LB:(t + 1) * LB], own) for t in range(hh // LB)]
    phase("gy_wait")
    for copy in gx:
        copy.wait_recv()
    phase("dot")
    for t in range(hh // LB):
        sl = slice(t * LB, (t + 1) * LB)
        mine = gpart[own, y, :, sl] + grd[0, y, :, sl]
        diff = (mine + grx[1, :, sl]) + (grx[2, :, sl] + grx[0, :, sl])
        zbuf[slot, :, sl] = jnp.sum(picked[t] * diff, axis=0, keepdims=True)
    rest = zbuf.at[pl.ds(0, len(score_devs))]
    z_sem = cp.recv_sem()
    for dev in score_devs:
        cp.send(zbuf.at[slot], zbuf.at[slot], dev, "score", rest, z_sem)
    phase("z_wait")
    wait_bytes(rest, z_sem)
    phase("loss")
    for q in range(NQ * NY):
        neg = -sum(zbuf[k * NQ * NY + q] for k in range(nz))
        loss_ref[q] = jnp.maximum(neg, 0.0) + jnp.log1p(jnp.exp(-jnp.abs(neg)))
    phase("drain")
    cp.drain()
    phase(None)
    assert (len(cp.groups) + len(cp.single), cp.recvs, len(loads)) == (NUM_SENDS, NUM_RECVS, NUM_LOADS)


def emit(*refs):
    n = len(refs) // 2
    sems = refs[-1]
    copies = [pltpu.make_async_copy(src, dst, sems.at[i]) for i, (src, dst) in enumerate(zip(refs[:n], refs[n:]))]
    for copy in copies:
        copy.start()
    for copy in copies:
        copy.wait()


def solution(mesh):
    def local_fn(mask_blk, user_sh, item_sh, triples):
        users, items = mask_blk.shape
        cols, own_users = user_sh.shape[1], user_sh.shape[0]
        quarter = items // NQ
        home = triples.shape[0] // NQ
        hh = home // NY
        vm, sem = pltpu.VMEM, pltpu.SemaphoreType.DMA
        nl = NUM_LAYERS
        sc = quarter // NS
        tiles = (NQ, quarter // LANES, users, LANES)
        per_item, hots = (NQ, 1, quarter), (NQ, home // LANES, GL, LANES)
        triple_row = (NQ, 1, home)
        scratch = [
            vm((NQ, users, quarter), jnp.int32), vm(tiles, BF16), vm(tiles, BF16),
            *[vm(per_item, F32)] * 5,
            vm((users, LANES), jnp.int32), vm((1, users), F32), vm((1, users), F32), vm((users, LANES), F32),
            vm(triples.shape[::-1], jnp.int32),
            vm((nl + 1, cols, users), BF16), vm((nl, cols, users), F32), vm((nl, cols, users), F32),
            vm((nl + 1, NQ, NS, cols, sc), BF16), vm((nl, NQ, NS, cols, sc), F32),
            vm((nl, 2, NS, cols, sc), F32), vm((nl, NS, cols, sc), F32), vm((nl, NS, cols, sc), F32),
            vm(hots, BF16), vm(hots, BF16), vm((hh // LANES, GL, LANES), BF16),
            vm(triple_row, jnp.int32), vm(triple_row, jnp.int32), vm((1, hh), jnp.int32),
            vm((NQ, NY, cols, hh), F32), vm((3, cols, hh), F32), vm((2, NY, cols, hh), F32), vm((3, cols, hh), F32),
            vm((NQ, cols, users), BF16), vm((mesh.size, 1, hh), F32),
            sem((NUM_LOADS,)), sem((NUM_SENDS,)), sem((NUM_RECVS,)),
        ]
        vspec = pl.BlockSpec(memory_space=pltpu.VMEM)
        out_u, out_i, loss = pl.pallas_call(
            kernel,
            out_shape=[
                jax.ShapeDtypeStruct((cols, own_users), BF16),
                jax.ShapeDtypeStruct((cols, quarter), BF16),
                jax.ShapeDtypeStruct((NQ * NY, 1, hh), F32)],
            in_specs=[pl.BlockSpec(memory_space=pltpu.HBM)] * 4,
            out_specs=[vspec, vspec, vspec],
            scratch_shapes=scratch,
            compiler_params=pltpu.CompilerParams(
                collective_id=0, has_side_effects=True, vmem_limit_bytes=VMEM_LIMIT),
        )(*[pltpu.with_memory_space_constraint(a, pltpu.HBM) for a in (mask_blk, user_sh.T, item_sh.T, triples.T)])
        out_u, out_i, loss = pl.pallas_call(
            emit,
            out_shape=[jax.ShapeDtypeStruct(a.shape, a.dtype) for a in (out_u, out_i, loss)],
            in_specs=[vspec] * 3, out_specs=[pl.BlockSpec(memory_space=pltpu.HBM)] * 3,
            scratch_shapes=[sem((3,))],
            compiler_params=pltpu.CompilerParams(vmem_limit_bytes=2 ** 20),
        )(out_u, out_i, loss)
        return out_u.T, out_i.T, loss.reshape(-1)

    return jax.shard_map(
        local_fn, mesh=mesh,
        in_specs=(P("row", "col"), P(("row", "col"), "emb"), P(("col", "row"), "emb"), P()),
        out_specs=(P(("row", "col"), "emb"), P(("col", "row"), "emb"), P()),
        check_vma=False)
```

```python
import functools

import jax
import jax.numpy as jnp
from jax import lax
from jax.experimental import pallas as pl
from jax.experimental.pallas import tpu as pltpu
from jax.sharding import PartitionSpec as P

NUM_LAYERS = 3
MESH = pl.DeviceIdType.MESH
F32 = jnp.float32
BF16 = jnp.bfloat16

NY = 2
NQ = 4
NM = 2
NS = 4
LB = 256
GL = 256
LANES = 128
ROWS = 16


class Copies:
    def __init__(self, send_sems, recv_sems):
        self.send_sems, self.recv_sems = send_sems, recv_sems
        self.recvs, self.groups, self.single = 0, {}, []

    def recv_sem(self):
        self.recvs += 1
        return self.recv_sems.at[self.recvs - 1]

    def send(self, src, dst, device, group=None, whole=None, recv_sem=None):
        count = len(self.groups) + len(self.single)
        if group is None:
            sem = self.send_sems.at[count]
        else:
            if group not in self.groups:
                self.groups[group] = (self.send_sems.at[count], whole)
            sem = self.groups[group][0]
        copy = pltpu.make_async_remote_copy(
            src_ref=src, dst_ref=dst, send_sem=sem,
            recv_sem=self.recv_sem() if recv_sem is None else recv_sem,
            device_id=device, device_id_type=MESH)
        copy.start()
        if group is None:
            self.single.append(copy)
        return copy

    def drain(self):
        for copy in self.single:
            copy.wait_send()
        for sem, whole in self.groups.values():
            wait_bytes(whole, sem)


def wait_bytes(ref, sem):
    pltpu.make_async_copy(ref, ref, sem).wait()


VMEM_LIMIT = 52 * 2 ** 20
NUM_SENDS = 31
NUM_RECVS = 64
NUM_LOADS = NQ * NM + NS + 2


class Phase:
    def __init__(self):
        self.current = None

    def __call__(self, name):
        if self.current is not None:
            self.current.__exit__(None, None, None)
        self.current = None
        if name:
            self.current = jax.named_scope(name)
            self.current.__enter__()


def kernel(mask_hbm, u0_hbm, i0_hbm, trip_hbm, outu_ref, outi_ref, loss_ref,
           maskv, maskb, adj, csum, crd, crx, cch, invi, racc, rsum, rrecv, invu, trip_ref,
           upan, upart, urecv, ipan, ipart, ird, irx, isum,
           ohp, ohn, ohu, hip, hin, hiu, gpart, gsum, grd, grx, eu, zbuf,
           in_sems, send_sems, recv_sems):
    users, quarter = maskv.shape[1:]
    own_users = u0_hbm.shape[1]
    sc = ipan.shape[-1]
    hh = gpart.shape[-1]
    home = NY * hh
    mh = quarter // NM
    pieces, halves = range(NS), range(2)
    own, core, other, both = range(NQ)
    order = (both, other, core, own)

    z, y, r = lax.axis_index("emb"), lax.axis_index("col"), lax.axis_index("row")
    x, c = r // 2, r % 2
    nz = zbuf.shape[0] // (NQ * NY)
    slot = (z * NQ + r) * NY + y

    def rel(m):
        xx = x if m in (own, core) else 1 - x
        cc = c if m in (own, other) else 1 - c
        return 2 * xx + cc

    dev_d, dev_x, dev_xd = [(z, y, rel(m)) for m in (core, other, both)]
    dev_y, dev_xy = (z, 1 - y, r), (z, 1 - y, rel(other))
    flip = [(1 - z // 2, 1 - z % 2), (1 - z // 2, z % 2), (z // 2, 1 - z % 2), (z // 2, z % 2)]
    score_devs = [(2 * a + b, yy, rel(m)) for a, b in flip for yy in (1 - y, y) for m in order][:-1]

    cp = Copies(send_sems, recv_sems)
    phase = Phase()
    phase("start")
    loads = []

    def load(src, dst):
        copy = pltpu.make_async_copy(src, dst, in_sems.at[len(loads)])
        copy.start()
        loads.append(copy)
        return copy

    y_off = pl.multiple_of(y * own_users, own_users)
    own_u = pl.ds(y_off, own_users)
    mask_copies, small = {}, []
    for m in order:
        for h in range(NM):
            off = pl.multiple_of(rel(m) * quarter + h * mh, mh)
            mask_copies[m, h] = load(mask_hbm.at[:, pl.ds(off, mh)], maskv.at[m, :, pl.ds(h * mh, mh)])
        if m == both:
            small.append(load(u0_hbm, upan.at[0, :, own_u]))
            small += [load(i0_hbm.at[:, pl.ds(s * sc, sc)], ipan.at[0, own, s]) for s in pieces]
            small.append(load(trip_hbm, trip_ref))

    barrier = pltpu.get_barrier_semaphore()
    for dev in score_devs:
        pl.semaphore_signal(barrier, inc=1, device_id=dev, device_id_type=MESH)

    racc[...] = jnp.zeros_like(racc)

    def sums(m):
        for h in range(NM):
            mask_copies[m, h].wait()

            def body(j, carry):
                off = pl.multiple_of(h * mh + j * LB, LB)
                tile = h * (mh // LANES) + j * (LB // LANES)
                part = None
                for i in range(users // ROWS):
                    rows = pl.ds(ROWS * i, ROWS)
                    blk = maskv[m, rows, pl.ds(off, LB)]
                    ones = blk.astype(F32).astype(BF16)
                    row = None
                    for g in range(LB // LANES):
                        lanes = slice(LANES * g, LANES * (g + 1))
                        maskb[m, tile + g, rows, :] = ones[:, lanes]
                        row = blk[:, lanes] if row is None else row + blk[:, lanes]
                    racc[rows, :] += row
                    two = blk[:ROWS // 2] + blk[ROWS // 2:]
                    part = two if part is None else part + two
                csum[m, :, pl.ds(off, LB)] = jnp.sum(part.astype(F32), axis=0, keepdims=True)
                return carry
            lax.fori_loop(0, mh // LB, body, 0)

    def one_hot(lanes):
        hit = lax.broadcasted_iota(jnp.int32, (GL, LANES), 0) == lanes
        return jnp.where(hit, 1.0, 0.0).astype(BF16)

    def hot_block(oh, t):
        n = LB // LANES
        return jnp.concatenate([oh[t * n + i] for i in range(n)], axis=1)

    def one_hots(m):
        base = pl.multiple_of(rel(m) * home, home)
        for row, oh, hi in ((1, ohp, hip), (2, ohn, hin)):
            ids = trip_ref[pl.ds(row, 1), pl.ds(base, home)]
            owned = ids // quarter == y * NQ + r
            hi[m] = (ids % quarter) // GL
            low = jnp.where(owned, ids % GL, -1)
            for t in range(home // LANES):
                oh[m, t] = one_hot(low[:, t * LANES:(t + 1) * LANES])

    def user_one_hots():
        base = pl.multiple_of((r * NY + y) * hh, hh)
        uids = trip_ref[pl.ds(0, 1), pl.ds(base, hh)]
        hiu[...] = uids // users
        low = uids % users
        for t in range(hh // LANES):
            ohu[t] = one_hot(low[:, t * LANES:(t + 1) * LANES])

    csum_d, csum_x = {}, cp.recv_sem()

    def chip_sums(m):
        csum_d[m].wait_recv()
        cch[m] = csum[m] + crd[m]
        cp.send(cch.at[m], crx.at[m ^ other], dev_x, "chip", cch, csum_x)

    def send_sums(m):
        csum_d[m ^ core] = cp.send(csum.at[m], crd.at[m ^ core], dev_d, "sums", csum)

    phase("sums32")
    sums(both)
    sums(other)
    for copy in small:
        copy.wait()
    phase("barrier")
    pl.semaphore_wait(barrier, len(score_devs))
    phase("sums10")
    send_sums(both)
    send_sums(other)
    u0_y = cp.send(upan.at[0, :, own_u], upan.at[0, :, own_u], dev_y)
    i0_d = cp.send(ipan.at[0, own], ipan.at[0, core], dev_d)
    sums(core)
    send_sums(core)
    chip_sums(both)
    chip_sums(other)
    sums(own)
    send_sums(own)
    phase("rows")
    rows = jnp.transpose(racc[...].astype(F32), (1, 0))
    rsum[...] = jnp.sum(rows, axis=0, keepdims=True)
    rs_y = cp.send(rsum, rrecv, dev_y)
    chip_sums(core)
    one_hots(both)
    phase("chip0")
    chip_sums(own)
    i0_x = cp.send(ipan.at[0, own], ipan.at[0, other], dev_x)
    phase("onehots")
    one_hots(other)
    one_hots(core)
    phase("rs_wait")
    u0_y.wait_recv()
    rs_y.wait_recv()
    inv_row = lax.rsqrt(jnp.maximum(rsum[...] + rrecv[...], 1.0))
    invu[...] = jnp.transpose(jnp.broadcast_to(inv_row, (LANES, users)), (1, 0))
    phase("cx_wait")
    wait_bytes(crx, csum_x)
    for m in order:
        invi[m] = lax.rsqrt(jnp.maximum(cch[m] + crx[m], 1.0))

    tiles = sc // LANES

    def build(m, s):
        for tile in range(s * tiles, (s + 1) * tiles):
            scale = (invu[...] * invi[m, :, tile * LANES:(tile + 1) * LANES]).astype(BF16)
            adj[m, tile] = scale * maskb[m, tile]

    def block(m, s, n, rows):
        return jnp.concatenate([adj[m, t, rows, :] for t in range(s * tiles, (s + n) * tiles)], axis=1)

    def items(k, m, some=pieces):
        for s in some:
            ipart[k, m, s] = jnp.dot(upan[k], block(m, s, 1, slice(0, users)), preferred_element_type=F32)

    def user_part(k, m, acc=None, s=0, n=NS):
        table = jnp.concatenate([ipan[k, m, s + i] for i in range(n)], axis=1)
        out = []
        for h in halves:
            part = lax.dot_general(
                table, block(m, s, n, slice(h * own_users, (h + 1) * own_users)),
                (((1,), (1,)), ((), ())), preferred_element_type=F32)
            out.append(part if acc is None else acc[h] + part)
        return out

    d, xs, g, gd, f = {}, {}, {}, {}, {}

    def core_send(k, s):
        d[k, s] = cp.send(ipart.at[k, both, s], ird.at[k, 1, s], dev_d, ("core", k), ipart.at[k, both])

    def core_send_own(k):
        d[k] = cp.send(ipart.at[k, core], ird.at[k, 0], dev_d)

    def x_send(k, s):
        d[k, s].wait_recv()
        isum[k, s] = ipart[k, other, s] + ird[k, 1, s]
        xs[k, s] = cp.send(isum.at[k, s], irx.at[k, s], dev_x, ("x", k), isum.at[k])

    def own_piece(k, s):
        if s == 0:
            d[k].wait_recv()
        xs[k, s].wait_recv()
        total = (ipart[k, own, s] + ird[k, 0, s]) + irx[k, s]
        ipan[k + 1, own, s] = total.astype(BF16)

    def own_gather(k, s):
        own_piece(k, s)
        g[k + 1, s] = cp.send(
            ipan.at[k + 1, own, s], ipan.at[k + 1, other, s], dev_x, ("gather", k), ipan.at[k + 1, own])
        if s == NS - 1:
            gd[k + 1] = cp.send(ipan.at[k + 1, own], ipan.at[k + 1, core], dev_d)

    def forward(k, s):
        g[k, s].wait_recv()
        f[k, s] = cp.send(ipan.at[k, other, s], ipan.at[k, both, s], dev_d, ("forward", k), ipan.at[k, other])

    def send_user(k, acc):
        for h in halves:
            upart[k, :, h * own_users:(h + 1) * own_users] = acc[h]
        return cp.send(upart.at[k], urecv.at[k], dev_y)

    def take_user(k, got):
        got.wait_recv()
        upan[k + 1] = (upart[k] + urecv[k]).astype(BF16)

    last = NS - 1
    phase("build32")
    for s in pieces:
        build(both, s)
        items(0, both, [s])
        build(other, s)
        core_send(0, s)
        items(0, other, [s])
        if s > 1:
            x_send(0, s - 2)
    phase("build10")
    for s in pieces:
        build(core, s)
        if s in (1, last):
            x_send(0, NS - 2 + s // 2)
    for s in pieces:
        build(own, s)
    phase("i0_x_wait")
    i0_x.wait_recv()
    i0_f = cp.send(ipan.at[0, other], ipan.at[0, both], dev_d)
    phase("upart0")
    i0_d.wait_recv()
    acc = user_part(0, core, user_part(0, own))
    acc = user_part(0, other, acc)
    phase("upart0b")
    i0_f.wait_recv()
    acc = user_part(0, both, acc)
    u1 = send_user(0, acc)
    phase("items1_10")
    items(0, core)
    core_send_own(0)
    items(0, own)
    one_hots(own)
    user_one_hots()
    for s in range(last):
        phase(f"own1_{s}")
        own_gather(0, s)
    phase("u1_wait")
    take_user(0, u1)

    def items_x(k, between=None):
        items(k, both)
        items(k, other, [0])
        for s in pieces:
            core_send(k, s)
        if between is not None:
            between()
        items(k, other, range(1, NS))

    phase("items2_32")
    items_x(1)
    phase("own1_last")
    own_gather(0, last)
    phase("items2_10")
    items(1, core)
    core_send_own(1)
    items(1, own)
    phase("x2")
    for s in pieces:
        x_send(1, s)
    phase("fwd1_0")
    forward(1, 0)
    acc = user_part(1, own)
    phase("fwd1_1")
    forward(1, 1)
    gd[1].wait_recv()
    acc = user_part(1, core, acc)
    phase("fwd1_2")
    forward(1, 2)
    acc = user_part(1, other, acc, 0, last)
    phase("fwd1_3")
    forward(1, last)
    acc = user_part(1, other, acc, last, 1)
    for s in range(last):
        f[1, s].wait_recv()
    acc = user_part(1, both, acc, 0, last)
    phase("f1_wait")
    f[1, last].wait_recv()
    acc = user_part(1, both, acc, last, 1)
    u2 = send_user(1, acc)
    phase("own2_01")
    own_gather(1, 0)
    own_gather(1, 1)
    phase("u2_wait")
    take_user(1, u2)
    phase("items3_32")
    items_x(2, lambda: own_gather(1, 2))
    items(2, core)
    phase("x3")
    x_send(2, 0)
    core_send_own(2)
    phase("own2_3")
    own_gather(1, last)
    for s in range(1, NS):
        x_send(2, s)
    phase("items3_own")
    items(2, own)
    phase("upart2_01")
    acc = user_part(2, own)
    gd[2].wait_recv()
    acc = user_part(2, core, acc)
    phase("fwd2_01")
    for s in halves:
        forward(2, s)
    acc = user_part(2, other, acc, 0, 2)
    for s in halves:
        f[2, s].wait_recv()
    acc = user_part(2, both, acc, 0, 2)
    phase("fwd2_23")
    for s in (2, last):
        forward(2, s)
    acc = user_part(2, other, acc, 2, NS - 2)
    phase("f2_wait")
    for s in (2, last):
        f[2, s].wait_recv()
    acc = user_part(2, both, acc, 2, NS - 2)
    u3 = send_user(2, acc)

    def mean4(a, b, e, h):
        tot = ((a.astype(F32) + b.astype(F32)) + e.astype(F32)) + h.astype(F32)
        return (tot * (1.0 / (NUM_LAYERS + 1))).astype(BF16)

    def pick(tab, oh, hi, first):
        got = jnp.dot(tab, oh, preferred_element_type=F32)
        n = got.shape[0] // ROWS
        out = jnp.where(hi == first, got[:ROWS], 0.0)
        for i in range(1, n):
            out = out + jnp.where(hi == first + i, got[i * ROWS:(i + 1) * ROWS], 0.0)
        return out

    def final_piece(s):
        own_piece(2, s)
        outi_ref[:, s * sc:(s + 1) * sc] = mean4(*[ipan[k, own, s] for k in range(NUM_LAYERS + 1)])

    def differences(m, h, first, n):
        groups = range(first * sc // GL, (first + n) * sc // GL)
        table = jnp.concatenate([outi_ref[:, i * GL:(i + 1) * GL] for i in groups], axis=0)
        for t in range(h * (hh // LB), (h + 1) * (hh // LB)):
            sl = slice(t * LB, (t + 1) * LB)
            pos = pick(table, hot_block(ohp.at[m], t), hip[m, :, sl], groups[0])
            neg = pick(table, hot_block(ohn.at[m], t), hin[m, :, sl], groups[0])
            out = slice(t * LB - h * hh, (t + 1) * LB - h * hh)
            gpart[m, h, :, out] = pos - neg if first == 0 else (gpart[m, h, :, out] + pos) - neg

    phase("own3")
    for s in range(last):
        final_piece(s)
    phase("diff_012")
    for m in order:
        for h in halves:
            differences(m, h, 0, last)
    phase("u3_wait")
    take_user(2, u3)
    phase("finalu")
    eu[own] = mean4(*[upan[k] for k in range(NUM_LAYERS + 1)])
    others = eu.at[pl.ds(core, NQ - 1)]
    eu_sem = cp.recv_sem()
    for m, dev in ((core, dev_d), (other, dev_x), (both, dev_xd)):
        cp.send(eu.at[own], eu.at[m], dev, "eu", others, eu_sem)
    outu_ref[...] = eu[own, :, own_u]

    phase("own3_last")
    final_piece(last)
    gd3 = {}
    phase("diff3")
    for h in halves:
        differences(both, h, last, 1)
        gd3[h] = cp.send(gpart.at[both, h], grd.at[1, h], dev_d)
    for h in halves:
        differences(other, h, last, 1)
    for h in halves:
        differences(core, h, last, 1)
    gd1 = cp.send(gpart.at[core], grd.at[0], dev_d)
    phase("gd3_wait")
    for h in halves:
        gd3[h].wait_recv()

    g_sem = cp.recv_sem()

    def home_send(i, m, h, dev):
        gsum[i] = gpart[m, h] + grd[m // 2, h]
        cp.send(gsum.at[i], grx.at[i], dev, "home", gsum, g_sem)

    home_send(0, other, 1 - y, dev_xy)
    home_send(1, other, y, dev_x)
    phase("diff0")
    for h in halves:
        differences(own, h, last, 1)
    phase("gd1_wait")
    gd1.wait_recv()
    home_send(2, own, 1 - y, dev_y)
    phase("e_wait")
    wait_bytes(others, eu_sem)
    phase("picku")
    utab = jnp.concatenate([eu[m] for m in range(NQ)], axis=0)
    place = jnp.where(hiu[...] // 2 == x, own, other) + jnp.where(hiu[...] % 2 == c, own, core)
    picked = [pick(utab, hot_block(ohu, t), place[:, t * LB:(t + 1) * LB], own) for t in range(hh // LB)]
    phase("gy_wait")
    wait_bytes(grx, g_sem)
    phase("dot")
    for t in range(hh // LB):
        sl = slice(t * LB, (t + 1) * LB)
        mine = gpart[own, y, :, sl] + grd[0, y, :, sl]
        diff = (mine + grx[1, :, sl]) + (grx[2, :, sl] + grx[0, :, sl])
        zbuf[slot, :, sl] = jnp.sum(picked[t] * diff, axis=0, keepdims=True)
    rest = zbuf.at[pl.ds(0, len(score_devs))]
    z_sem = cp.recv_sem()
    for dev in score_devs:
        cp.send(zbuf.at[slot], zbuf.at[slot], dev, "score", rest, z_sem)
    phase("z_wait")
    wait_bytes(rest, z_sem)
    phase("loss")
    for q in range(NQ * NY):
        neg = -sum(zbuf[k * NQ * NY + q] for k in range(nz))
        loss_ref[q] = jnp.maximum(neg, 0.0) + jnp.log1p(jnp.exp(-jnp.abs(neg)))
    phase("drain")
    cp.drain()
    phase(None)
    assert (len(cp.groups) + len(cp.single), cp.recvs, len(loads)) == (NUM_SENDS, NUM_RECVS, NUM_LOADS)


def emit(*refs):
    n = len(refs) // 2
    sems = refs[-1]
    copies = [pltpu.make_async_copy(src, dst, sems.at[i]) for i, (src, dst) in enumerate(zip(refs[:n], refs[n:]))]
    for copy in copies:
        copy.start()
    for copy in copies:
        copy.wait()


def solution(mesh):
    def local_fn(mask_blk, user_sh, item_sh, triples):
        users, items = mask_blk.shape
        cols, own_users = user_sh.shape[1], user_sh.shape[0]
        quarter = items // NQ
        home = triples.shape[0] // NQ
        hh = home // NY
        vm, sem = pltpu.VMEM, pltpu.SemaphoreType.DMA
        nl = NUM_LAYERS
        sc = quarter // NS
        tiles = (NQ, quarter // LANES, users, LANES)
        per_item, hots = (NQ, 1, quarter), (NQ, home // LANES, GL, LANES)
        triple_row = (NQ, 1, home)
        scratch = [
            vm((NQ, users, quarter), jnp.int32), vm(tiles, BF16), vm(tiles, BF16),
            *[vm(per_item, F32)] * 5,
            vm((users, LANES), jnp.int32), vm((1, users), F32), vm((1, users), F32), vm((users, LANES), F32),
            vm(triples.shape[::-1], jnp.int32),
            vm((nl + 1, cols, users), BF16), vm((nl, cols, users), F32), vm((nl, cols, users), F32),
            vm((nl + 1, NQ, NS, cols, sc), BF16), vm((nl, NQ, NS, cols, sc), F32),
            vm((nl, 2, NS, cols, sc), F32), vm((nl, NS, cols, sc), F32), vm((nl, NS, cols, sc), F32),
            vm(hots, BF16), vm(hots, BF16), vm((hh // LANES, GL, LANES), BF16),
            vm(triple_row, jnp.int32), vm(triple_row, jnp.int32), vm((1, hh), jnp.int32),
            vm((NQ, NY, cols, hh), F32), vm((3, cols, hh), F32), vm((2, NY, cols, hh), F32), vm((3, cols, hh), F32),
            vm((NQ, cols, users), BF16), vm((mesh.size, 1, hh), F32),
            sem((NUM_LOADS,)), sem((NUM_SENDS,)), sem((NUM_RECVS,)),
        ]
        vspec = pl.BlockSpec(memory_space=pltpu.VMEM)
        out_u, out_i, loss = pl.pallas_call(
            kernel,
            out_shape=[
                jax.ShapeDtypeStruct((cols, own_users), BF16),
                jax.ShapeDtypeStruct((cols, quarter), BF16),
                jax.ShapeDtypeStruct((NQ * NY, 1, hh), F32)],
            in_specs=[pl.BlockSpec(memory_space=pltpu.HBM)] * 4,
            out_specs=[vspec, vspec, vspec],
            scratch_shapes=scratch,
            compiler_params=pltpu.CompilerParams(
                collective_id=0, has_side_effects=True, vmem_limit_bytes=VMEM_LIMIT),
        )(*[pltpu.with_memory_space_constraint(a, pltpu.HBM) for a in (mask_blk, user_sh.T, item_sh.T, triples.T)])
        out_u, out_i, loss = pl.pallas_call(
            emit,
            out_shape=[jax.ShapeDtypeStruct(a.shape, a.dtype) for a in (out_u, out_i, loss)],
            in_specs=[vspec] * 3, out_specs=[pl.BlockSpec(memory_space=pltpu.HBM)] * 3,
            scratch_shapes=[sem((3,))],
            compiler_params=pltpu.CompilerParams(vmem_limit_bytes=2 ** 20),
        )(out_u, out_i, loss)
        return out_u.T, out_i.T, loss.reshape(-1)

    return jax.shard_map(
        local_fn, mesh=mesh,
        in_specs=(P("row", "col"), P(("row", "col"), "emb"), P(("col", "row"), "emb"), P()),
        out_specs=(P(("row", "col"), "emb"), P(("col", "row"), "emb"), P()),
        check_vma=False)
```

```python
import functools

import jax
import jax.numpy as jnp
from jax import lax
from jax.experimental import pallas as pl
from jax.experimental.pallas import tpu as pltpu
from jax.sharding import PartitionSpec as P

NUM_LAYERS = 3
MESH = pl.DeviceIdType.MESH
F32 = jnp.float32
BF16 = jnp.bfloat16

NY = 2
NQ = 4
NM = 4
NS = 4
LB = 256
GL = 256
LANES = 128
ROWS = 16


class Copies:
    def __init__(self, send_sems, recv_sems):
        self.send_sems, self.recv_sems = send_sems, recv_sems
        self.recvs, self.groups, self.single = 0, {}, []

    def recv_sem(self):
        self.recvs += 1
        return self.recv_sems.at[self.recvs - 1]

    def send(self, src, dst, device, group=None, whole=None, recv_sem=None):
        count = len(self.groups) + len(self.single)
        if group is None:
            sem = self.send_sems.at[count]
        else:
            if group not in self.groups:
                self.groups[group] = (self.send_sems.at[count], whole)
            sem = self.groups[group][0]
        copy = pltpu.make_async_remote_copy(
            src_ref=src, dst_ref=dst, send_sem=sem,
            recv_sem=self.recv_sem() if recv_sem is None else recv_sem,
            device_id=device, device_id_type=MESH)
        copy.start()
        if group is None:
            self.single.append(copy)
        return copy

    def drain(self):
        for copy in self.single:
            copy.wait_send()
        for sem, whole in self.groups.values():
            wait_bytes(whole, sem)


def wait_bytes(ref, sem):
    pltpu.make_async_copy(ref, ref, sem).wait()


VMEM_LIMIT = 52 * 2 ** 20
NUM_SENDS = 31
NUM_RECVS = 57
NUM_LOADS = NQ * NM + 3


class Phase:
    def __init__(self):
        self.current = None

    def __call__(self, name):
        if self.current is not None:
            self.current.__exit__(None, None, None)
        self.current = None
        if name:
            self.current = jax.named_scope(name)
            self.current.__enter__()


def kernel(mask_hbm, u0_hbm, i0_hbm, trip_hbm, outu_ref, outi_ref, loss_ref,
           maskv, maskb, adj, csum, crd, crx, cch, invi, racc, rsum, rrecv, invu, trip_ref,
           upan, upart, urecv, ipan, ipart, ird, irx, isum,
           ohp, ohn, ohu, hip, hin, hiu, gpart, gsum, grd, grx, eu, zbuf,
           in_sems, send_sems, recv_sems):
    users, quarter = maskv.shape[1:]
    own_users = u0_hbm.shape[1]
    sc = ipan.shape[-1]
    hh = gpart.shape[-1]
    home = NY * hh
    mh = quarter // NM
    pieces, halves = range(NS), range(2)
    own, core, other, both = range(NQ)
    order = (both, other, core, own)

    z, y, r = lax.axis_index("emb"), lax.axis_index("col"), lax.axis_index("row")
    x, c = r // 2, r % 2
    nz = zbuf.shape[0] // (NQ * NY)
    slot = (z * NQ + r) * NY + y

    def rel(m):
        xx = x if m in (own, core) else 1 - x
        cc = c if m in (own, other) else 1 - c
        return 2 * xx + cc

    dev_d, dev_x, dev_xd = [(z, y, rel(m)) for m in (core, other, both)]
    dev_y, dev_xy = (z, 1 - y, r), (z, 1 - y, rel(other))
    flip = [(1 - z // 2, 1 - z % 2), (1 - z // 2, z % 2), (z // 2, 1 - z % 2), (z // 2, z % 2)]
    score_devs = [(2 * a + b, yy, rel(m)) for a, b in flip for yy in (1 - y, y) for m in order][:-1]

    cp = Copies(send_sems, recv_sems)
    phase = Phase()
    phase("start")
    loads = []

    def load(src, dst, sem=None):
        if sem is None:
            loads.append(in_sems.at[len(loads)])
            sem = loads[-1]
        copy = pltpu.make_async_copy(src, dst, sem)
        copy.start()
        return copy

    y_off = pl.multiple_of(y * own_users, own_users)
    own_u = pl.ds(y_off, own_users)
    mask_copies, small = {}, []
    for m in order:
        for h in range(NM):
            off = pl.multiple_of(rel(m) * quarter + h * mh, mh)
            mask_copies[m, h] = load(mask_hbm.at[:, pl.ds(off, mh)], maskv.at[m, :, pl.ds(h * mh, mh)])
        if m == both:
            small.append(load(u0_hbm, upan.at[0, :, own_u]))
            loads.append(in_sems.at[len(loads)])
            i0_sem = loads[-1]
            for s in pieces:
                load(i0_hbm.at[:, pl.ds(s * sc, sc)], ipan.at[0, own, s], i0_sem)
            small.append(load(trip_hbm, trip_ref))

    barrier = pltpu.get_barrier_semaphore()
    for dev in score_devs:
        pl.semaphore_signal(barrier, inc=1, device_id=dev, device_id_type=MESH)

    racc[...] = jnp.zeros_like(racc)

    def sums(m):
        for h in range(NM):
            mask_copies[m, h].wait()

            def body(j, carry):
                off = pl.multiple_of(h * mh + j * LB, LB)
                tile = h * (mh // LANES) + j * (LB // LANES)
                part = None
                for i in range(users // ROWS):
                    rows = pl.ds(ROWS * i, ROWS)
                    blk = maskv[m, rows, pl.ds(off, LB)]
                    ones = blk.astype(F32).astype(BF16)
                    row = None
                    for g in range(LB // LANES):
                        lanes = slice(LANES * g, LANES * (g + 1))
                        maskb[m, tile + g, rows, :] = ones[:, lanes]
                        row = blk[:, lanes] if row is None else row + blk[:, lanes]
                    racc[rows, :] += row
                    two = blk[:ROWS // 2] + blk[ROWS // 2:]
                    part = two if part is None else part + two
                csum[m, :, pl.ds(off, LB)] = jnp.sum(part.astype(F32), axis=0, keepdims=True)
                return carry
            lax.fori_loop(0, mh // LB, body, 0)

    def one_hot(lanes):
        hit = lax.broadcasted_iota(jnp.int32, (GL, LANES), 0) == lanes
        return jnp.where(hit, 1.0, 0.0).astype(BF16)

    def hot_block(oh, t):
        n = LB // LANES
        return jnp.concatenate([oh[t * n + i] for i in range(n)], axis=1)

    def one_hots(m):
        base = pl.multiple_of(rel(m) * home, home)
        for row, oh, hi in ((1, ohp, hip), (2, ohn, hin)):
            ids = trip_ref[pl.ds(row, 1), pl.ds(base, home)]
            owned = ids // quarter == y * NQ + r
            hi[m] = (ids % quarter) // GL
            low = jnp.where(owned, ids % GL, -1)
            for t in range(home // LANES):
                oh[m, t] = one_hot(low[:, t * LANES:(t + 1) * LANES])

    def user_one_hots():
        base = pl.multiple_of((r * NY + y) * hh, hh)
        uids = trip_ref[pl.ds(0, 1), pl.ds(base, hh)]
        hiu[...] = uids // users
        low = uids % users
        for t in range(hh // LANES):
            ohu[t] = one_hot(low[:, t * LANES:(t + 1) * LANES])

    csum_d, csum_x = {}, cp.recv_sem()

    def chip_sums(m):
        csum_d[m].wait_recv()
        cch[m] = csum[m] + crd[m]
        cp.send(cch.at[m], crx.at[m ^ other], dev_x, "chip", cch, csum_x)

    def send_sums(m):
        csum_d[m ^ core] = cp.send(csum.at[m], crd.at[m ^ core], dev_d, "sums", csum)

    phase("sums32")
    sums(both)
    sums(other)
    for copy in small:
        copy.wait()
    wait_bytes(ipan.at[0, own], i0_sem)
    phase("barrier")
    pl.semaphore_wait(barrier, len(score_devs))
    phase("sums10")
    send_sums(both)
    send_sums(other)
    u0_y = cp.send(upan.at[0, :, own_u], upan.at[0, :, own_u], dev_y)
    i0_d = cp.send(ipan.at[0, own], ipan.at[0, core], dev_d)
    sums(core)
    send_sums(core)
    chip_sums(both)
    chip_sums(other)
    sums(own)
    send_sums(own)
    phase("rows")
    rows = jnp.transpose(racc[...].astype(F32), (1, 0))
    rsum[...] = jnp.sum(rows, axis=0, keepdims=True)
    rs_y = cp.send(rsum, rrecv, dev_y)
    chip_sums(core)
    one_hots(both)
    phase("chip0")
    chip_sums(own)
    i0_x = cp.send(ipan.at[0, own], ipan.at[0, other], dev_x)
    phase("onehots")
    one_hots(other)
    one_hots(core)
    phase("rs_wait")
    u0_y.wait_recv()
    rs_y.wait_recv()
    inv_row = lax.rsqrt(jnp.maximum(rsum[...] + rrecv[...], 1.0))
    invu[...] = jnp.transpose(jnp.broadcast_to(inv_row, (LANES, users)), (1, 0))
    phase("cx_wait")
    wait_bytes(crx, csum_x)
    for m in order:
        invi[m] = lax.rsqrt(jnp.maximum(cch[m] + crx[m], 1.0))

    tiles = sc // LANES

    def build(m, s):
        for tile in range(s * tiles, (s + 1) * tiles):
            scale = (invu[...] * invi[m, :, tile * LANES:(tile + 1) * LANES]).astype(BF16)
            adj[m, tile] = scale * maskb[m, tile]

    def block(m, s, n, rows):
        return jnp.concatenate([adj[m, t, rows, :] for t in range(s * tiles, (s + n) * tiles)], axis=1)

    def items(k, m, some=pieces):
        for s in some:
            ipart[k, m, s] = jnp.dot(upan[k], block(m, s, 1, slice(0, users)), preferred_element_type=F32)

    def user_part(k, m, acc=None, s=0, n=NS):
        table = jnp.concatenate([ipan[k, m, s + i] for i in range(n)], axis=1)
        out = []
        for h in halves:
            part = lax.dot_general(
                table, block(m, s, n, slice(h * own_users, (h + 1) * own_users)),
                (((1,), (1,)), ((), ())), preferred_element_type=F32)
            out.append(part if acc is None else acc[h] + part)
        return out

    d, xs, g, gd, f = {}, {}, {}, {}, {}
    shared, last = {}, NS - 1

    def share(*name):
        if name not in shared:
            shared[name] = cp.recv_sem()
        return shared[name]

    def core_send(k, s):
        d[k, s] = cp.send(ipart.at[k, both, s], ird.at[k, 1, s], dev_d, ("core", k), ipart.at[k, both],
            share("core", k) if k == 1 else None)

    def core_send_own(k):
        d[k] = cp.send(ipart.at[k, core], ird.at[k, 0], dev_d)

    def x_send(k, s):
        if k != 1:
            d[k, s].wait_recv()
        elif s == 0:
            wait_bytes(ird.at[k, 1], share("core", k))
        isum[k, s] = ipart[k, other, s] + ird[k, 1, s]
        xs[k, s] = cp.send(isum.at[k, s], irx.at[k, s], dev_x, ("x", k), isum.at[k])

    def own_piece(k, s):
        if s == 0:
            d[k].wait_recv()
        xs[k, s].wait_recv()
        total = (ipart[k, own, s] + ird[k, 0, s]) + irx[k, s]
        ipan[k + 1, own, s] = total.astype(BF16)

    def own_gather(k, s):
        own_piece(k, s)
        g[k + 1, s] = cp.send(
            ipan.at[k + 1, own, s], ipan.at[k + 1, other, s], dev_x, ("gather", k), ipan.at[k + 1, own])
        if s == NS - 1:
            gd[k + 1] = cp.send(ipan.at[k + 1, own], ipan.at[k + 1, core], dev_d)

    batches = {1: (range(last), range(last, NS)), 2: (halves, range(2, NS))}

    def take_forwarded(k, i):
        batch = batches[k][i]
        wait_bytes(ipan.at[k, both, pl.ds(batch.start, len(batch))], share("forward", k, i == 0))

    def forward(k, s):
        g[k, s].wait_recv()
        f[k, s] = cp.send(ipan.at[k, other, s], ipan.at[k, both, s], dev_d, ("forward", k), ipan.at[k, other],
            share("forward", k, s in batches[k][0]))

    def send_user(k, acc):
        for h in halves:
            upart[k, :, h * own_users:(h + 1) * own_users] = acc[h]
        return cp.send(upart.at[k], urecv.at[k], dev_y)

    def take_user(k, got):
        got.wait_recv()
        upan[k + 1] = (upart[k] + urecv[k]).astype(BF16)

    phase("build32")
    for s in range(NS + 1):
        if s < NS:
            build(both, s)
            items(0, both, [s])
        if s:
            build(other, s - 1)
        if s < NS:
            core_send(0, s)
        if s:
            items(0, other, [s - 1])
        if s in range(2, NS):
            x_send(0, s - 2)
    phase("build10")
    for s in pieces:
        build(core, s)
        if s in (1, last):
            x_send(0, NS - 2 + s // 2)
    for s in pieces:
        build(own, s)
    phase("i0_x_wait")
    i0_x.wait_recv()
    i0_f = cp.send(ipan.at[0, other], ipan.at[0, both], dev_d)
    phase("upart0")
    i0_d.wait_recv()
    acc = user_part(0, core, user_part(0, own))
    acc = user_part(0, other, acc)
    phase("upart0b")
    i0_f.wait_recv()
    acc = user_part(0, both, acc)
    u1 = send_user(0, acc)
    phase("items1_10")
    items(0, core)
    core_send_own(0)
    items(0, own)
    for s in range(last):
        if s == last - 1:
            one_hots(own)
            user_one_hots()
        phase(f"own1_{s}")
        own_gather(0, s)
    phase("u1_wait")
    take_user(0, u1)

    def items_x(k, between=None):
        items(k, both)
        items(k, other, [0])
        for s in pieces:
            core_send(k, s)
        if between is not None:
            between()
        items(k, other, range(1, NS))

    phase("items2_32")
    items_x(1)
    phase("own1_last")
    own_gather(0, last)
    phase("items2_10")
    items(1, core)
    core_send_own(1)
    items(1, own)
    phase("x2")
    for s in pieces:
        x_send(1, s)
    phase("fwd1_0")
    forward(1, 0)
    acc = user_part(1, own)
    phase("fwd1_1")
    forward(1, 1)
    gd[1].wait_recv()
    acc = user_part(1, core, acc)
    phase("fwd1_2")
    forward(1, 2)
    acc = user_part(1, other, acc, 0, last)
    phase("fwd1_3")
    forward(1, last)
    acc = user_part(1, other, acc, last, 1)
    take_forwarded(1, 0)
    acc = user_part(1, both, acc, 0, last)
    phase("f1_wait")
    take_forwarded(1, 1)
    acc = user_part(1, both, acc, last, 1)
    u2 = send_user(1, acc)
    phase("own2_01")
    own_gather(1, 0)
    own_gather(1, 1)
    phase("u2_wait")
    take_user(1, u2)
    phase("items3_32")
    items_x(2, lambda: own_gather(1, 2))
    items(2, core)
    phase("x3")
    x_send(2, 0)
    core_send_own(2)
    phase("own2_3")
    own_gather(1, last)
    for s in range(1, NS):
        x_send(2, s)
    phase("items3_own")
    items(2, own)
    phase("upart2_01")
    acc = user_part(2, own)
    gd[2].wait_recv()
    acc = user_part(2, core, acc)
    phase("fwd2_01")
    for s in halves:
        forward(2, s)
    acc = user_part(2, other, acc, 0, 2)
    take_forwarded(2, 0)
    acc = user_part(2, both, acc, 0, 2)
    phase("fwd2_23")
    for s in (2, last):
        forward(2, s)
    acc = user_part(2, other, acc, 2, NS - 2)
    phase("f2_wait")
    take_forwarded(2, 1)
    acc = user_part(2, both, acc, 2, NS - 2)
    u3 = send_user(2, acc)

    def mean4(a, b, e, h):
        tot = ((a.astype(F32) + b.astype(F32)) + e.astype(F32)) + h.astype(F32)
        return (tot * (1.0 / (NUM_LAYERS + 1))).astype(BF16)

    def pick(tab, oh, hi, first):
        got = jnp.dot(tab, oh, preferred_element_type=F32)
        n = got.shape[0] // ROWS
        out = jnp.where(hi == first, got[:ROWS], 0.0)
        for i in range(1, n):
            out = out + jnp.where(hi == first + i, got[i * ROWS:(i + 1) * ROWS], 0.0)
        return out

    def final_piece(s):
        own_piece(2, s)
        outi_ref[:, s * sc:(s + 1) * sc] = mean4(*[ipan[k, own, s] for k in range(NUM_LAYERS + 1)])

    def differences(m, h, first, n):
        groups = range(first * sc // GL, (first + n) * sc // GL)
        table = jnp.concatenate([outi_ref[:, i * GL:(i + 1) * GL] for i in groups], axis=0)
        for t in range(h * (hh // LB), (h + 1) * (hh // LB)):
            sl = slice(t * LB, (t + 1) * LB)
            pos = pick(table, hot_block(ohp.at[m], t), hip[m, :, sl], groups[0])
            neg = pick(table, hot_block(ohn.at[m], t), hin[m, :, sl], groups[0])
            out = slice(t * LB - h * hh, (t + 1) * LB - h * hh)
            gpart[m, h, :, out] = pos - neg if first == 0 else (gpart[m, h, :, out] + pos) - neg

    phase("own3")
    for s in range(last):
        final_piece(s)
    phase("diff_012")
    for m in order:
        for h in halves:
            differences(m, h, 0, last)
    phase("u3_wait")
    take_user(2, u3)
    phase("finalu")
    eu[own] = mean4(*[upan[k] for k in range(NUM_LAYERS + 1)])
    others = eu.at[pl.ds(core, NQ - 1)]
    eu_sem = cp.recv_sem()
    for m, dev in ((core, dev_d), (other, dev_x), (both, dev_xd)):
        cp.send(eu.at[own], eu.at[m], dev, "eu", others, eu_sem)
    outu_ref[...] = eu[own, :, own_u]

    phase("own3_last")
    final_piece(last)
    gd3 = {}
    phase("diff3")
    for h in halves:
        differences(both, h, last, 1)
        gd3[h] = cp.send(gpart.at[both, h], grd.at[1, h], dev_d)
    for h in halves:
        differences(other, h, last, 1)
    for h in halves:
        differences(core, h, last, 1)
    gd1 = cp.send(gpart.at[core], grd.at[0], dev_d)
    phase("gd3_wait")
    for h in halves:
        gd3[h].wait_recv()

    g_sem = cp.recv_sem()

    def home_send(i, m, h, dev):
        gsum[i] = gpart[m, h] + grd[m // 2, h]
        cp.send(gsum.at[i], grx.at[i], dev, "home", gsum, g_sem)

    home_send(0, other, 1 - y, dev_xy)
    home_send(1, other, y, dev_x)
    phase("diff0")
    for h in halves:
        differences(own, h, last, 1)
    phase("gd1_wait")
    gd1.wait_recv()
    home_send(2, own, 1 - y, dev_y)
    phase("e_wait")
    wait_bytes(others, eu_sem)
    phase("picku")
    utab = jnp.concatenate([eu[m] for m in range(NQ)], axis=0)
    place = jnp.where(hiu[...] // 2 == x, own, other) + jnp.where(hiu[...] % 2 == c, own, core)
    picked = [pick(utab, hot_block(ohu, t), place[:, t * LB:(t + 1) * LB], own) for t in range(hh // LB)]
    phase("gy_wait")
    wait_bytes(grx, g_sem)
    phase("dot")
    for t in range(hh // LB):
        sl = slice(t * LB, (t + 1) * LB)
        mine = gpart[own, y, :, sl] + grd[0, y, :, sl]
        diff = (mine + grx[1, :, sl]) + (grx[2, :, sl] + grx[0, :, sl])
        zbuf[slot, :, sl] = jnp.sum(picked[t] * diff, axis=0, keepdims=True)
    rest = zbuf.at[pl.ds(0, len(score_devs))]
    z_sem = cp.recv_sem()
    for dev in score_devs:
        cp.send(zbuf.at[slot], zbuf.at[slot], dev, "score", rest, z_sem)
    phase("z_wait")
    wait_bytes(rest, z_sem)
    phase("loss")
    for q in range(NQ * NY):
        neg = -sum(zbuf[k * NQ * NY + q] for k in range(nz))
        loss_ref[q] = jnp.maximum(neg, 0.0) + jnp.log1p(jnp.exp(-jnp.abs(neg)))
    phase("drain")
    cp.drain()
    phase(None)
    assert (len(cp.groups) + len(cp.single), cp.recvs, len(loads)) == (NUM_SENDS, NUM_RECVS, NUM_LOADS)


def emit(*refs):
    n = len(refs) // 2
    sems = refs[-1]
    copies = [pltpu.make_async_copy(src, dst, sems.at[i]) for i, (src, dst) in enumerate(zip(refs[:n], refs[n:]))]
    for copy in copies:
        copy.start()
    for copy in copies:
        copy.wait()


def solution(mesh):
    def local_fn(mask_blk, user_sh, item_sh, triples):
        users, items = mask_blk.shape
        cols, own_users = user_sh.shape[1], user_sh.shape[0]
        quarter = items // NQ
        home = triples.shape[0] // NQ
        hh = home // NY
        vm, sem = pltpu.VMEM, pltpu.SemaphoreType.DMA
        nl = NUM_LAYERS
        sc = quarter // NS
        tiles = (NQ, quarter // LANES, users, LANES)
        per_item, hots = (NQ, 1, quarter), (NQ, home // LANES, GL, LANES)
        triple_row = (NQ, 1, home)
        scratch = [
            vm((NQ, users, quarter), jnp.int32), vm(tiles, BF16), vm(tiles, BF16),
            *[vm(per_item, F32)] * 5,
            vm((users, LANES), jnp.int32), vm((1, users), F32), vm((1, users), F32), vm((users, LANES), F32),
            vm(triples.shape[::-1], jnp.int32),
            vm((nl + 1, cols, users), BF16), vm((nl, cols, users), F32), vm((nl, cols, users), F32),
            vm((nl + 1, NQ, NS, cols, sc), BF16), vm((nl, NQ, NS, cols, sc), F32),
            vm((nl, 2, NS, cols, sc), F32), vm((nl, NS, cols, sc), F32), vm((nl, NS, cols, sc), F32),
            vm(hots, BF16), vm(hots, BF16), vm((hh // LANES, GL, LANES), BF16),
            vm(triple_row, jnp.int32), vm(triple_row, jnp.int32), vm((1, hh), jnp.int32),
            vm((NQ, NY, cols, hh), F32), vm((3, cols, hh), F32), vm((2, NY, cols, hh), F32), vm((3, cols, hh), F32),
            vm((NQ, cols, users), BF16), vm((mesh.size, 1, hh), F32),
            sem((NUM_LOADS,)), sem((NUM_SENDS,)), sem((NUM_RECVS,)),
        ]
        vspec = pl.BlockSpec(memory_space=pltpu.VMEM)
        out_u, out_i, loss = pl.pallas_call(
            kernel,
            out_shape=[
                jax.ShapeDtypeStruct((cols, own_users), BF16),
                jax.ShapeDtypeStruct((cols, quarter), BF16),
                jax.ShapeDtypeStruct((NQ * NY, 1, hh), F32)],
            in_specs=[pl.BlockSpec(memory_space=pltpu.HBM)] * 4,
            out_specs=[vspec, vspec, vspec],
            scratch_shapes=scratch,
            compiler_params=pltpu.CompilerParams(
                collective_id=0, has_side_effects=True, vmem_limit_bytes=VMEM_LIMIT),
        )(*[pltpu.with_memory_space_constraint(a, pltpu.HBM) for a in (mask_blk, user_sh.T, item_sh.T, triples.T)])
        out_u, out_i, loss = pl.pallas_call(
            emit,
            out_shape=[jax.ShapeDtypeStruct(a.shape, a.dtype) for a in (out_u, out_i, loss)],
            in_specs=[vspec] * 3, out_specs=[pl.BlockSpec(memory_space=pltpu.HBM)] * 3,
            scratch_shapes=[sem((3,))],
            compiler_params=pltpu.CompilerParams(vmem_limit_bytes=2 ** 20),
        )(out_u, out_i, loss)
        return out_u.T, out_i.T, loss.reshape(-1)

    return jax.shard_map(
        local_fn, mesh=mesh,
        in_specs=(P("row", "col"), P(("row", "col"), "emb"), P(("col", "row"), "emb"), P()),
        out_specs=(P(("row", "col"), "emb"), P(("col", "row"), "emb"), P()),
        check_vma=False)
```

```python
import functools

import jax
import jax.numpy as jnp
from jax import lax
from jax.experimental import pallas as pl
from jax.experimental.pallas import tpu as pltpu
from jax.sharding import PartitionSpec as P

NUM_LAYERS = 3
MESH = pl.DeviceIdType.MESH
F32 = jnp.float32
BF16 = jnp.bfloat16

NY = 2
NQ = 4
NM = 4
NS = 4
LB = 256
GL = 256
LANES = 128
ROWS = 16


class Copies:
    def __init__(self, send_sems, recv_sems):
        self.send_sems, self.recv_sems = send_sems, recv_sems
        self.recvs, self.groups, self.single = 0, {}, []

    def recv_sem(self):
        self.recvs += 1
        return self.recv_sems.at[self.recvs - 1]

    def send(self, src, dst, device, group=None, whole=None, recv_sem=None):
        count = len(self.groups) + len(self.single)
        if group is None:
            sem = self.send_sems.at[count]
        else:
            if group not in self.groups:
                self.groups[group] = (self.send_sems.at[count], whole)
            sem = self.groups[group][0]
        copy = pltpu.make_async_remote_copy(
            src_ref=src, dst_ref=dst, send_sem=sem,
            recv_sem=self.recv_sem() if recv_sem is None else recv_sem,
            device_id=device, device_id_type=MESH)
        copy.start()
        if group is None:
            self.single.append(copy)
        return copy

    def drain(self):
        for copy in self.single:
            copy.wait_send()
        for sem, whole in self.groups.values():
            wait_bytes(whole, sem)


def wait_bytes(ref, sem):
    pltpu.make_async_copy(ref, ref, sem).wait()


VMEM_LIMIT = 52 * 2 ** 20
NUM_SENDS = 31
NUM_RECVS = 57
NUM_LOADS = NQ * NM + 3


class Phase:
    def __init__(self):
        self.current = None

    def __call__(self, name):
        if self.current is not None:
            self.current.__exit__(None, None, None)
        self.current = None
        if name:
            self.current = jax.named_scope(name)
            self.current.__enter__()


def kernel(mask_hbm, u0_hbm, i0_hbm, trip_hbm, outu_ref, outi_ref, loss_ref,
           maskv, maskb, adj, csum, crd, crx, cch, invi, racc, rsum, rrecv, invu, trip_ref,
           upan, upart, urecv, ipan, ipart, ird, irx, isum,
           ohp, ohn, ohu, hip, hin, hiu, gpart, gsum, grd, grx, eu, zbuf,
           in_sems, send_sems, recv_sems):
    users, quarter = maskv.shape[1:]
    own_users = u0_hbm.shape[1]
    sc = ipan.shape[-1]
    hh = gpart.shape[-1]
    home = NY * hh
    mh = quarter // NM
    pieces, halves = range(NS), range(2)
    own, core, other, both = range(NQ)
    order = (both, other, core, own)

    z, y, r = lax.axis_index("emb"), lax.axis_index("col"), lax.axis_index("row")
    x, c = r // 2, r % 2
    nz = zbuf.shape[0] // (NQ * NY)
    slot = (z * NQ + r) * NY + y

    def rel(m):
        xx = x if m in (own, core) else 1 - x
        cc = c if m in (own, other) else 1 - c
        return 2 * xx + cc

    dev_d, dev_x, dev_xd = [(z, y, rel(m)) for m in (core, other, both)]
    dev_y, dev_xy = (z, 1 - y, r), (z, 1 - y, rel(other))
    flip = [(1 - z // 2, 1 - z % 2), (1 - z // 2, z % 2), (z // 2, 1 - z % 2), (z // 2, z % 2)]
    score_devs = [(2 * a + b, yy, rel(m)) for a, b in flip for yy in (1 - y, y) for m in order][:-1]

    cp = Copies(send_sems, recv_sems)
    phase = Phase()
    phase("start")
    loads = []

    def load(src, dst, sem=None):
        if sem is None:
            loads.append(in_sems.at[len(loads)])
            sem = loads[-1]
        copy = pltpu.make_async_copy(src, dst, sem)
        copy.start()
        return copy

    y_off = pl.multiple_of(y * own_users, own_users)
    own_u = pl.ds(y_off, own_users)
    mask_copies, small = {}, []
    for m in order:
        for h in range(NM):
            off = pl.multiple_of(rel(m) * quarter + h * mh, mh)
            mask_copies[m, h] = load(mask_hbm.at[:, pl.ds(off, mh)], maskv.at[m, :, pl.ds(h * mh, mh)])
        if m == both:
            small.append(load(u0_hbm, upan.at[0, :, own_u]))
            loads.append(in_sems.at[len(loads)])
            i0_sem = loads[-1]
            for s in pieces:
                load(i0_hbm.at[:, pl.ds(s * sc, sc)], ipan.at[0, own, s], i0_sem)
            small.append(load(trip_hbm, trip_ref))

    barrier = pltpu.get_barrier_semaphore()
    for dev in score_devs:
        pl.semaphore_signal(barrier, inc=1, device_id=dev, device_id_type=MESH)

    racc[...] = jnp.zeros_like(racc)

    def sums(m):
        for h in range(NM):
            mask_copies[m, h].wait()

            def body(j, carry):
                off = pl.multiple_of(h * mh + j * LB, LB)
                tile = h * (mh // LANES) + j * (LB // LANES)
                part = None
                for i in range(users // ROWS):
                    rows = pl.ds(ROWS * i, ROWS)
                    blk = maskv[m, rows, pl.ds(off, LB)]
                    ones = blk.astype(F32).astype(BF16)
                    row = None
                    for g in range(LB // LANES):
                        lanes = slice(LANES * g, LANES * (g + 1))
                        maskb[m, tile + g, rows, :] = ones[:, lanes]
                        row = blk[:, lanes] if row is None else row + blk[:, lanes]
                    racc[rows, :] += row
                    two = blk[:ROWS // 2] + blk[ROWS // 2:]
                    part = two if part is None else part + two
                csum[m, :, pl.ds(off, LB)] = jnp.sum(part.astype(F32), axis=0, keepdims=True)
                return carry
            lax.fori_loop(0, mh // LB, body, 0)

    def one_hot(lanes):
        hit = lax.broadcasted_iota(jnp.int32, (GL, LANES), 0) == lanes
        return jnp.where(hit, 1.0, 0.0).astype(BF16)

    def hot_block(oh, t):
        n = LB // LANES
        return jnp.concatenate([oh[t * n + i] for i in range(n)], axis=1)

    def one_hots(m):
        base = pl.multiple_of(rel(m) * home, home)
        for row, oh, hi in ((1, ohp, hip), (2, ohn, hin)):
            ids = trip_ref[pl.ds(row, 1), pl.ds(base, home)]
            owned = ids // quarter == y * NQ + r
            hi[m] = (ids % quarter) // GL
            low = jnp.where(owned, ids % GL, -1)
            for t in range(home // LANES):
                oh[m, t] = one_hot(low[:, t * LANES:(t + 1) * LANES])

    def user_one_hots():
        base = pl.multiple_of((r * NY + y) * hh, hh)
        uids = trip_ref[pl.ds(0, 1), pl.ds(base, hh)]
        hiu[...] = uids // users
        low = uids % users
        for t in range(hh // LANES):
            ohu[t] = one_hot(low[:, t * LANES:(t + 1) * LANES])

    csum_d, csum_x = {}, cp.recv_sem()

    def chip_sums(m):
        csum_d[m].wait_recv()
        cch[m] = csum[m] + crd[m]
        cp.send(cch.at[m], crx.at[m ^ other], dev_x, "chip", cch, csum_x)

    def send_sums(m):
        csum_d[m ^ core] = cp.send(csum.at[m], crd.at[m ^ core], dev_d, "sums", csum)

    phase("sums32")
    sums(both)
    sums(other)
    for copy in small:
        copy.wait()
    wait_bytes(ipan.at[0, own], i0_sem)
    phase("barrier")
    pl.semaphore_wait(barrier, len(score_devs))
    phase("sums10")
    send_sums(both)
    send_sums(other)
    u0_y = cp.send(upan.at[0, :, own_u], upan.at[0, :, own_u], dev_y)
    i0_d = cp.send(ipan.at[0, own], ipan.at[0, core], dev_d)
    sums(core)
    send_sums(core)
    chip_sums(both)
    chip_sums(other)
    sums(own)
    send_sums(own)
    phase("rows")
    rows = jnp.transpose(racc[...].astype(F32), (1, 0))
    rsum[...] = jnp.sum(rows, axis=0, keepdims=True)
    rs_y = cp.send(rsum, rrecv, dev_y)
    chip_sums(core)
    one_hots(both)
    phase("chip0")
    chip_sums(own)
    i0_x = cp.send(ipan.at[0, own], ipan.at[0, other], dev_x)
    phase("onehots")
    one_hots(other)
    one_hots(core)
    phase("rs_wait")
    u0_y.wait_recv()
    rs_y.wait_recv()
    inv_row = lax.rsqrt(jnp.maximum(rsum[...] + rrecv[...], 1.0))
    invu[...] = jnp.transpose(jnp.broadcast_to(inv_row, (LANES, users)), (1, 0))
    phase("cx_wait")
    wait_bytes(crx, csum_x)
    for m in order:
        invi[m] = lax.rsqrt(jnp.maximum(cch[m] + crx[m], 1.0))

    tiles = sc // LANES

    def build(m, s):
        for tile in range(s * tiles, (s + 1) * tiles):
            scale = (invu[...] * invi[m, :, tile * LANES:(tile + 1) * LANES]).astype(BF16)
            adj[m, tile] = scale * maskb[m, tile]

    def block(m, s, n, rows):
        return jnp.concatenate([adj[m, t, rows, :] for t in range(s * tiles, (s + n) * tiles)], axis=1)

    def items(k, m, some=pieces):
        for s in some:
            ipart[k, m, s] = jnp.dot(upan[k], block(m, s, 1, slice(0, users)), preferred_element_type=F32)

    def user_part(k, m, acc=None, s=0, n=NS):
        table = jnp.concatenate([ipan[k, m, s + i] for i in range(n)], axis=1)
        out = []
        for h in halves:
            part = lax.dot_general(
                table, block(m, s, n, slice(h * own_users, (h + 1) * own_users)),
                (((1,), (1,)), ((), ())), preferred_element_type=F32)
            out.append(part if acc is None else acc[h] + part)
        return out

    d, xs, g, gd, f = {}, {}, {}, {}, {}
    shared, last = {}, NS - 1

    def share(*name):
        if name not in shared:
            shared[name] = cp.recv_sem()
        return shared[name]

    def core_send(k, s):
        d[k, s] = cp.send(ipart.at[k, both, s], ird.at[k, 1, s], dev_d, ("core", k), ipart.at[k, both],
            share("core", k) if k == 1 else None)

    def core_send_own(k):
        d[k] = cp.send(ipart.at[k, core], ird.at[k, 0], dev_d)

    def x_send(k, s):
        if k != 1:
            d[k, s].wait_recv()
        elif s == 0:
            wait_bytes(ird.at[k, 1], share("core", k))
        isum[k, s] = ipart[k, other, s] + ird[k, 1, s]
        xs[k, s] = cp.send(isum.at[k, s], irx.at[k, s], dev_x, ("x", k), isum.at[k])

    def own_piece(k, s):
        if s == 0:
            d[k].wait_recv()
        xs[k, s].wait_recv()
        total = (ipart[k, own, s] + ird[k, 0, s]) + irx[k, s]
        ipan[k + 1, own, s] = total.astype(BF16)

    def own_gather(k, s):
        own_piece(k, s)
        g[k + 1, s] = cp.send(
            ipan.at[k + 1, own, s], ipan.at[k + 1, other, s], dev_x, ("gather", k), ipan.at[k + 1, own])
        if s == NS - 1:
            gd[k + 1] = cp.send(ipan.at[k + 1, own], ipan.at[k + 1, core], dev_d)

    batches = {1: (range(last), range(last, NS)), 2: (halves, range(2, NS))}

    def take_forwarded(k, i):
        batch = batches[k][i]
        wait_bytes(ipan.at[k, both, pl.ds(batch.start, len(batch))], share("forward", k, i == 0))

    def forward(k, s):
        g[k, s].wait_recv()
        f[k, s] = cp.send(ipan.at[k, other, s], ipan.at[k, both, s], dev_d, ("forward", k), ipan.at[k, other],
            share("forward", k, s in batches[k][0]))

    def send_user(k, acc):
        for h in halves:
            upart[k, :, h * own_users:(h + 1) * own_users] = acc[h]
        return cp.send(upart.at[k], urecv.at[k], dev_y)

    def take_user(k, got):
        got.wait_recv()
        upan[k + 1] = (upart[k] + urecv[k]).astype(BF16)

    phase("build32")
    for s in range(NS + 1):
        if s < NS:
            build(both, s)
            items(0, both, [s])
        if s:
            build(other, s - 1)
        if s < NS:
            core_send(0, s)
        if s:
            items(0, other, [s - 1])
        if s in range(2, NS):
            x_send(0, s - 2)
    phase("build10")
    for s in pieces:
        build(core, s)
        if s in (1, last):
            x_send(0, NS - 2 + s // 2)
    for s in pieces:
        build(own, s)
    phase("i0_x_wait")
    i0_x.wait_recv()
    i0_f = cp.send(ipan.at[0, other], ipan.at[0, both], dev_d)
    phase("upart0")
    i0_d.wait_recv()
    acc = user_part(0, core, user_part(0, own))
    acc = user_part(0, other, acc)
    phase("upart0b")
    i0_f.wait_recv()
    acc = user_part(0, both, acc)
    u1 = send_user(0, acc)
    phase("items1_10")
    items(0, core)
    core_send_own(0)
    items(0, own)
    for s in range(last):
        if s == last - 1:
            one_hots(own)
            user_one_hots()
        phase(f"own1_{s}")
        own_gather(0, s)
    phase("u1_wait")
    take_user(0, u1)

    def items_x(k, between=None):
        items(k, both)
        items(k, other, [0])
        for s in pieces:
            core_send(k, s)
        if between is not None:
            between()
        items(k, other, range(1, NS))

    phase("items2_32")
    items_x(1)
    phase("own1_last")
    own_gather(0, last)
    phase("items2_10")
    items(1, core)
    core_send_own(1)
    phase("x2")
    for s in pieces:
        x_send(1, s)
    items(1, own)
    phase("fwd1_0")
    forward(1, 0)
    acc = user_part(1, own)
    phase("fwd1_1")
    forward(1, 1)
    gd[1].wait_recv()
    acc = user_part(1, core, acc)
    phase("fwd1_2")
    forward(1, 2)
    acc = user_part(1, other, acc, 0, last)
    phase("fwd1_3")
    forward(1, last)
    acc = user_part(1, other, acc, last, 1)
    take_forwarded(1, 0)
    acc = user_part(1, both, acc, 0, last)
    phase("f1_wait")
    take_forwarded(1, 1)
    acc = user_part(1, both, acc, last, 1)
    u2 = send_user(1, acc)
    phase("own2_01")
    own_gather(1, 0)
    own_gather(1, 1)
    phase("u2_wait")
    take_user(1, u2)
    phase("items3_32")
    items_x(2, lambda: own_gather(1, 2))
    items(2, core)
    phase("x3")
    x_send(2, 0)
    core_send_own(2)
    phase("own2_3")
    own_gather(1, last)
    for s in range(1, NS):
        x_send(2, s)
    phase("items3_own")
    items(2, own)
    phase("upart2_01")
    acc = user_part(2, own)
    gd[2].wait_recv()
    acc = user_part(2, core, acc)
    phase("fwd2_01")
    for s in halves:
        forward(2, s)
    acc = user_part(2, other, acc, 0, 2)
    take_forwarded(2, 0)
    acc = user_part(2, both, acc, 0, 2)
    phase("fwd2_23")
    for s in (2, last):
        forward(2, s)
    acc = user_part(2, other, acc, 2, NS - 2)
    phase("f2_wait")
    take_forwarded(2, 1)
    acc = user_part(2, both, acc, 2, NS - 2)
    u3 = send_user(2, acc)

    def mean4(a, b, e, h):
        tot = ((a.astype(F32) + b.astype(F32)) + e.astype(F32)) + h.astype(F32)
        return (tot * (1.0 / (NUM_LAYERS + 1))).astype(BF16)

    def pick(tab, oh, hi, first):
        got = jnp.dot(tab, oh, preferred_element_type=F32)
        n = got.shape[0] // ROWS
        out = jnp.where(hi == first, got[:ROWS], 0.0)
        for i in range(1, n):
            out = out + jnp.where(hi == first + i, got[i * ROWS:(i + 1) * ROWS], 0.0)
        return out

    def final_piece(s):
        own_piece(2, s)
        outi_ref[:, s * sc:(s + 1) * sc] = mean4(*[ipan[k, own, s] for k in range(NUM_LAYERS + 1)])

    def differences(m, h, first, n):
        groups = range(first * sc // GL, (first + n) * sc // GL)
        table = jnp.concatenate([outi_ref[:, i * GL:(i + 1) * GL] for i in groups], axis=0)
        for t in range(h * (hh // LB), (h + 1) * (hh // LB)):
            sl = slice(t * LB, (t + 1) * LB)
            pos = pick(table, hot_block(ohp.at[m], t), hip[m, :, sl], groups[0])
            neg = pick(table, hot_block(ohn.at[m], t), hin[m, :, sl], groups[0])
            out = slice(t * LB - h * hh, (t + 1) * LB - h * hh)
            gpart[m, h, :, out] = pos - neg if first == 0 else (gpart[m, h, :, out] + pos) - neg

    phase("own3")
    for s in range(last):
        final_piece(s)
    phase("diff_012")
    for m in order:
        for h in halves:
            differences(m, h, 0, last)
    phase("u3_wait")
    take_user(2, u3)
    phase("finalu")
    eu[own] = mean4(*[upan[k] for k in range(NUM_LAYERS + 1)])
    others = eu.at[pl.ds(core, NQ - 1)]
    eu_sem = cp.recv_sem()
    for m, dev in ((core, dev_d), (other, dev_x), (both, dev_xd)):
        cp.send(eu.at[own], eu.at[m], dev, "eu", others, eu_sem)
    outu_ref[...] = eu[own, :, own_u]

    phase("own3_last")
    final_piece(last)
    gd3 = {}
    phase("diff3")
    for h in halves:
        differences(both, h, last, 1)
        gd3[h] = cp.send(gpart.at[both, h], grd.at[1, h], dev_d)
    for h in halves:
        differences(other, h, last, 1)
    for h in halves:
        differences(core, h, last, 1)
    gd1 = cp.send(gpart.at[core], grd.at[0], dev_d)
    phase("gd3_wait")
    for h in halves:
        gd3[h].wait_recv()

    g_sem = cp.recv_sem()

    def home_send(i, m, h, dev):
        gsum[i] = gpart[m, h] + grd[m // 2, h]
        cp.send(gsum.at[i], grx.at[i], dev, "home", gsum, g_sem)

    home_send(0, other, 1 - y, dev_xy)
    home_send(1, other, y, dev_x)
    phase("diff0")
    for h in halves:
        differences(own, h, last, 1)
    phase("gd1_wait")
    gd1.wait_recv()
    home_send(2, own, 1 - y, dev_y)
    phase("e_wait")
    wait_bytes(others, eu_sem)
    phase("picku")
    utab = jnp.concatenate([eu[m] for m in range(NQ)], axis=0)
    place = jnp.where(hiu[...] // 2 == x, own, other) + jnp.where(hiu[...] % 2 == c, own, core)
    picked = [pick(utab, hot_block(ohu, t), place[:, t * LB:(t + 1) * LB], own) for t in range(hh // LB)]
    phase("gy_wait")
    wait_bytes(grx, g_sem)
    phase("dot")
    for t in range(hh // LB):
        sl = slice(t * LB, (t + 1) * LB)
        mine = gpart[own, y, :, sl] + grd[0, y, :, sl]
        diff = (mine + grx[1, :, sl]) + (grx[2, :, sl] + grx[0, :, sl])
        zbuf[slot, :, sl] = jnp.sum(picked[t] * diff, axis=0, keepdims=True)
    rest = zbuf.at[pl.ds(0, len(score_devs))]
    z_sem = cp.recv_sem()
    for dev in score_devs:
        cp.send(zbuf.at[slot], zbuf.at[slot], dev, "score", rest, z_sem)
    phase("z_wait")
    wait_bytes(rest, z_sem)
    phase("loss")
    for q in range(NQ * NY):
        neg = -sum(zbuf[k * NQ * NY + q] for k in range(nz))
        loss_ref[q] = jnp.maximum(neg, 0.0) + jnp.log1p(jnp.exp(-jnp.abs(neg)))
    phase("drain")
    cp.drain()
    phase(None)
    assert (len(cp.groups) + len(cp.single), cp.recvs, len(loads)) == (NUM_SENDS, NUM_RECVS, NUM_LOADS)


def emit(*refs):
    n = len(refs) // 2
    sems = refs[-1]
    copies = [pltpu.make_async_copy(src, dst, sems.at[i]) for i, (src, dst) in enumerate(zip(refs[:n], refs[n:]))]
    for copy in copies:
        copy.start()
    for copy in copies:
        copy.wait()


def solution(mesh):
    def local_fn(mask_blk, user_sh, item_sh, triples):
        users, items = mask_blk.shape
        cols, own_users = user_sh.shape[1], user_sh.shape[0]
        quarter = items // NQ
        home = triples.shape[0] // NQ
        hh = home // NY
        vm, sem = pltpu.VMEM, pltpu.SemaphoreType.DMA
        nl = NUM_LAYERS
        sc = quarter // NS
        tiles = (NQ, quarter // LANES, users, LANES)
        per_item, hots = (NQ, 1, quarter), (NQ, home // LANES, GL, LANES)
        triple_row = (NQ, 1, home)
        scratch = [
            vm((NQ, users, quarter), jnp.int32), vm(tiles, BF16), vm(tiles, BF16),
            *[vm(per_item, F32)] * 5,
            vm((users, LANES), jnp.int32), vm((1, users), F32), vm((1, users), F32), vm((users, LANES), F32),
            vm(triples.shape[::-1], jnp.int32),
            vm((nl + 1, cols, users), BF16), vm((nl, cols, users), F32), vm((nl, cols, users), F32),
            vm((nl + 1, NQ, NS, cols, sc), BF16), vm((nl, NQ, NS, cols, sc), F32),
            vm((nl, 2, NS, cols, sc), F32), vm((nl, NS, cols, sc), F32), vm((nl, NS, cols, sc), F32),
            vm(hots, BF16), vm(hots, BF16), vm((hh // LANES, GL, LANES), BF16),
            vm(triple_row, jnp.int32), vm(triple_row, jnp.int32), vm((1, hh), jnp.int32),
            vm((NQ, NY, cols, hh), F32), vm((3, cols, hh), F32), vm((2, NY, cols, hh), F32), vm((3, cols, hh), F32),
            vm((NQ, cols, users), BF16), vm((mesh.size, 1, hh), F32),
            sem((NUM_LOADS,)), sem((NUM_SENDS,)), sem((NUM_RECVS,)),
        ]
        vspec = pl.BlockSpec(memory_space=pltpu.VMEM)
        out_u, out_i, loss = pl.pallas_call(
            kernel,
            out_shape=[
                jax.ShapeDtypeStruct((cols, own_users), BF16),
                jax.ShapeDtypeStruct((cols, quarter), BF16),
                jax.ShapeDtypeStruct((NQ * NY, 1, hh), F32)],
            in_specs=[pl.BlockSpec(memory_space=pltpu.HBM)] * 4,
            out_specs=[vspec, vspec, vspec],
            scratch_shapes=scratch,
            compiler_params=pltpu.CompilerParams(
                collective_id=0, has_side_effects=True, vmem_limit_bytes=VMEM_LIMIT),
        )(*[pltpu.with_memory_space_constraint(a, pltpu.HBM) for a in (mask_blk, user_sh.T, item_sh.T, triples.T)])
        out_u, out_i, loss = pl.pallas_call(
            emit,
            out_shape=[jax.ShapeDtypeStruct(a.shape, a.dtype) for a in (out_u, out_i, loss)],
            in_specs=[vspec] * 3, out_specs=[pl.BlockSpec(memory_space=pltpu.HBM)] * 3,
            scratch_shapes=[sem((3,))],
            compiler_params=pltpu.CompilerParams(vmem_limit_bytes=2 ** 20),
        )(out_u, out_i, loss)
        return out_u.T, out_i.T, loss.reshape(-1)

    return jax.shard_map(
        local_fn, mesh=mesh,
        in_specs=(P("row", "col"), P(("row", "col"), "emb"), P(("col", "row"), "emb"), P()),
        out_specs=(P(("row", "col"), "emb"), P(("col", "row"), "emb"), P()),
        check_vma=False)
```
